8 devices in a mesh: fld: 1 (over z), col: 2 (over y), row: 4 (over x, core).
Axes of the slice: x: 2, y: 2, z: 1, core: 2. Of those that a mesh axis runs over, the one named last changes fastest.
Arguments:
- u_real: float32 [32, 64, 64, 64], P('fld', None, 'row', 'col')
- u_imag: float32 [32, 64, 64, 64], P('fld', None, 'row', 'col')
- g_filter: float32 [64, 64, 64], P('row', 'col')
Outputs:
- output 1: float32 [32, 64, 64, 64], P('fld', 'row', 'col')
- output 2: float32 [32, 64, 64, 64], P('fld', 'row', 'col')
All inputs are finite; a program needn't handle non-finite values.
Results may differ from the reference program's by a relative error of at most 0.001.
Values are sent between devices in bfloat16 or wider.
A program may use at most 1 GiB of HBM per device.

```python
import jax
import jax.numpy as jnp
from jax import lax

N = 64
BATCH = 32


def setup_inputs(seed: int = 0, part: int = 0) -> dict:
    root_key = jax.random.key(seed)
    field_key = jax.random.fold_in(jax.random.fold_in(root_key, 1), part)
    key_re, key_im = jax.random.split(field_key)
    u_real = jax.random.normal(key_re, (BATCH, N, N, N), jnp.float32)
    u_imag = jax.random.normal(key_im, (BATCH, N, N, N), jnp.float32)
    wave_num = ((jnp.arange(N) + N // 2) % N - N // 2).astype(jnp.float32)
    wave_sq = wave_num * wave_num
    k_sq = wave_sq[:, None, None] + wave_sq[None, :, None] + wave_sq[None, None, :]
    profile = 2.0 / (1.0 + 16.0 * k_sq / (N * N))
    jitter = jax.random.uniform(jax.random.fold_in(root_key, 2), (N, N, N), jnp.float32)
    g_filter = profile * (0.5 + jitter)
    return {"u_real": u_real, "u_imag": u_imag, "g_filter": g_filter}


def reference(u_real, u_imag, g_filter):
    def one_field(field_pair):
        field_re, field_im = field_pair
        spectrum = jnp.fft.fftn(field_re + 1j * field_im, norm="ortho")
        filtered = spectrum * g_filter
        return jnp.real(filtered).astype(jnp.float32), jnp.imag(filtered).astype(jnp.float32)
    w_real, w_imag = lax.map(one_field, (u_real, u_imag))
    return w_real, w_imag
```

```python
import functools
import math

import jax
import jax.numpy as jnp
import numpy as np
from jax import lax
from jax.experimental import pallas as pl
from jax.experimental.pallas import tpu as pltpu
from jax.sharding import PartitionSpec as P

MESH = pl.DeviceIdType.MESH
HALF = math.sqrt(0.5)
GROUPS, PACK, UNITS, LAG = 8, 4, 16, 2


def dft4(b):
    (r0, i0), (r1, i1), (r2, i2), (r3, i3) = b
    sr0, si0, sr1, si1 = r0 + r2, i0 + i2, r0 - r2, i0 - i2
    sr2, si2, sr3, si3 = r1 + r3, i1 + i3, r1 - r3, i1 - i3
    return [(sr0 + sr2, si0 + si2), (sr1 + si3, si1 - sr3), (sr0 - sr2, si0 - si2), (sr1 - si3, si1 + sr3)]


def dft8(a):
    even = [(a[j][0] + a[j + 4][0], a[j][1] + a[j + 4][1]) for j in range(4)]
    odd = [(a[j][0] - a[j + 4][0], a[j][1] - a[j + 4][1]) for j in range(4)]
    (r1, i1), (r2, i2), (r3, i3) = odd[1:]
    odd = [odd[0], ((r1 + i1) * HALF, (i1 - r1) * HALF), (i2, -r2), ((i3 - r3) * HALF, (r3 + i3) * -HALF)]
    even, odd = dft4(even), dft4(odd)
    return [(even if k % 2 == 0 else odd)[k // 2] for k in range(8)]


def times(a, tr, ti):
    return a[0] * tr - a[1] * ti, a[0] * ti + a[1] * tr


def twiddle(m):
    angle = -2.0 * math.pi * (m % 64) / 64.0
    return math.cos(angle) / 8.0, math.sin(angle) / 8.0


def lane_matrix():
    z, kz = np.arange(64), np.arange(64)
    angle = 2.0 * np.pi * ((z[:, None] * kz[None, :]) % 64) / 64.0
    cos, sin = np.cos(angle) / 8.0, np.sin(angle) / 8.0
    blocks = np.stack([np.concatenate([cos, -sin], 1), np.concatenate([sin, cos], 1)])
    out = np.zeros((2, 2, PACK, 32, PACK, 128))
    for c in range(2):
        for f in range(PACK):
            out[c, :, f, :, f, :] = blocks[:, 32 * c : 32 * c + 32]
    return out.reshape(2, 256, PACK * 128).astype(np.float32)


def sublane_twiddle():
    k1, x2 = np.arange(8), np.arange(8)
    angle = -2.0 * np.pi * (k1[:, None] * x2[None, :]) / 64.0
    both = np.stack([np.cos(angle), np.sin(angle)]) / 8.0
    return np.broadcast_to(both[..., None], (2, 8, 8, 128)).astype(np.float32)


def kernel(ur, ui, gf, wz, tw, out, inr, ini, xbuf, b2, r2, obuf, wv, tv, gs, gv, asc, bsc, lsc,
           in_sem, c_sem, s1, d1, s2, d2, o_sem):
    row, col = lax.axis_index("row"), lax.axis_index("col")
    core = lax.rem(row, 2)
    dests = [2 - core, 3 - core, 1 + 2 * core]
    other = 1 - col

    barrier = pltpu.get_barrier_semaphore()
    for p in (1, 2, 3):
        pl.semaphore_signal(barrier, inc=1, device_id={"row": lax.rem(row + p, 4)}, device_id_type=MESH)
    pl.semaphore_signal(barrier, inc=1, device_id={"col": other}, device_id_type=MESH)

    def load(g, k):
        src, dst = ((ur, inr), (ui, ini))[k]
        return pltpu.make_async_copy(src.at[g], dst.at[g], in_sem.at[2 * g + k])

    load(0, 0).start()
    load(0, 1).start()
    consts = [
        pltpu.make_async_copy(tw, tv, c_sem.at[0]),
        pltpu.make_async_copy(wz.at[col], wv.at[pl.ds(0, 256)], c_sem.at[1]),
        pltpu.make_async_copy(wz.at[other], wv.at[pl.ds(256, 256)], c_sem.at[2]),
        pltpu.make_async_copy(gf, gs, c_sem.at[3]),
    ]
    consts[0].start()

    @pl.loop(1, GROUPS)
    def _(g):
        load(g, 0).start()
        load(g, 1).start()

    for copy in consts[1:]:
        copy.start()
    consts[0].wait()

    def step_x(g, first, count):
        slots = [3 + lax.rem(k + 4 - row, 4) for k in range(4)]
        bases = [[(2 * g + t) * 7 + slots[k] for t in range(2)] for k in range(4)]

        def one(y, s):
            ar = inr[g, :, y].reshape(PACK * 32, 64).T
            ai = ini[g, :, y].reshape(PACK * 32, 64).T
            a = dft8([(ar[8 * j : 8 * j + 8], ai[8 * j : 8 * j + 8]) for j in range(8)])
            for k1 in range(8):
                vr, vi = times(a[k1], tv[0, k1], tv[1, k1])
                asc[s, 0, pl.ds(8 * k1, 8), :] = vr
                asc[s, 1, pl.ds(8 * k1, 8), :] = vi
            b = dft8([tuple(asc[s, q, pl.ds(x2, 8, stride=8), :] for q in range(2)) for x2 in range(8)])
            for k2 in range(8):
                for q in range(2):
                    xbuf[bases[k2 // 2][k2 % 2], y, q] = b[k2][q]

        @pl.loop(0, count // 2)
        def _(i):
            one(first + 2 * i, 0)
            one(first + 2 * i + 1, 1)

    def send_row(u, j):
        p = dests[j]
        return pltpu.make_async_remote_copy(
            src_ref=xbuf.at[u * 7 + 3 + p], dst_ref=xbuf.at[u * 7 + 3 - p],
            send_sem=s1.at[u * 3 + j], recv_sem=d1.at[u * 3 + 3 - p],
            device_id={"row": lax.rem(row + p, 4)}, device_id_type=MESH)

    def wait_row(u, slot):
        part = xbuf.at[u * 7 + slot]
        pltpu.make_async_remote_copy(
            src_ref=part, dst_ref=part, send_sem=s1.at[u * 3], recv_sem=d1.at[u * 3 + slot],
            device_id={"row": row}, device_id_type=MESH).wait_recv()

    def send_col(u):
        return pltpu.make_async_remote_copy(
            src_ref=b2.at[pl.ds(u * 4 + 2 * other, 2)], dst_ref=r2.at[pl.ds(u * 2, 2)],
            send_sem=s2.at[u], recv_sem=d2.at[u], device_id={"col": other}, device_id_type=MESH)

    def step_y(u):
        slots = [u * 7 + lax.rem(r + 7 - row, 4) for r in range(4)]
        for y2 in range(8):
            a = dft8([tuple(xbuf[slots[y1 // 2], 8 * (y1 % 2) + y2, q] for q in range(2)) for y1 in range(8)])
            for k1 in range(8):
                vr, vi = times(a[k1], *twiddle(k1 * y2))
                bsc[k1, y2, 0] = vr
                bsc[k1, y2, 1] = vi
        for k1 in range(8):
            b = dft8([(bsc[k1, y2, 0], bsc[k1, y2, 1]) for y2 in range(8)])
            for k2 in range(8):
                for q in range(2):
                    b2[u * 4 + 2 * (k2 // 4) + q, pl.ds(8 * (k1 + 8 * (k2 % 4)), 8), :] = b[k2][q]

    def write(u):
        return pltpu.make_async_copy(
            obuf.at[lax.rem(u, 4)],
            out.at[pl.ds(PACK * (u // 2), PACK), pl.ds(8 * lax.rem(u, 2), 8)], o_sem.at[lax.rem(u, 4)])

    def step_z(u):
        for kx in range(8):
            for q in range(2):
                lsc[pl.ds(32 * kx, 32), pl.ds(128 * q, 128)] = b2[u * 4 + 2 * col + q, pl.ds(kx, 32, stride=8), :]
                lsc[pl.ds(32 * kx, 32), pl.ds(256 + 128 * q, 128)] = r2[u * 2 + q, pl.ds(kx, 32, stride=8), :]
        gain = gv[pl.ds(pl.multiple_of(256 * lax.rem(u, 2), 256), 256), :]
        for n in range(2):
            w = jnp.dot(lsc[...], wv[:, 256 * n : 256 * n + 256], precision=lax.Precision.HIGHEST,
                        preferred_element_type=jnp.float32)
            for f in range(2):
                obuf[lax.rem(u, 4), 2 * n + f] = (w[:, 128 * f : 128 * f + 128] * gain).reshape(8, 32, 128)

    for g in range(2):
        load(g, 0).wait()
        load(g, 1).wait()
        step_x(g, 0, 16)
        if g == 0:
            pl.semaphore_wait(barrier, 4)
        for t in range(2):
            for j in range(3):
                send_row(2 * g + t, j).start()

    for copy in consts[1:]:
        copy.wait()
    gain = gs[...].reshape(512, 64)
    gv[...] = jnp.concatenate([gain, gain], axis=1)

    @pl.loop(0, UNITS + LAG)
    def _(t):
        @pl.when(t < UNITS)
        def _():
            for slot in range(3):
                wait_row(t, slot)
            step_y(t)
            send_col(t).start()

        g = t // 2 + 2

        @pl.when(g < GROUPS)
        def _():
            half = lax.rem(t, 2)

            @pl.when(half == 0)
            def _():
                load(g, 0).wait()
                load(g, 1).wait()

            step_x(g, 8 * half, 8)

            @pl.when(half == 1)
            def _():
                for k in range(2):
                    for j in range(3):
                        send_row(2 * g + k, j).start()

        @pl.when(t >= LAG)
        def _():
            u = t - LAG
            send_col(u).wait_recv()

            @pl.when(u >= 4)
            def _():
                write(u - 4).wait()

            step_z(u)
            write(u).start()

    @pl.loop(0, UNITS)
    def _(u):
        for j in range(3):
            send_row(u, j).wait_send()
        send_col(u).wait_send()

    @pl.loop(UNITS - 4, UNITS)
    def _(u):
        write(u).wait()


def solution(mesh):
    f32 = jnp.float32

    def local_forward(u_real, u_imag, g_filter):
        parts = [jnp.transpose(v, (0, 2, 3, 1)).reshape(GROUPS, PACK, 16, 32, 64) for v in (u_real, u_imag)]
        packed = pl.pallas_call(
            kernel,
            out_shape=jax.ShapeDtypeStruct((32, 16, 32, 128), f32),
            in_specs=[pl.BlockSpec(memory_space=pltpu.HBM)] * 5,
            out_specs=pl.BlockSpec(memory_space=pltpu.HBM),
            scratch_shapes=[
                pltpu.VMEM((GROUPS, PACK, 16, 32, 64), f32),
                pltpu.VMEM((GROUPS, PACK, 16, 32, 64), f32),
                pltpu.VMEM((UNITS * 7, 16, 2, 8, 128), f32),
                pltpu.VMEM((UNITS * 4, 256, 128), f32),
                pltpu.VMEM((UNITS * 2, 256, 128), f32),
                pltpu.VMEM((4, PACK, 8, 32, 128), f32),
                pltpu.VMEM((512, 512), f32),
                pltpu.VMEM((2, 8, 8, 128), f32),
                pltpu.VMEM((16, 32, 64), f32),
                pltpu.VMEM((512, 128), f32),
                pltpu.VMEM((2, 2, 64, 128), f32),
                pltpu.VMEM((8, 8, 2, 8, 128), f32),
                pltpu.VMEM((256, 512), f32),
                pltpu.SemaphoreType.DMA((2 * GROUPS,)),
                pltpu.SemaphoreType.DMA((4,)),
                pltpu.SemaphoreType.DMA((3 * UNITS,)),
                pltpu.SemaphoreType.DMA((3 * UNITS,)),
                pltpu.SemaphoreType.DMA((UNITS,)),
                pltpu.SemaphoreType.DMA((UNITS,)),
                pltpu.SemaphoreType.DMA((4,)),
            ],
            compiler_params=pltpu.CompilerParams(
                collective_id=0, has_side_effects=True, vmem_limit_bytes=60 * 1024 * 1024),
            name="dft3",
        )(*parts, g_filter, jnp.asarray(lane_matrix()), jnp.asarray(sublane_twiddle()))
        return packed[..., :64], packed[..., 64:]

    field_spec = P("fld", None, "row", "col")
    out_spec = P("fld", "row", "col", None)
    return jax.shard_map(local_forward, mesh=mesh, in_specs=(field_spec, field_spec, P("row", "col", None)),
                         out_specs=(out_spec, out_spec), check_vma=False)
```

```python
import functools
import math

import jax
import jax.numpy as jnp
import numpy as np
from jax import lax
from jax.experimental import pallas as pl
from jax.experimental.pallas import tpu as pltpu
from jax.sharding import PartitionSpec as P

MESH = pl.DeviceIdType.MESH
HALF = math.sqrt(0.5)
GROUPS, PACK, UNITS, LAG, RING = 8, 4, 16, 2, 4


def dft4(b):
    (r0, i0), (r1, i1), (r2, i2), (r3, i3) = b
    sr0, si0, sr1, si1 = r0 + r2, i0 + i2, r0 - r2, i0 - i2
    sr2, si2, sr3, si3 = r1 + r3, i1 + i3, r1 - r3, i1 - i3
    return [(sr0 + sr2, si0 + si2), (sr1 + si3, si1 - sr3), (sr0 - sr2, si0 - si2), (sr1 - si3, si1 + sr3)]


def dft8(a):
    even = [(a[j][0] + a[j + 4][0], a[j][1] + a[j + 4][1]) for j in range(4)]
    odd = [(a[j][0] - a[j + 4][0], a[j][1] - a[j + 4][1]) for j in range(4)]
    (r1, i1), (r2, i2), (r3, i3) = odd[1:]
    odd = [odd[0], ((r1 + i1) * HALF, (i1 - r1) * HALF), (i2, -r2), ((i3 - r3) * HALF, (r3 + i3) * -HALF)]
    even, odd = dft4(even), dft4(odd)
    return [(even if k % 2 == 0 else odd)[k // 2] for k in range(8)]


def times(a, tr, ti):
    return a[0] * tr - a[1] * ti, a[0] * ti + a[1] * tr


def twiddle(m):
    angle = -2.0 * math.pi * (m % 64) / 64.0
    return math.cos(angle) / 8.0, math.sin(angle) / 8.0


def lane_matrix():
    z, kz = np.arange(64), np.arange(64)
    angle = 2.0 * np.pi * ((z[:, None] * kz[None, :]) % 64) / 64.0
    cos, sin = np.cos(angle) / 8.0, np.sin(angle) / 8.0
    blocks = np.stack([np.concatenate([cos, -sin], 1), np.concatenate([sin, cos], 1)])
    out = np.zeros((2, 2, PACK, 32, PACK, 128))
    for c in range(2):
        for f in range(PACK):
            out[c, :, f, :, f, :] = blocks[:, 32 * c : 32 * c + 32]
    return out.reshape(2, 256, PACK * 128).astype(np.float32)


def sublane_twiddle():
    k1, x2 = np.arange(8), np.arange(8)
    angle = -2.0 * np.pi * (k1[:, None] * x2[None, :]) / 64.0
    both = np.stack([np.cos(angle), np.sin(angle)]) / 8.0
    return np.broadcast_to(both[..., None], (2, 8, 8, 128)).astype(np.float32)


def kernel(ur, ui, gf, wz, tw, outr, outi, inr, ini, xbuf, b2, r2, wv, tv, gs, gv, asc, bsc, lsc,
           in_sem, c_sem, s1, d1, s2, d2):
    row, col = lax.axis_index("row"), lax.axis_index("col")
    core = lax.rem(row, 2)
    dests = [2 - core, 3 - core, 1 + 2 * core]
    other = 1 - col

    barrier = pltpu.get_barrier_semaphore()
    for p in (1, 2, 3):
        pl.semaphore_signal(barrier, inc=1, device_id={"row": lax.rem(row + p, 4)}, device_id_type=MESH)
    pl.semaphore_signal(barrier, inc=1, device_id={"col": other}, device_id_type=MESH)

    def load(g, k):
        src, dst = ((ur, inr), (ui, ini))[k]
        return pltpu.make_async_copy(src.at[g], dst.at[lax.rem(g, RING)], in_sem.at[2 * lax.rem(g, RING) + k])

    load(0, 0).start()
    load(0, 1).start()
    consts = [
        pltpu.make_async_copy(tw, tv, c_sem.at[0]),
        pltpu.make_async_copy(wz.at[col], wv.at[pl.ds(0, 256)], c_sem.at[1]),
        pltpu.make_async_copy(wz.at[other], wv.at[pl.ds(256, 256)], c_sem.at[2]),
        pltpu.make_async_copy(gf, gs, c_sem.at[3]),
    ]
    consts[0].start()

    @pl.loop(1, RING)
    def _(g):
        load(g, 0).start()
        load(g, 1).start()

    for copy in consts[1:]:
        copy.start()
    consts[0].wait()

    def step_x(g, first, count):
        ring = lax.rem(g, RING)
        slots = [3 + lax.rem(k + 4 - row, 4) for k in range(4)]
        bases = [[(2 * g + t) * 7 + slots[k] for t in range(2)] for k in range(4)]

        def one(y, s):
            ar = inr[ring, :, y].reshape(PACK * 32, 64).T
            ai = ini[ring, :, y].reshape(PACK * 32, 64).T
            a = dft8([(ar[8 * j : 8 * j + 8], ai[8 * j : 8 * j + 8]) for j in range(8)])
            for k1 in range(8):
                vr, vi = times(a[k1], tv[0, k1], tv[1, k1])
                asc[s, 0, pl.ds(8 * k1, 8), :] = vr
                asc[s, 1, pl.ds(8 * k1, 8), :] = vi
            b = dft8([tuple(asc[s, q, pl.ds(x2, 8, stride=8), :] for q in range(2)) for x2 in range(8)])
            for k2 in range(8):
                for q in range(2):
                    xbuf[bases[k2 // 2][k2 % 2], y, q] = b[k2][q]

        @pl.loop(0, count // 2)
        def _(i):
            one(first + 2 * i, 0)
            one(first + 2 * i + 1, 1)

    def send_row(u, j, first=0, count=16):
        p = dests[j]
        return pltpu.make_async_remote_copy(
            src_ref=xbuf.at[u * 7 + 3 + p, pl.ds(first, count)], dst_ref=xbuf.at[u * 7 + 3 - p, pl.ds(first, count)],
            send_sem=s1.at[u * 3 + j], recv_sem=d1.at[u * 3 + 3 - p],
            device_id={"row": lax.rem(row + p, 4)}, device_id_type=MESH)

    def wait_row(u, slot):
        part = xbuf.at[u * 7 + slot]
        pltpu.make_async_remote_copy(
            src_ref=part, dst_ref=part, send_sem=s1.at[u * 3], recv_sem=d1.at[u * 3 + slot],
            device_id={"row": row}, device_id_type=MESH).wait_recv()

    def send_col(u):
        return pltpu.make_async_remote_copy(
            src_ref=b2.at[pl.ds(u * 4 + 2 * other, 2)], dst_ref=r2.at[pl.ds(u * 2, 2)],
            send_sem=s2.at[u], recv_sem=d2.at[u], device_id={"col": other}, device_id_type=MESH)

    def step_y(u):
        slots = [u * 7 + lax.rem(r + 7 - row, 4) for r in range(4)]
        for y2 in range(8):
            a = dft8([tuple(xbuf[slots[y1 // 2], 8 * (y1 % 2) + y2, q] for q in range(2)) for y1 in range(8)])
            for k1 in range(8):
                vr, vi = times(a[k1], *twiddle(k1 * y2))
                bsc[k1, y2, 0] = vr
                bsc[k1, y2, 1] = vi
        for k1 in range(8):
            b = dft8([(bsc[k1, y2, 0], bsc[k1, y2, 1]) for y2 in range(8)])
            for k2 in range(8):
                for q in range(2):
                    b2[u * 4 + 2 * (k2 // 4) + q, pl.ds(8 * (k1 + 8 * (k2 % 4)), 8), :] = b[k2][q]

    def step_z(u):
        for kx in range(8):
            for q in range(2):
                lsc[pl.ds(32 * kx, 32), pl.ds(128 * q, 128)] = b2[u * 4 + 2 * col + q, pl.ds(kx, 32, stride=8), :]
                lsc[pl.ds(32 * kx, 32), pl.ds(256 + 128 * q, 128)] = r2[u * 2 + q, pl.ds(kx, 32, stride=8), :]
        gain = gv[pl.ds(pl.multiple_of(256 * lax.rem(u, 2), 256), 256), :]
        for n in range(2):
            w = jnp.dot(lsc[...], wv[:, 256 * n : 256 * n + 256], precision=lax.Precision.HIGHEST,
                        preferred_element_type=jnp.float32)
            for f in range(2):
                pair = w[:, 128 * f : 128 * f + 128] * gain
                at = (PACK * (u // 2) + 2 * n + f, pl.ds(8 * lax.rem(u, 2), 8))
                outr[at] = pair[:, :64].reshape(8, 32, 64)
                outi[at] = pair[:, 64:].reshape(8, 32, 64)

    load(0, 0).wait()
    load(0, 1).wait()
    step_x(0, 0, 4)
    pl.semaphore_wait(barrier, 4)
    send_row(0, 0, 0, 4).start()
    send_row(0, 1, 0, 4).start()
    for y in (4, 8, 12):
        step_x(0, y, 4)
        send_row(0, 0, y, 4).start()
    send_row(0, 1, 4, 12).start()
    send_row(0, 2).start()
    for j in range(3):
        send_row(1, j).start()
    for k in range(2):
        load(RING, k).start()
        load(1, k).wait()
    step_x(1, 0, 16)
    for t in range(2):
        for j in range(3):
            send_row(2 + t, j).start()
    for k in range(2):
        load(RING + 1, k).start()

    for copy in consts[1:]:
        copy.wait()
    gain = gs[...].reshape(512, 64)
    gv[...] = jnp.concatenate([gain, gain], axis=1)

    @pl.loop(0, UNITS + LAG)
    def _(t):
        @pl.when(t < UNITS)
        def _():
            for slot in range(3):
                wait_row(t, slot)
            step_y(t)
            send_col(t).start()

        g = t // 2 + 2

        @pl.when(g < GROUPS)
        def _():
            half = lax.rem(t, 2)

            @pl.when(half == 0)
            def _():
                load(g, 0).wait()
                load(g, 1).wait()

            step_x(g, 8 * half, 8)

            @pl.when(half == 1)
            def _():
                for k in range(2):
                    for j in range(3):
                        send_row(2 * g + k, j).start()

                @pl.when(g + RING < GROUPS)
                def _():
                    load(g + RING, 0).start()
                    load(g + RING, 1).start()

        @pl.when(t >= LAG)
        def _():
            u = t - LAG
            send_col(u).wait_recv()
            step_z(u)

    @pl.loop(0, UNITS)
    def _(u):
        for j in range(3):
            send_row(u, j).wait_send()
        send_col(u).wait_send()


def put(vr, vi, outr, outi, sem):
    copies = [pltpu.make_async_copy(v.at[pl.ds(8 * i, 8)], o.at[pl.ds(8 * i, 8)], sem.at[4 * k + i])
              for i in range(4) for k, (v, o) in enumerate(((vr, outr), (vi, outi)))]
    for copy in copies:
        copy.start()
    for copy in copies:
        copy.wait()


def solution(mesh):
    f32 = jnp.float32

    def local_forward(u_real, u_imag, g_filter):
        parts = [jnp.transpose(v, (0, 2, 3, 1)).reshape(GROUPS, PACK, 16, 32, 64) for v in (u_real, u_imag)]
        spectrum = pl.pallas_call(
            kernel,
            out_shape=[pltpu.VMEM((32, 16, 32, 64), f32)] * 2,
            in_specs=[pl.BlockSpec(memory_space=pltpu.HBM)] * 5,
            out_specs=[pl.BlockSpec(memory_space=pltpu.VMEM)] * 2,
            scratch_shapes=[
                pltpu.VMEM((RING, PACK, 16, 32, 64), f32),
                pltpu.VMEM((RING, PACK, 16, 32, 64), f32),
                pltpu.VMEM((UNITS * 7, 16, 2, 8, 128), f32),
                pltpu.VMEM((UNITS * 4, 256, 128), f32),
                pltpu.VMEM((UNITS * 2, 256, 128), f32),
                pltpu.VMEM((512, 512), f32),
                pltpu.VMEM((2, 8, 8, 128), f32),
                pltpu.VMEM((16, 32, 64), f32),
                pltpu.VMEM((512, 128), f32),
                pltpu.VMEM((2, 2, 64, 128), f32),
                pltpu.VMEM((8, 8, 2, 8, 128), f32),
                pltpu.VMEM((256, 512), f32),
                pltpu.SemaphoreType.DMA((2 * RING,)),
                pltpu.SemaphoreType.DMA((4,)),
                pltpu.SemaphoreType.DMA((3 * UNITS,)),
                pltpu.SemaphoreType.DMA((3 * UNITS,)),
                pltpu.SemaphoreType.DMA((UNITS,)),
                pltpu.SemaphoreType.DMA((UNITS,)),
            ],
            compiler_params=pltpu.CompilerParams(
                collective_id=0, has_side_effects=True, vmem_limit_bytes=40 * 1024 * 1024),
            name="dft3",
        )(*parts, g_filter, jnp.asarray(lane_matrix()), jnp.asarray(sublane_twiddle()))
        return pl.pallas_call(
            put,
            out_shape=[jax.ShapeDtypeStruct((32, 16, 32, 64), f32)] * 2,
            in_specs=[pl.BlockSpec(memory_space=pltpu.VMEM)] * 2,
            out_specs=[pl.BlockSpec(memory_space=pltpu.HBM)] * 2,
            scratch_shapes=[pltpu.SemaphoreType.DMA((8,))],
            compiler_params=pltpu.CompilerParams(vmem_limit_bytes=4 * 1024 * 1024),
            name="put",
        )(*spectrum)

    field_spec = P("fld", None, "row", "col")
    out_spec = P("fld", "row", "col", None)
    return jax.shard_map(local_forward, mesh=mesh, in_specs=(field_spec, field_spec, P("row", "col", None)),
                         out_specs=(out_spec, out_spec), check_vma=False)
```

```python
import functools
import math

import jax
import jax.numpy as jnp
import numpy as np
from jax import lax
from jax.experimental import pallas as pl
from jax.experimental.pallas import tpu as pltpu
from jax.sharding import PartitionSpec as P

MESH = pl.DeviceIdType.MESH
HALF = math.sqrt(0.5)
GROUPS, PACK, UNITS, LAG, RING = 8, 4, 16, 2, 4


def dft4(b):
    (r0, i0), (r1, i1), (r2, i2), (r3, i3) = b
    sr0, si0, sr1, si1 = r0 + r2, i0 + i2, r0 - r2, i0 - i2
    sr2, si2, sr3, si3 = r1 + r3, i1 + i3, r1 - r3, i1 - i3
    return [(sr0 + sr2, si0 + si2), (sr1 + si3, si1 - sr3), (sr0 - sr2, si0 - si2), (sr1 - si3, si1 + sr3)]


def dft8(a):
    even = [(a[j][0] + a[j + 4][0], a[j][1] + a[j + 4][1]) for j in range(4)]
    odd = [(a[j][0] - a[j + 4][0], a[j][1] - a[j + 4][1]) for j in range(4)]
    (r1, i1), (r2, i2), (r3, i3) = odd[1:]
    odd = [odd[0], ((r1 + i1) * HALF, (i1 - r1) * HALF), (i2, -r2), ((i3 - r3) * HALF, (r3 + i3) * -HALF)]
    even, odd = dft4(even), dft4(odd)
    return [(even if k % 2 == 0 else odd)[k // 2] for k in range(8)]


def times(a, tr, ti):
    return a[0] * tr - a[1] * ti, a[0] * ti + a[1] * tr


def twiddle(m):
    angle = -2.0 * math.pi * (m % 64) / 64.0
    return math.cos(angle) / 8.0, math.sin(angle) / 8.0


def lane_matrix():
    z, kz = np.arange(64), np.arange(64)
    angle = 2.0 * np.pi * ((z[:, None] * kz[None, :]) % 64) / 64.0
    cos, sin = np.cos(angle) / 8.0, np.sin(angle) / 8.0
    blocks = np.stack([np.concatenate([cos, -sin], 1), np.concatenate([sin, cos], 1)])
    out = np.zeros((2, 2, PACK, 32, PACK, 128))
    for c in range(2):
        for f in range(PACK):
            out[c, :, f, :, f, :] = blocks[:, 32 * c : 32 * c + 32]
    return out.reshape(2, 256, PACK * 128).astype(np.float32)


def sublane_twiddle():
    k1, x2 = np.arange(8), np.arange(8)
    angle = -2.0 * np.pi * (k1[:, None] * x2[None, :]) / 64.0
    both = np.stack([np.cos(angle), np.sin(angle)]) / 8.0
    return np.broadcast_to(both[..., None], (2, 8, 8, 128)).astype(np.float32)


def lane_product(lhs, mat, gain, outr, outi, at):
    for n in range(2):
        w = jnp.dot(lhs[...], mat[:, 256 * n : 256 * n + 256], precision=lax.Precision.HIGHEST,
                    preferred_element_type=jnp.float32)
        for f in range(2):
            pair = w[:, 128 * f : 128 * f + 128] * gain
            outr[at(2 * n + f)] = pair[:, :64].reshape(8, 32, 64)
            outi[at(2 * n + f)] = pair[:, 64:].reshape(8, 32, 64)


def kernel(ur, ui, gf, wz, tw, outr, outi, wv, last, gv, inr, ini, xbuf, b2, r2, tv, gs, asc, bsc, lsc,
           in_sem, q_sem, c_sem, s1, d1, s2, d2):
    row, col = lax.axis_index("row"), lax.axis_index("col")
    core = lax.rem(row, 2)
    dests = [2 - core, 3 - core, 1 + 2 * core]
    other = 1 - col

    barrier = pltpu.get_barrier_semaphore()
    for p in (1, 2, 3):
        pl.semaphore_signal(barrier, inc=1, device_id={"row": lax.rem(row + p, 4)}, device_id_type=MESH)
    pl.semaphore_signal(barrier, inc=1, device_id={"col": other}, device_id_type=MESH)

    def load(g, k):
        src, dst = ((ur, inr), (ui, ini))[k]
        return pltpu.make_async_copy(src.at[g], dst.at[lax.rem(g, RING)], in_sem.at[2 * lax.rem(g, RING) + k])

    def quarter(i, k):
        src, dst = ((ur, inr), (ui, ini))[k]
        part = (0, slice(None), pl.ds(4 * i, 4))
        return pltpu.make_async_copy(src.at[part], dst.at[part], q_sem.at[2 * i + k])

    consts = [
        pltpu.make_async_copy(tw, tv, c_sem.at[0]),
        pltpu.make_async_copy(wz.at[col], wv.at[pl.ds(0, 256)], c_sem.at[1]),
        pltpu.make_async_copy(wz.at[other], wv.at[pl.ds(256, 256)], c_sem.at[2]),
        pltpu.make_async_copy(gf, gs, c_sem.at[3]),
    ]
    for i in range(4):
        quarter(i, 0).start()
        quarter(i, 1).start()
        if i == 0:
            consts[0].start()

    def step_x(g, first, count):
        ring = lax.rem(g, RING)
        slots = [3 + lax.rem(k + 4 - row, 4) for k in range(4)]
        bases = [[(2 * g + t) * 7 + slots[k] for t in range(2)] for k in range(4)]

        def one(y, s):
            ar = inr[ring, :, y].reshape(PACK * 32, 64).T
            ai = ini[ring, :, y].reshape(PACK * 32, 64).T
            a = dft8([(ar[8 * j : 8 * j + 8], ai[8 * j : 8 * j + 8]) for j in range(8)])
            for k1 in range(8):
                vr, vi = times(a[k1], tv[0, k1], tv[1, k1])
                asc[s, 0, pl.ds(8 * k1, 8), :] = vr
                asc[s, 1, pl.ds(8 * k1, 8), :] = vi
            b = dft8([tuple(asc[s, q, pl.ds(x2, 8, stride=8), :] for q in range(2)) for x2 in range(8)])
            for k2 in range(8):
                for q in range(2):
                    xbuf[bases[k2 // 2][k2 % 2], y, q] = b[k2][q]

        @pl.loop(0, count // 2)
        def _(i):
            one(first + 2 * i, 0)
            one(first + 2 * i + 1, 1)

    def send_row(u, j, first=0, count=16):
        p = dests[j]
        return pltpu.make_async_remote_copy(
            src_ref=xbuf.at[u * 7 + 3 + p, pl.ds(first, count)], dst_ref=xbuf.at[u * 7 + 3 - p, pl.ds(first, count)],
            send_sem=s1.at[u * 3 + j], recv_sem=d1.at[u * 3 + 3 - p],
            device_id={"row": lax.rem(row + p, 4)}, device_id_type=MESH)

    def wait_row(u, slot):
        part = xbuf.at[u * 7 + slot]
        pltpu.make_async_remote_copy(
            src_ref=part, dst_ref=part, send_sem=s1.at[u * 3], recv_sem=d1.at[u * 3 + slot],
            device_id={"row": row}, device_id_type=MESH).wait_recv()

    def send_col(u):
        return pltpu.make_async_remote_copy(
            src_ref=b2.at[pl.ds(u * 4 + 2 * other, 2)], dst_ref=r2.at[pl.ds(u * 2, 2)],
            send_sem=s2.at[u], recv_sem=d2.at[u], device_id={"col": other}, device_id_type=MESH)

    def step_y(u):
        slots = [u * 7 + lax.rem(r + 7 - row, 4) for r in range(4)]
        for y2 in range(8):
            a = dft8([tuple(xbuf[slots[y1 // 2], 8 * (y1 % 2) + y2, q] for q in range(2)) for y1 in range(8)])
            for k1 in range(8):
                vr, vi = times(a[k1], *twiddle(k1 * y2))
                bsc[k1, y2, 0] = vr
                bsc[k1, y2, 1] = vi
        for k1 in range(8):
            b = dft8([(bsc[k1, y2, 0], bsc[k1, y2, 1]) for y2 in range(8)])
            for k2 in range(8):
                for q in range(2):
                    b2[u * 4 + 2 * (k2 // 4) + q, pl.ds(8 * (k1 + 8 * (k2 % 4)), 8), :] = b[k2][q]

    def gather_z(u, dst):
        for kx in range(8):
            for q in range(2):
                dst[pl.ds(32 * kx, 32), pl.ds(128 * q, 128)] = b2[u * 4 + 2 * col + q, pl.ds(kx, 32, stride=8), :]
                dst[pl.ds(32 * kx, 32), pl.ds(256 + 128 * q, 128)] = r2[u * 2 + q, pl.ds(kx, 32, stride=8), :]

    def step_z(u):
        gather_z(u, lsc)
        gain = gv[pl.ds(pl.multiple_of(256 * lax.rem(u, 2), 256), 256), :]
        lane_product(lsc, wv, gain, outr, outi, lambda f: (PACK * (u // 2) + f, pl.ds(8 * lax.rem(u, 2), 8)))

    consts[0].wait()
    for i in range(4):
        quarter(i, 0).wait()
        quarter(i, 1).wait()
        step_x(0, 4 * i, 4)
        if i == 0:
            pl.semaphore_wait(barrier, 4)
            send_row(0, 1, 0, 4).start()
        send_row(0, 0, 4 * i, 4).start()
    send_row(0, 1, 4, 12).start()
    send_row(0, 2).start()
    for j in range(3):
        send_row(1, j).start()

    @pl.loop(1, RING)
    def _(g):
        load(g, 0).start()
        load(g, 1).start()

    for copy in consts[1:]:
        copy.start()
    for k in range(2):
        load(RING, k).start()
        load(1, k).wait()
    step_x(1, 0, 16)
    for t in range(2):
        for j in range(3):
            send_row(2 + t, j).start()
    for k in range(2):
        load(RING + 1, k).start()

    for copy in consts[1:]:
        copy.wait()
    gain = gs[...].reshape(512, 64)
    gv[...] = jnp.concatenate([gain, gain], axis=1)

    @pl.loop(0, UNITS + LAG - 1)
    def _(t):
        @pl.when(t < UNITS)
        def _():
            for slot in range(3):
                wait_row(t, slot)
            step_y(t)
            send_col(t).start()

        g = t // 2 + 2

        @pl.when(g < GROUPS)
        def _():
            half = lax.rem(t, 2)

            @pl.when(half == 0)
            def _():
                load(g, 0).wait()
                load(g, 1).wait()

            step_x(g, 8 * half, 8)

            @pl.when(half == 1)
            def _():
                for k in range(2):
                    for j in range(3):
                        send_row(2 * g + k, j).start()

                @pl.when(g + RING < GROUPS)
                def _():
                    load(g + RING, 0).start()
                    load(g + RING, 1).start()

        @pl.when(t >= LAG)
        def _():
            u = t - LAG
            send_col(u).wait_recv()
            step_z(u)

    send_col(UNITS - 1).wait_recv()
    gather_z(UNITS - 1, last)

    @pl.loop(0, UNITS)
    def _(u):
        for j in range(3):
            send_row(u, j).wait_send()
        send_col(u).wait_send()


def put(vr, vi, mat, last, gain, outr, outi, lr, li, sem):
    cuts = [(pl.ds(7 * i, 7), slice(None)) for i in range(4)] + [(pl.ds(28, 4), pl.ds(0, 8))]
    copies = [pltpu.make_async_copy(v.at[cut], o.at[cut], sem.at[2 * i + k])
              for i, cut in enumerate(cuts) for k, (v, o) in enumerate(((vr, outr), (vi, outi)))]
    for copy in copies:
        copy.start()
    lane_product(last, mat, gain[256:, :], lr, li, lambda f: f)
    cut = (pl.ds(28, 4), pl.ds(8, 8))
    tail = [pltpu.make_async_copy(v, o.at[cut], sem.at[10 + k]) for k, (v, o) in enumerate(((lr, outr), (li, outi)))]
    for copy in tail:
        copy.start()
    for copy in copies + tail:
        copy.wait()


def solution(mesh):
    f32 = jnp.float32

    def local_forward(u_real, u_imag, g_filter):
        parts = [jnp.transpose(v, (0, 2, 3, 1)).reshape(GROUPS, PACK, 16, 32, 64) for v in (u_real, u_imag)]
        spectrum = pl.pallas_call(
            kernel,
            out_shape=[pltpu.VMEM((32, 16, 32, 64), f32)] * 2 + [
                pltpu.VMEM((512, 512), f32), pltpu.VMEM((256, 512), f32), pltpu.VMEM((512, 128), f32)],
            in_specs=[pl.BlockSpec(memory_space=pltpu.HBM)] * 5,
            out_specs=[pl.BlockSpec(memory_space=pltpu.VMEM)] * 5,
            scratch_shapes=[
                pltpu.VMEM((RING, PACK, 16, 32, 64), f32),
                pltpu.VMEM((RING, PACK, 16, 32, 64), f32),
                pltpu.VMEM((UNITS * 7, 16, 2, 8, 128), f32),
                pltpu.VMEM((UNITS * 4, 256, 128), f32),
                pltpu.VMEM((UNITS * 2, 256, 128), f32),
                pltpu.VMEM((2, 8, 8, 128), f32),
                pltpu.VMEM((16, 32, 64), f32),
                pltpu.VMEM((2, 2, 64, 128), f32),
                pltpu.VMEM((8, 8, 2, 8, 128), f32),
                pltpu.VMEM((256, 512), f32),
                pltpu.SemaphoreType.DMA((2 * RING,)),
                pltpu.SemaphoreType.DMA((8,)),
                pltpu.SemaphoreType.DMA((4,)),
                pltpu.SemaphoreType.DMA((3 * UNITS,)),
                pltpu.SemaphoreType.DMA((3 * UNITS,)),
                pltpu.SemaphoreType.DMA((UNITS,)),
                pltpu.SemaphoreType.DMA((UNITS,)),
            ],
            compiler_params=pltpu.CompilerParams(
                collective_id=0, has_side_effects=True, vmem_limit_bytes=40 * 1024 * 1024),
            name="dft3",
        )(*parts, g_filter, jnp.asarray(lane_matrix()), jnp.asarray(sublane_twiddle()))
        return pl.pallas_call(
            put,
            out_shape=[jax.ShapeDtypeStruct((32, 16, 32, 64), f32)] * 2,
            in_specs=[pl.BlockSpec(memory_space=pltpu.VMEM)] * 5,
            out_specs=[pl.BlockSpec(memory_space=pltpu.HBM)] * 2,
            scratch_shapes=[pltpu.VMEM((PACK, 8, 32, 64), f32)] * 2 + [pltpu.SemaphoreType.DMA((12,))],
            compiler_params=pltpu.CompilerParams(vmem_limit_bytes=8 * 1024 * 1024),
            name="put",
        )(*spectrum)

    field_spec = P("fld", None, "row", "col")
    out_spec = P("fld", "row", "col", None)
    return jax.shard_map(local_forward, mesh=mesh, in_specs=(field_spec, field_spec, P("row", "col", None)),
                         out_specs=(out_spec, out_spec), check_vma=False)
```

```python
import functools
import math

import jax
import jax.numpy as jnp
import numpy as np
from jax import lax
from jax.experimental import pallas as pl
from jax.experimental.pallas import tpu as pltpu
from jax.sharding import PartitionSpec as P

MESH = pl.DeviceIdType.MESH
HALF = math.sqrt(0.5)
GROUPS, PACK, UNITS, LAG, RING = 8, 4, 16, 2, 4


def dft4(b):
    (r0, i0), (r1, i1), (r2, i2), (r3, i3) = b
    sr0, si0, sr1, si1 = r0 + r2, i0 + i2, r0 - r2, i0 - i2
    sr2, si2, sr3, si3 = r1 + r3, i1 + i3, r1 - r3, i1 - i3
    return [(sr0 + sr2, si0 + si2), (sr1 + si3, si1 - sr3), (sr0 - sr2, si0 - si2), (sr1 - si3, si1 + sr3)]


def dft8(a):
    even = [(a[j][0] + a[j + 4][0], a[j][1] + a[j + 4][1]) for j in range(4)]
    odd = [(a[j][0] - a[j + 4][0], a[j][1] - a[j + 4][1]) for j in range(4)]
    (r1, i1), (r2, i2), (r3, i3) = odd[1:]
    odd = [odd[0], ((r1 + i1) * HALF, (i1 - r1) * HALF), (i2, -r2), ((i3 - r3) * HALF, (r3 + i3) * -HALF)]
    even, odd = dft4(even), dft4(odd)
    return [(even if k % 2 == 0 else odd)[k // 2] for k in range(8)]


def times(a, tr, ti):
    return a[0] * tr - a[1] * ti, a[0] * ti + a[1] * tr


def twiddle(m):
    angle = -2.0 * math.pi * (m % 64) / 64.0
    return math.cos(angle) / 8.0, math.sin(angle) / 8.0


def lane_matrix():
    z, kz = np.arange(64), np.arange(64)
    angle = 2.0 * np.pi * ((z[:, None] * kz[None, :]) % 64) / 64.0
    cos, sin = np.cos(angle) / 8.0, np.sin(angle) / 8.0
    blocks = np.stack([np.concatenate([cos, -sin], 1), np.concatenate([sin, cos], 1)])
    out = np.zeros((2, 2, PACK, 32, PACK, 128))
    for c in range(2):
        for f in range(PACK):
            out[c, :, f, :, f, :] = blocks[:, 32 * c : 32 * c + 32]
    return out.reshape(2, 256, PACK * 128).astype(np.float32)


def sublane_twiddle():
    k1, x2 = np.arange(8), np.arange(8)
    angle = -2.0 * np.pi * (k1[:, None] * x2[None, :]) / 64.0
    both = np.stack([np.cos(angle), np.sin(angle)]) / 8.0
    return np.broadcast_to(both[..., None], (2, 8, 8, 128)).astype(np.float32)


def lane_product(lhs, mat, gain, outr, outi, at):
    for n in range(2):
        w = jnp.dot(lhs[...], mat[:, 256 * n : 256 * n + 256], precision=lax.Precision.HIGHEST,
                    preferred_element_type=jnp.float32)
        for f in range(2):
            pair = w[:, 128 * f : 128 * f + 128] * gain
            outr[at(2 * n + f)] = pair[:, :64].reshape(8, 32, 64)
            outi[at(2 * n + f)] = pair[:, 64:].reshape(8, 32, 64)


def kernel(ur, ui, gf, wz, tw, outr, outi, wv, last, gv, inr, ini, xbuf, b2, r2, tv, gs, asc, bsc, lsc,
           in_sem, q_sem, c_sem, s1, d1, s2, d2):
    row, col = lax.axis_index("row"), lax.axis_index("col")
    core = lax.rem(row, 2)
    dests = [1 + 2 * core, 2 - core, 3 - core]
    other = 1 - col

    barrier = pltpu.get_barrier_semaphore()
    for p in (1, 2, 3):
        pl.semaphore_signal(barrier, inc=1, device_id={"row": lax.rem(row + p, 4)}, device_id_type=MESH)
    pl.semaphore_signal(barrier, inc=1, device_id={"col": other}, device_id_type=MESH)

    def load(g, k):
        src, dst = ((ur, inr), (ui, ini))[k]
        return pltpu.make_async_copy(src.at[g], dst.at[lax.rem(g, RING)], in_sem.at[2 * lax.rem(g, RING) + k])

    def quarter(i, k):
        src, dst = ((ur, inr), (ui, ini))[k]
        part = (0, slice(None), pl.ds(4 * i, 4))
        return pltpu.make_async_copy(src.at[part], dst.at[part], q_sem.at[2 * i + k])

    consts = [
        pltpu.make_async_copy(tw, tv, c_sem.at[0]),
        pltpu.make_async_copy(wz.at[col], wv.at[pl.ds(0, 256)], c_sem.at[1]),
        pltpu.make_async_copy(wz.at[other], wv.at[pl.ds(256, 256)], c_sem.at[2]),
        pltpu.make_async_copy(gf, gs, c_sem.at[3]),
    ]
    for i in range(4):
        quarter(i, 0).start()
        quarter(i, 1).start()
        if i == 0:
            consts[0].start()

    def step_x(g, first, count):
        ring = lax.rem(g, RING)
        slots = [3 + lax.rem(k + 4 - row, 4) for k in range(4)]
        bases = [[(2 * g + t) * 7 + slots[k] for t in range(2)] for k in range(4)]

        def one(y, s):
            ar = inr[ring, :, y].reshape(PACK * 32, 64).T
            ai = ini[ring, :, y].reshape(PACK * 32, 64).T
            a = dft8([(ar[8 * j : 8 * j + 8], ai[8 * j : 8 * j + 8]) for j in range(8)])
            for k1 in range(8):
                vr, vi = times(a[k1], tv[0, k1], tv[1, k1])
                asc[s, 0, pl.ds(8 * k1, 8), :] = vr
                asc[s, 1, pl.ds(8 * k1, 8), :] = vi
            b = dft8([tuple(asc[s, q, pl.ds(x2, 8, stride=8), :] for q in range(2)) for x2 in range(8)])
            for k2 in range(8):
                for q in range(2):
                    xbuf[bases[k2 // 2][k2 % 2], y, q] = b[k2][q]

        @pl.loop(0, count // 2)
        def _(i):
            one(first + 2 * i, 0)
            one(first + 2 * i + 1, 1)

    def send_row(u, j, first=0, count=16):
        p = dests[j]
        return pltpu.make_async_remote_copy(
            src_ref=xbuf.at[u * 7 + 3 + p, pl.ds(first, count)], dst_ref=xbuf.at[u * 7 + 3 - p, pl.ds(first, count)],
            send_sem=s1.at[u * 3 + j], recv_sem=d1.at[u * 3 + 3 - p],
            device_id={"row": lax.rem(row + p, 4)}, device_id_type=MESH)

    def wait_row(u, slot):
        part = xbuf.at[u * 7 + slot]
        pltpu.make_async_remote_copy(
            src_ref=part, dst_ref=part, send_sem=s1.at[u * 3], recv_sem=d1.at[u * 3 + slot],
            device_id={"row": row}, device_id_type=MESH).wait_recv()

    def send_col(u):
        return pltpu.make_async_remote_copy(
            src_ref=b2.at[pl.ds(u * 4 + 2 * other, 2)], dst_ref=r2.at[pl.ds(u * 2, 2)],
            send_sem=s2.at[u], recv_sem=d2.at[u], device_id={"col": other}, device_id_type=MESH)

    def step_y(u):
        slots = [u * 7 + lax.rem(r + 7 - row, 4) for r in range(4)]
        for y2 in range(8):
            a = dft8([tuple(xbuf[slots[y1 // 2], 8 * (y1 % 2) + y2, q] for q in range(2)) for y1 in range(8)])
            for k1 in range(8):
                vr, vi = times(a[k1], *twiddle(k1 * y2))
                bsc[k1, y2, 0] = vr
                bsc[k1, y2, 1] = vi
        for k1 in range(8):
            b = dft8([(bsc[k1, y2, 0], bsc[k1, y2, 1]) for y2 in range(8)])
            for k2 in range(8):
                for q in range(2):
                    b2[u * 4 + 2 * (k2 // 4) + q, pl.ds(8 * (k1 + 8 * (k2 % 4)), 8), :] = b[k2][q]

    def gather_z(u, dst):
        for kx in range(8):
            for q in range(2):
                dst[pl.ds(32 * kx, 32), pl.ds(128 * q, 128)] = b2[u * 4 + 2 * col + q, pl.ds(kx, 32, stride=8), :]
                dst[pl.ds(32 * kx, 32), pl.ds(256 + 128 * q, 128)] = r2[u * 2 + q, pl.ds(kx, 32, stride=8), :]

    def step_z(u):
        gather_z(u, lsc)
        gain = gv[pl.ds(pl.multiple_of(256 * lax.rem(u, 2), 256), 256), :]
        lane_product(lsc, wv, gain, outr, outi, lambda f: (PACK * (u // 2) + f, pl.ds(8 * lax.rem(u, 2), 8)))

    consts[0].wait()
    for i in range(4):
        quarter(i, 0).wait()
        quarter(i, 1).wait()
        step_x(0, 4 * i, 4)
        if i == 0:
            pl.semaphore_wait(barrier, 4)
            send_row(0, 2, 0, 4).start()
        send_row(0, 1, 4 * i, 4).start()
    send_row(0, 0).start()
    send_row(0, 2, 4, 12).start()
    for j in range(3):
        send_row(1, j).start()

    @pl.loop(1, RING)
    def _(g):
        load(g, 0).start()
        load(g, 1).start()

    for copy in consts[1:]:
        copy.start()
    for k in range(2):
        load(RING, k).start()
        load(1, k).wait()
    step_x(1, 0, 16)
    for t in range(2):
        for j in range(3):
            send_row(2 + t, j).start()
    for k in range(2):
        load(RING + 1, k).start()

    for copy in consts[1:]:
        copy.wait()
    gain = gs[...].reshape(512, 64)
    gv[...] = jnp.concatenate([gain, gain], axis=1)

    @pl.loop(0, UNITS + LAG - 1)
    def _(t):
        @pl.when(t < UNITS)
        def _():
            for slot in range(3):
                wait_row(t, slot)
            step_y(t)
            send_col(t).start()

        g = t // 2 + 2

        @pl.when(g < GROUPS)
        def _():
            half = lax.rem(t, 2)

            @pl.when(half == 0)
            def _():
                load(g, 0).wait()
                load(g, 1).wait()

            step_x(g, 8 * half, 8)

            @pl.when(half == 1)
            def _():
                for k in range(2):
                    for j in range(3):
                        send_row(2 * g + k, j).start()

                @pl.when(g + RING < GROUPS)
                def _():
                    load(g + RING, 0).start()
                    load(g + RING, 1).start()

        @pl.when(t >= LAG)
        def _():
            u = t - LAG
            send_col(u).wait_recv()
            step_z(u)

    @pl.loop(0, UNITS)
    def _(u):
        for j in range(3):
            send_row(u, j).wait_send()

    @pl.loop(0, UNITS - 1)
    def _(u):
        send_col(u).wait_send()

    send_col(UNITS - 1).wait_recv()
    gather_z(UNITS - 1, last)
    send_col(UNITS - 1).wait_send()


def put(vr, vi, mat, last, gain, outr, outi, lr, li, sem):
    cuts = [(pl.ds(7 * i, 7), slice(None)) for i in range(4)] + [(pl.ds(28, 4), pl.ds(0, 8))]
    copies = [pltpu.make_async_copy(v.at[cut], o.at[cut], sem.at[2 * i + k])
              for i, cut in enumerate(cuts) for k, (v, o) in enumerate(((vr, outr), (vi, outi)))]
    for copy in copies:
        copy.start()
    lane_product(last, mat, gain[256:, :], lr, li, lambda f: f)
    cut = (pl.ds(28, 4), pl.ds(8, 8))
    tail = [pltpu.make_async_copy(v, o.at[cut], sem.at[10 + k]) for k, (v, o) in enumerate(((lr, outr), (li, outi)))]
    for copy in tail:
        copy.start()
    for copy in copies + tail:
        copy.wait()


def solution(mesh):
    f32 = jnp.float32

    def local_forward(u_real, u_imag, g_filter):
        parts = [jnp.transpose(v, (0, 2, 3, 1)).reshape(GROUPS, PACK, 16, 32, 64) for v in (u_real, u_imag)]
        spectrum = pl.pallas_call(
            kernel,
            out_shape=[pltpu.VMEM((32, 16, 32, 64), f32)] * 2 + [
                pltpu.VMEM((512, 512), f32), pltpu.VMEM((256, 512), f32), pltpu.VMEM((512, 128), f32)],
            in_specs=[pl.BlockSpec(memory_space=pltpu.HBM)] * 5,
            out_specs=[pl.BlockSpec(memory_space=pltpu.VMEM)] * 5,
            scratch_shapes=[
                pltpu.VMEM((RING, PACK, 16, 32, 64), f32),
                pltpu.VMEM((RING, PACK, 16, 32, 64), f32),
                pltpu.VMEM((UNITS * 7, 16, 2, 8, 128), f32),
                pltpu.VMEM((UNITS * 4, 256, 128), f32),
                pltpu.VMEM((UNITS * 2, 256, 128), f32),
                pltpu.VMEM((2, 8, 8, 128), f32),
                pltpu.VMEM((16, 32, 64), f32),
                pltpu.VMEM((2, 2, 64, 128), f32),
                pltpu.VMEM((8, 8, 2, 8, 128), f32),
                pltpu.VMEM((256, 512), f32),
                pltpu.SemaphoreType.DMA((2 * RING,)),
                pltpu.SemaphoreType.DMA((8,)),
                pltpu.SemaphoreType.DMA((4,)),
                pltpu.SemaphoreType.DMA((3 * UNITS,)),
                pltpu.SemaphoreType.DMA((3 * UNITS,)),
                pltpu.SemaphoreType.DMA((UNITS,)),
                pltpu.SemaphoreType.DMA((UNITS,)),
            ],
            compiler_params=pltpu.CompilerParams(
                collective_id=0, has_side_effects=True, vmem_limit_bytes=40 * 1024 * 1024),
            name="dft3",
        )(*parts, g_filter, jnp.asarray(lane_matrix()), jnp.asarray(sublane_twiddle()))
        return pl.pallas_call(
            put,
            out_shape=[jax.ShapeDtypeStruct((32, 16, 32, 64), f32)] * 2,
            in_specs=[pl.BlockSpec(memory_space=pltpu.VMEM)] * 5,
            out_specs=[pl.BlockSpec(memory_space=pltpu.HBM)] * 2,
            scratch_shapes=[pltpu.VMEM((PACK, 8, 32, 64), f32)] * 2 + [pltpu.SemaphoreType.DMA((12,))],
            compiler_params=pltpu.CompilerParams(vmem_limit_bytes=8 * 1024 * 1024),
            name="put",
        )(*spectrum)

    field_spec = P("fld", None, "row", "col")
    out_spec = P("fld", "row", "col", None)
    return jax.shard_map(local_forward, mesh=mesh, in_specs=(field_spec, field_spec, P("row", "col", None)),
                         out_specs=(out_spec, out_spec), check_vma=False)
```

```python
import functools
import math

import jax
import jax.numpy as jnp
import numpy as np
from jax import lax
from jax.experimental import pallas as pl
from jax.experimental.pallas import tpu as pltpu
from jax.sharding import PartitionSpec as P

MESH = pl.DeviceIdType.MESH
HALF = math.sqrt(0.5)
GROUPS, PACK, UNITS, LAG, RING = 8, 4, 16, 2, 4


def dft4(b):
    (r0, i0), (r1, i1), (r2, i2), (r3, i3) = b
    sr0, si0, sr1, si1 = r0 + r2, i0 + i2, r0 - r2, i0 - i2
    sr2, si2, sr3, si3 = r1 + r3, i1 + i3, r1 - r3, i1 - i3
    return [(sr0 + sr2, si0 + si2), (sr1 + si3, si1 - sr3), (sr0 - sr2, si0 - si2), (sr1 - si3, si1 + sr3)]


def dft8(a):
    even = [(a[j][0] + a[j + 4][0], a[j][1] + a[j + 4][1]) for j in range(4)]
    odd = [(a[j][0] - a[j + 4][0], a[j][1] - a[j + 4][1]) for j in range(4)]
    (r1, i1), (r2, i2), (r3, i3) = odd[1:]
    odd = [odd[0], ((r1 + i1) * HALF, (i1 - r1) * HALF), (i2, -r2), ((i3 - r3) * HALF, (r3 + i3) * -HALF)]
    even, odd = dft4(even), dft4(odd)
    return [(even if k % 2 == 0 else odd)[k // 2] for k in range(8)]


def times(a, tr, ti):
    return a[0] * tr - a[1] * ti, a[0] * ti + a[1] * tr


def twiddle(m):
    angle = -2.0 * math.pi * (m % 64) / 64.0
    return math.cos(angle) / 8.0, math.sin(angle) / 8.0


def lane_matrix():
    z, kz = np.arange(64), np.arange(64)
    angle = 2.0 * np.pi * ((z[:, None] * kz[None, :]) % 64) / 64.0
    cos, sin = np.cos(angle) / 8.0, np.sin(angle) / 8.0
    blocks = np.stack([np.concatenate([cos, -sin], 1), np.concatenate([sin, cos], 1)])
    out = np.zeros((2, 2, PACK, 32, PACK, 128))
    for c in range(2):
        for f in range(PACK):
            out[c, :, f, :, f, :] = blocks[:, 32 * c : 32 * c + 32]
    return out.reshape(2, 256, PACK * 128).astype(np.float32)


def sublane_twiddle():
    k1, x2 = np.arange(8), np.arange(8)
    angle = -2.0 * np.pi * (k1[:, None] * x2[None, :]) / 64.0
    both = np.stack([np.cos(angle), np.sin(angle)]) / 8.0
    return np.broadcast_to(both[..., None], (2, 8, 8, 128)).astype(np.float32)


def lane_product(lhs, mat, gain, outr, outi, at):
    for n in range(2):
        w = jnp.dot(lhs[...], mat[:, 256 * n : 256 * n + 256], precision=lax.Precision.HIGHEST,
                    preferred_element_type=jnp.float32)
        for f in range(2):
            pair = w[:, 128 * f : 128 * f + 128] * gain
            outr[at(2 * n + f)] = pair[:, :64].reshape(8, 32, 64)
            outi[at(2 * n + f)] = pair[:, 64:].reshape(8, 32, 64)


def kernel(ur, ui, gf, wz, tw, outr, outi, wv, last, gv, inr, ini, xbuf, b2, r2, tv, gs, asc, bsc, lsc,
           in_sem, q_sem, c_sem, s1, d1, s2, d2):
    row, col = lax.axis_index("row"), lax.axis_index("col")
    core = lax.rem(row, 2)
    dests = [1 + 2 * core, 2 - core, 3 - core]
    other = 1 - col

    barrier = pltpu.get_barrier_semaphore()
    for p in (1, 2, 3):
        pl.semaphore_signal(barrier, inc=1, device_id={"row": lax.rem(row + p, 4)}, device_id_type=MESH)
    pl.semaphore_signal(barrier, inc=1, device_id={"col": other}, device_id_type=MESH)

    def load(g, k):
        src, dst = ((ur, inr), (ui, ini))[k]
        return pltpu.make_async_copy(src.at[g], dst.at[lax.rem(g, RING)], in_sem.at[2 * lax.rem(g, RING) + k])

    def quarter(i, k):
        src, dst = ((ur, inr), (ui, ini))[k]
        part = (0, slice(None), pl.ds(4 * i, 4))
        return pltpu.make_async_copy(src.at[part], dst.at[part], q_sem.at[2 * i + k])

    consts = [
        pltpu.make_async_copy(tw, tv, c_sem.at[0]),
        pltpu.make_async_copy(wz.at[col], wv.at[pl.ds(0, 256)], c_sem.at[1]),
        pltpu.make_async_copy(wz.at[other], wv.at[pl.ds(256, 256)], c_sem.at[2]),
        pltpu.make_async_copy(gf, gs, c_sem.at[3]),
    ]
    for i in range(4):
        quarter(i, 0).start()
        quarter(i, 1).start()
        if i == 0:
            consts[0].start()

    def step_x(g, first, count):
        ring = lax.rem(g, RING)
        slots = [3 + lax.rem(k + 4 - row, 4) for k in range(4)]
        bases = [[(2 * g + t) * 7 + slots[k] for t in range(2)] for k in range(4)]

        def one(y, s):
            ar = inr[ring, :, y].reshape(PACK * 32, 64).T
            ai = ini[ring, :, y].reshape(PACK * 32, 64).T
            a = dft8([(ar[8 * j : 8 * j + 8], ai[8 * j : 8 * j + 8]) for j in range(8)])
            for k1 in range(8):
                vr, vi = times(a[k1], tv[0, k1], tv[1, k1])
                asc[s, 0, pl.ds(8 * k1, 8), :] = vr
                asc[s, 1, pl.ds(8 * k1, 8), :] = vi
            b = dft8([tuple(asc[s, q, pl.ds(x2, 8, stride=8), :] for q in range(2)) for x2 in range(8)])
            for k2 in range(8):
                for q in range(2):
                    xbuf[bases[k2 // 2][k2 % 2], y, q] = b[k2][q]

        @pl.loop(0, count // 2)
        def _(i):
            one(first + 2 * i, 0)
            one(first + 2 * i + 1, 1)

    def send_row(u, j, first=0, count=16):
        p = dests[j]
        return pltpu.make_async_remote_copy(
            src_ref=xbuf.at[u * 7 + 3 + p, pl.ds(first, count)], dst_ref=xbuf.at[u * 7 + 3 - p, pl.ds(first, count)],
            send_sem=s1.at[u * 3 + j], recv_sem=d1.at[u * 3 + 3 - p],
            device_id={"row": lax.rem(row + p, 4)}, device_id_type=MESH)

    def wait_row(u, slot):
        part = xbuf.at[u * 7 + slot]
        pltpu.make_async_remote_copy(
            src_ref=part, dst_ref=part, send_sem=s1.at[u * 3], recv_sem=d1.at[u * 3 + slot],
            device_id={"row": row}, device_id_type=MESH).wait_recv()

    def send_col(u):
        return pltpu.make_async_remote_copy(
            src_ref=b2.at[pl.ds(u * 4 + 2 * other, 2)], dst_ref=r2.at[pl.ds(u * 2, 2)],
            send_sem=s2.at[u], recv_sem=d2.at[u], device_id={"col": other}, device_id_type=MESH)

    def step_y(u):
        slots = [u * 7 + lax.rem(r + 7 - row, 4) for r in range(4)]
        for y2 in range(8):
            a = dft8([tuple(xbuf[slots[y1 // 2], 8 * (y1 % 2) + y2, q] for q in range(2)) for y1 in range(8)])
            for k1 in range(8):
                vr, vi = times(a[k1], *twiddle(k1 * y2))
                bsc[k1, y2, 0] = vr
                bsc[k1, y2, 1] = vi
        for k1 in range(8):
            b = dft8([(bsc[k1, y2, 0], bsc[k1, y2, 1]) for y2 in range(8)])
            for k2 in range(8):
                for q in range(2):
                    b2[u * 4 + 2 * (k2 // 4) + q, pl.ds(8 * (k1 + 8 * (k2 % 4)), 8), :] = b[k2][q]

    def gather_z(u, dst):
        for kx in range(8):
            for q in range(2):
                dst[pl.ds(32 * kx, 32), pl.ds(128 * q, 128)] = b2[u * 4 + 2 * col + q, pl.ds(kx, 32, stride=8), :]
                dst[pl.ds(32 * kx, 32), pl.ds(256 + 128 * q, 128)] = r2[u * 2 + q, pl.ds(kx, 32, stride=8), :]

    def step_z(u):
        gather_z(u, lsc)
        gain = gv[pl.ds(pl.multiple_of(256 * lax.rem(u, 2), 256), 256), :]
        lane_product(lsc, wv, gain, outr, outi, lambda f: (PACK * (u // 2) + f, pl.ds(8 * lax.rem(u, 2), 8)))

    consts[0].wait()
    for i in range(4):
        quarter(i, 0).wait()
        quarter(i, 1).wait()
        step_x(0, 4 * i, 4)
        if i == 0:
            pl.semaphore_wait(barrier, 4)
            send_row(0, 2, 0, 4).start()
        send_row(0, 1, 4 * i, 4).start()
    send_row(0, 0).start()
    send_row(0, 2, 4, 12).start()

    @pl.loop(1, RING)
    def _(g):
        load(g, 0).start()
        load(g, 1).start()

    for copy in consts[1:]:
        copy.start()
    for k in range(2):
        load(RING, k).start()
        load(1, k).wait()
    for j in range(3):
        send_row(1, j).start()
    step_x(1, 0, 16)
    for k in range(2):
        load(RING + 1, k).start()

    for copy in consts[1:]:
        copy.wait()
    gain = gs[...].reshape(512, 64)
    gv[...] = jnp.concatenate([gain, gain], axis=1)

    @pl.loop(0, UNITS + LAG - 1)
    def _(t):
        @pl.when(t < UNITS)
        def _():
            for slot in range(3):
                wait_row(t, slot)
            step_y(t)
            send_col(t).start()

            @pl.when(t < UNITS - 2)
            def _():
                for j in range(3):
                    send_row(t + 2, j).start()

        g = t // 2 + 2

        @pl.when(g < GROUPS)
        def _():
            half = lax.rem(t, 2)

            @pl.when(half == 0)
            def _():
                load(g, 0).wait()
                load(g, 1).wait()

            step_x(g, 8 * half, 8)

            @pl.when(half == 1)
            def _():
                @pl.when(g + RING < GROUPS)
                def _():
                    load(g + RING, 0).start()
                    load(g + RING, 1).start()

        @pl.when(t >= LAG)
        def _():
            u = t - LAG
            send_col(u).wait_recv()
            step_z(u)

    @pl.loop(0, UNITS)
    def _(u):
        for j in range(3):
            send_row(u, j).wait_send()

    @pl.loop(0, UNITS - 1)
    def _(u):
        send_col(u).wait_send()

    send_col(UNITS - 1).wait_recv()
    gather_z(UNITS - 1, last)
    send_col(UNITS - 1).wait_send()


def put(vr, vi, mat, last, gain, outr, outi, lr, li, sem):
    cuts = [(pl.ds(7 * i, 7), slice(None)) for i in range(4)] + [(pl.ds(28, 4), pl.ds(0, 8))]
    copies = [pltpu.make_async_copy(v.at[cut], o.at[cut], sem.at[2 * i + k])
              for i, cut in enumerate(cuts) for k, (v, o) in enumerate(((vr, outr), (vi, outi)))]
    for copy in copies:
        copy.start()
    lane_product(last, mat, gain[256:, :], lr, li, lambda f: f)
    cut = (pl.ds(28, 4), pl.ds(8, 8))
    tail = [pltpu.make_async_copy(v, o.at[cut], sem.at[10 + k]) for k, (v, o) in enumerate(((lr, outr), (li, outi)))]
    for copy in tail:
        copy.start()
    for copy in copies + tail:
        copy.wait()


def solution(mesh):
    f32 = jnp.float32

    def local_forward(u_real, u_imag, g_filter):
        parts = [jnp.transpose(v, (0, 2, 3, 1)).reshape(GROUPS, PACK, 16, 32, 64) for v in (u_real, u_imag)]
        spectrum = pl.pallas_call(
            kernel,
            out_shape=[pltpu.VMEM((32, 16, 32, 64), f32)] * 2 + [
                pltpu.VMEM((512, 512), f32), pltpu.VMEM((256, 512), f32), pltpu.VMEM((512, 128), f32)],
            in_specs=[pl.BlockSpec(memory_space=pltpu.HBM)] * 5,
            out_specs=[pl.BlockSpec(memory_space=pltpu.VMEM)] * 5,
            scratch_shapes=[
                pltpu.VMEM((RING, PACK, 16, 32, 64), f32),
                pltpu.VMEM((RING, PACK, 16, 32, 64), f32),
                pltpu.VMEM((UNITS * 7, 16, 2, 8, 128), f32),
                pltpu.VMEM((UNITS * 4, 256, 128), f32),
                pltpu.VMEM((UNITS * 2, 256, 128), f32),
                pltpu.VMEM((2, 8, 8, 128), f32),
                pltpu.VMEM((16, 32, 64), f32),
                pltpu.VMEM((2, 2, 64, 128), f32),
                pltpu.VMEM((8, 8, 2, 8, 128), f32),
                pltpu.VMEM((256, 512), f32),
                pltpu.SemaphoreType.DMA((2 * RING,)),
                pltpu.SemaphoreType.DMA((8,)),
                pltpu.SemaphoreType.DMA((4,)),
                pltpu.SemaphoreType.DMA((3 * UNITS,)),
                pltpu.SemaphoreType.DMA((3 * UNITS,)),
                pltpu.SemaphoreType.DMA((UNITS,)),
                pltpu.SemaphoreType.DMA((UNITS,)),
            ],
            compiler_params=pltpu.CompilerParams(
                collective_id=0, has_side_effects=True, vmem_limit_bytes=40 * 1024 * 1024),
            name="dft3",
        )(*parts, g_filter, jnp.asarray(lane_matrix()), jnp.asarray(sublane_twiddle()))
        return pl.pallas_call(
            put,
            out_shape=[jax.ShapeDtypeStruct((32, 16, 32, 64), f32)] * 2,
            in_specs=[pl.BlockSpec(memory_space=pltpu.VMEM)] * 5,
            out_specs=[pl.BlockSpec(memory_space=pltpu.HBM)] * 2,
            scratch_shapes=[pltpu.VMEM((PACK, 8, 32, 64), f32)] * 2 + [pltpu.SemaphoreType.DMA((12,))],
            compiler_params=pltpu.CompilerParams(vmem_limit_bytes=8 * 1024 * 1024),
            name="put",
        )(*spectrum)

    field_spec = P("fld", None, "row", "col")
    out_spec = P("fld", "row", "col", None)
    return jax.shard_map(local_forward, mesh=mesh, in_specs=(field_spec, field_spec, P("row", "col", None)),
                         out_specs=(out_spec, out_spec), check_vma=False)
```

```python
import functools
import math

import jax
import jax.numpy as jnp
import numpy as np
from jax import lax
from jax.experimental import pallas as pl
from jax.experimental.pallas import tpu as pltpu
from jax.sharding import PartitionSpec as P

MESH = pl.DeviceIdType.MESH
HALF = math.sqrt(0.5)
GROUPS, PACK, UNITS, LAG, RING = 8, 4, 16, 2, 4


def dft4(b):
    (r0, i0), (r1, i1), (r2, i2), (r3, i3) = b
    sr0, si0, sr1, si1 = r0 + r2, i0 + i2, r0 - r2, i0 - i2
    sr2, si2, sr3, si3 = r1 + r3, i1 + i3, r1 - r3, i1 - i3
    return [(sr0 + sr2, si0 + si2), (sr1 + si3, si1 - sr3), (sr0 - sr2, si0 - si2), (sr1 - si3, si1 + sr3)]


def dft8(a):
    even = [(a[j][0] + a[j + 4][0], a[j][1] + a[j + 4][1]) for j in range(4)]
    odd = [(a[j][0] - a[j + 4][0], a[j][1] - a[j + 4][1]) for j in range(4)]
    (r1, i1), (r2, i2), (r3, i3) = odd[1:]
    odd = [odd[0], ((r1 + i1) * HALF, (i1 - r1) * HALF), (i2, -r2), ((i3 - r3) * HALF, (r3 + i3) * -HALF)]
    even, odd = dft4(even), dft4(odd)
    return [(even if k % 2 == 0 else odd)[k // 2] for k in range(8)]


def times(a, tr, ti):
    return a[0] * tr - a[1] * ti, a[0] * ti + a[1] * tr


def twiddle(m):
    angle = -2.0 * math.pi * (m % 64) / 64.0
    return math.cos(angle) / 8.0, math.sin(angle) / 8.0


def lane_matrix():
    z, kz = np.arange(64), np.arange(64)
    angle = 2.0 * np.pi * ((z[:, None] * kz[None, :]) % 64) / 64.0
    cos, sin = np.cos(angle) / 8.0, np.sin(angle) / 8.0
    blocks = np.stack([np.concatenate([cos, -sin], 1), np.concatenate([sin, cos], 1)])
    out = np.zeros((2, 2, PACK, 32, PACK, 128))
    for c in range(2):
        for f in range(PACK):
            out[c, :, f, :, f, :] = blocks[:, 32 * c : 32 * c + 32]
    return out.reshape(2, 256, PACK * 128).astype(np.float32)


def sublane_twiddle():
    k1, x2 = np.arange(8), np.arange(8)
    angle = -2.0 * np.pi * (k1[:, None] * x2[None, :]) / 64.0
    both = np.stack([np.cos(angle), np.sin(angle)]) / 8.0
    return np.broadcast_to(both[..., None], (2, 8, 8, 128)).astype(np.float32)


def lane_product(lhs, mat, gain, outr, outi, at):
    for n in range(2):
        w = jnp.dot(lhs[...], mat[:, 256 * n : 256 * n + 256], precision=lax.Precision.HIGHEST,
                    preferred_element_type=jnp.float32)
        for f in range(2):
            pair = w[:, 128 * f : 128 * f + 128] * gain
            outr[at(2 * n + f)] = pair[:, :64].reshape(8, 32, 64)
            outi[at(2 * n + f)] = pair[:, 64:].reshape(8, 32, 64)


def kernel(ur, ui, gf, wz, tw, outr, outi, wv, last, gv, inr, ini, xbuf, b2, r2, tv, gs, asc, bsc, lsc,
           in_sem, q_sem, c_sem, s1, d1, s2, d2):
    row, col = lax.axis_index("row"), lax.axis_index("col")
    core = lax.rem(row, 2)
    dests = [1 + 2 * core, 2 - core, 3 - core]
    other = 1 - col

    barrier = pltpu.get_barrier_semaphore()
    for p in (1, 2, 3):
        pl.semaphore_signal(barrier, inc=1, device_id={"row": lax.rem(row + p, 4)}, device_id_type=MESH)
    pl.semaphore_signal(barrier, inc=1, device_id={"col": other}, device_id_type=MESH)

    def load(g, k):
        src, dst = ((ur, inr), (ui, ini))[k]
        return pltpu.make_async_copy(src.at[g], dst.at[lax.rem(g, RING)], in_sem.at[2 * lax.rem(g, RING) + k])

    def quarter(i, k):
        src, dst = ((ur, inr), (ui, ini))[k]
        part = (0, slice(None), pl.ds(4 * i, 4))
        return pltpu.make_async_copy(src.at[part], dst.at[part], q_sem.at[2 * i + k])

    consts = [
        pltpu.make_async_copy(tw, tv, c_sem.at[0]),
        pltpu.make_async_copy(wz.at[col], wv.at[pl.ds(0, 256)], c_sem.at[1]),
        pltpu.make_async_copy(wz.at[other], wv.at[pl.ds(256, 256)], c_sem.at[2]),
        pltpu.make_async_copy(gf, gs, c_sem.at[3]),
    ]
    for i in range(4):
        quarter(i, 0).start()
        quarter(i, 1).start()
        if i == 0:
            consts[0].start()

    def step_x(g, first, count):
        ring = lax.rem(g, RING)
        slots = [3 + lax.rem(k + 4 - row, 4) for k in range(4)]
        bases = [[slots[k] * UNITS + 2 * g + t for t in range(2)] for k in range(4)]

        def one(y, s):
            ar = inr[ring, :, y].reshape(PACK * 32, 64).T
            ai = ini[ring, :, y].reshape(PACK * 32, 64).T
            a = dft8([(ar[8 * j : 8 * j + 8], ai[8 * j : 8 * j + 8]) for j in range(8)])
            for k1 in range(8):
                vr, vi = times(a[k1], tv[0, k1], tv[1, k1])
                asc[s, 0, pl.ds(8 * k1, 8), :] = vr
                asc[s, 1, pl.ds(8 * k1, 8), :] = vi
            b = dft8([tuple(asc[s, q, pl.ds(x2, 8, stride=8), :] for q in range(2)) for x2 in range(8)])
            for k2 in range(8):
                for q in range(2):
                    xbuf[bases[k2 // 2][k2 % 2], y, q] = b[k2][q]

        @pl.loop(0, count // 2)
        def _(i):
            one(first + 2 * i, 0)
            one(first + 2 * i + 1, 1)

    def send_row(u, n, j, first=0, count=16):
        p = dests[j]
        src, dst = (3 + p) * UNITS + u, (3 - p) * UNITS + u
        return pltpu.make_async_remote_copy(
            src_ref=xbuf.at[pl.ds(src, n), pl.ds(first, count)], dst_ref=xbuf.at[pl.ds(dst, n), pl.ds(first, count)],
            send_sem=s1.at[u * 3 + j], recv_sem=d1.at[u * 3 + 3 - p],
            device_id={"row": lax.rem(row + p, 4)}, device_id_type=MESH)

    def wait_row(u, n):
        for slot in range(3):
            part = xbuf.at[pl.ds(slot * UNITS + u, n)]
            pltpu.make_async_remote_copy(
                src_ref=part, dst_ref=part, send_sem=s1.at[u * 3], recv_sem=d1.at[u * 3 + slot],
                device_id={"row": row}, device_id_type=MESH).wait_recv()

    def batches(t, single, double):
        @pl.when((t < 2) | (t >= UNITS - 2))
        def _():
            single(t)

        @pl.when((t >= 2) & (t < UNITS - 2) & (lax.rem(t, 2) == 0))
        def _():
            double(t)

    def send_col(u):
        return pltpu.make_async_remote_copy(
            src_ref=b2.at[pl.ds(u * 4 + 2 * other, 2)], dst_ref=r2.at[pl.ds(u * 2, 2)],
            send_sem=s2.at[u], recv_sem=d2.at[u], device_id={"col": other}, device_id_type=MESH)

    def step_y(u):
        slots = [lax.rem(r + 7 - row, 4) * UNITS + u for r in range(4)]
        for y2 in range(8):
            a = dft8([tuple(xbuf[slots[y1 // 2], 8 * (y1 % 2) + y2, q] for q in range(2)) for y1 in range(8)])
            for k1 in range(8):
                vr, vi = times(a[k1], *twiddle(k1 * y2))
                bsc[k1, y2, 0] = vr
                bsc[k1, y2, 1] = vi
        for k1 in range(8):
            b = dft8([(bsc[k1, y2, 0], bsc[k1, y2, 1]) for y2 in range(8)])
            for k2 in range(8):
                for q in range(2):
                    b2[u * 4 + 2 * (k2 // 4) + q, pl.ds(8 * (k1 + 8 * (k2 % 4)), 8), :] = b[k2][q]

    def gather_z(u, dst):
        for kx in range(8):
            for q in range(2):
                dst[pl.ds(32 * kx, 32), pl.ds(128 * q, 128)] = b2[u * 4 + 2 * col + q, pl.ds(kx, 32, stride=8), :]
                dst[pl.ds(32 * kx, 32), pl.ds(256 + 128 * q, 128)] = r2[u * 2 + q, pl.ds(kx, 32, stride=8), :]

    def step_z(u):
        gather_z(u, lsc)
        gain = gv[pl.ds(pl.multiple_of(256 * lax.rem(u, 2), 256), 256), :]
        lane_product(lsc, wv, gain, outr, outi, lambda f: (PACK * (u // 2) + f, pl.ds(8 * lax.rem(u, 2), 8)))

    consts[0].wait()
    for i in range(4):
        quarter(i, 0).wait()
        quarter(i, 1).wait()
        step_x(0, 4 * i, 4)
        if i == 0:
            pl.semaphore_wait(barrier, 4)
            send_row(0, 1, 2, 0, 4).start()
        send_row(0, 1, 1, 4 * i, 4).start()
    send_row(0, 1, 0).start()
    send_row(0, 1, 2, 4, 12).start()
    for j in range(3):
        send_row(1, 1, j).start()

    @pl.loop(1, RING)
    def _(g):
        load(g, 0).start()
        load(g, 1).start()

    for copy in consts[1:]:
        copy.start()
    for k in range(2):
        load(RING, k).start()
        load(1, k).wait()
    step_x(1, 0, 16)
    for j in range(3):
        send_row(2, 2, j).start()
    for k in range(2):
        load(RING + 1, k).start()

    for copy in consts[1:]:
        copy.wait()
    gain = gs[...].reshape(512, 64)
    gv[...] = jnp.concatenate([gain, gain], axis=1)

    @pl.loop(0, UNITS + LAG - 1)
    def _(t):
        @pl.when(t < UNITS)
        def _():
            batches(t, lambda u: wait_row(u, 1), lambda u: wait_row(u, 2))
            step_y(t)
            send_col(t).start()

        g = t // 2 + 2

        @pl.when(g < GROUPS)
        def _():
            half = lax.rem(t, 2)

            @pl.when(half == 0)
            def _():
                load(g, 0).wait()
                load(g, 1).wait()

            step_x(g, 8 * half, 8)

            @pl.when(half == 1)
            def _():
                @pl.when(g < GROUPS - 1)
                def _():
                    for j in range(3):
                        send_row(2 * g, 2, j).start()

                @pl.when(g == GROUPS - 1)
                def _():
                    for u in (UNITS - 2, UNITS - 1):
                        for j in range(3):
                            send_row(u, 1, j).start()

                @pl.when(g + RING < GROUPS)
                def _():
                    load(g + RING, 0).start()
                    load(g + RING, 1).start()

        @pl.when(t >= LAG)
        def _():
            u = t - LAG
            send_col(u).wait_recv()
            step_z(u)

    @pl.loop(0, UNITS)
    def _(u):
        def done(u, n):
            for j in range(3):
                send_row(u, n, j).wait_send()

        batches(u, lambda u: done(u, 1), lambda u: done(u, 2))

    @pl.loop(0, UNITS - 1)
    def _(u):
        send_col(u).wait_send()

    send_col(UNITS - 1).wait_recv()
    gather_z(UNITS - 1, last)
    send_col(UNITS - 1).wait_send()


def put(vr, vi, mat, last, gain, outr, outi, lr, li, sem):
    cuts = [(pl.ds(7 * i, 7), slice(None)) for i in range(4)] + [(pl.ds(28, 4), pl.ds(0, 8))]
    copies = [pltpu.make_async_copy(v.at[cut], o.at[cut], sem.at[2 * i + k])
              for i, cut in enumerate(cuts) for k, (v, o) in enumerate(((vr, outr), (vi, outi)))]
    for copy in copies:
        copy.start()
    lane_product(last, mat, gain[256:, :], lr, li, lambda f: f)
    cut = (pl.ds(28, 4), pl.ds(8, 8))
    tail = [pltpu.make_async_copy(v, o.at[cut], sem.at[10 + k]) for k, (v, o) in enumerate(((lr, outr), (li, outi)))]
    for copy in tail:
        copy.start()
    for copy in copies + tail:
        copy.wait()


def solution(mesh):
    f32 = jnp.float32

    def local_forward(u_real, u_imag, g_filter):
        parts = [jnp.transpose(v, (0, 2, 3, 1)).reshape(GROUPS, PACK, 16, 32, 64) for v in (u_real, u_imag)]
        spectrum = pl.pallas_call(
            kernel,
            out_shape=[pltpu.VMEM((32, 16, 32, 64), f32)] * 2 + [
                pltpu.VMEM((512, 512), f32), pltpu.VMEM((256, 512), f32), pltpu.VMEM((512, 128), f32)],
            in_specs=[pl.BlockSpec(memory_space=pltpu.HBM)] * 5,
            out_specs=[pl.BlockSpec(memory_space=pltpu.VMEM)] * 5,
            scratch_shapes=[
                pltpu.VMEM((RING, PACK, 16, 32, 64), f32),
                pltpu.VMEM((RING, PACK, 16, 32, 64), f32),
                pltpu.VMEM((UNITS * 7, 16, 2, 8, 128), f32),
                pltpu.VMEM((UNITS * 4, 256, 128), f32),
                pltpu.VMEM((UNITS * 2, 256, 128), f32),
                pltpu.VMEM((2, 8, 8, 128), f32),
                pltpu.VMEM((16, 32, 64), f32),
                pltpu.VMEM((2, 2, 64, 128), f32),
                pltpu.VMEM((8, 8, 2, 8, 128), f32),
                pltpu.VMEM((256, 512), f32),
                pltpu.SemaphoreType.DMA((2 * RING,)),
                pltpu.SemaphoreType.DMA((8,)),
                pltpu.SemaphoreType.DMA((4,)),
                pltpu.SemaphoreType.DMA((3 * UNITS,)),
                pltpu.SemaphoreType.DMA((3 * UNITS,)),
                pltpu.SemaphoreType.DMA((UNITS,)),
                pltpu.SemaphoreType.DMA((UNITS,)),
            ],
            compiler_params=pltpu.CompilerParams(
                collective_id=0, has_side_effects=True, vmem_limit_bytes=40 * 1024 * 1024),
            name="dft3",
        )(*parts, g_filter, jnp.asarray(lane_matrix()), jnp.asarray(sublane_twiddle()))
        return pl.pallas_call(
            put,
            out_shape=[jax.ShapeDtypeStruct((32, 16, 32, 64), f32)] * 2,
            in_specs=[pl.BlockSpec(memory_space=pltpu.VMEM)] * 5,
            out_specs=[pl.BlockSpec(memory_space=pltpu.HBM)] * 2,
            scratch_shapes=[pltpu.VMEM((PACK, 8, 32, 64), f32)] * 2 + [pltpu.SemaphoreType.DMA((12,))],
            compiler_params=pltpu.CompilerParams(vmem_limit_bytes=8 * 1024 * 1024),
            name="put",
        )(*spectrum)

    field_spec = P("fld", None, "row", "col")
    out_spec = P("fld", "row", "col", None)
    return jax.shard_map(local_forward, mesh=mesh, in_specs=(field_spec, field_spec, P("row", "col", None)),
                         out_specs=(out_spec, out_spec), check_vma=False)
```

```python
import functools
import math

import jax
import jax.numpy as jnp
import numpy as np
from jax import lax
from jax.experimental import pallas as pl
from jax.experimental.pallas import tpu as pltpu
from jax.sharding import PartitionSpec as P

MESH = pl.DeviceIdType.MESH
HALF = math.sqrt(0.5)
GROUPS, PACK, UNITS, LAG, RING = 8, 4, 16, 2, 4


def dft4(b):
    (r0, i0), (r1, i1), (r2, i2), (r3, i3) = b
    sr0, si0, sr1, si1 = r0 + r2, i0 + i2, r0 - r2, i0 - i2
    sr2, si2, sr3, si3 = r1 + r3, i1 + i3, r1 - r3, i1 - i3
    return [(sr0 + sr2, si0 + si2), (sr1 + si3, si1 - sr3), (sr0 - sr2, si0 - si2), (sr1 - si3, si1 + sr3)]


def dft8(a):
    even = [(a[j][0] + a[j + 4][0], a[j][1] + a[j + 4][1]) for j in range(4)]
    odd = [(a[j][0] - a[j + 4][0], a[j][1] - a[j + 4][1]) for j in range(4)]
    (r1, i1), (r2, i2), (r3, i3) = odd[1:]
    odd = [odd[0], ((r1 + i1) * HALF, (i1 - r1) * HALF), (i2, -r2), ((i3 - r3) * HALF, (r3 + i3) * -HALF)]
    even, odd = dft4(even), dft4(odd)
    return [(even if k % 2 == 0 else odd)[k // 2] for k in range(8)]


def times(a, tr, ti):
    return a[0] * tr - a[1] * ti, a[0] * ti + a[1] * tr


def twiddle(m):
    angle = -2.0 * math.pi * (m % 64) / 64.0
    return math.cos(angle) / 8.0, math.sin(angle) / 8.0


def lane_matrix():
    z, kz = np.arange(64), np.arange(64)
    angle = 2.0 * np.pi * ((z[:, None] * kz[None, :]) % 64) / 64.0
    cos, sin = np.cos(angle) / 8.0, np.sin(angle) / 8.0
    blocks = np.stack([np.concatenate([cos, -sin], 1), np.concatenate([sin, cos], 1)])
    out = np.zeros((2, 2, PACK, 32, PACK, 128))
    for c in range(2):
        for f in range(PACK):
            out[c, :, f, :, f, :] = blocks[:, 32 * c : 32 * c + 32]
    return out.reshape(2, 256, PACK * 128).astype(np.float32)


def sublane_twiddle():
    k1, x2 = np.arange(8), np.arange(8)
    angle = -2.0 * np.pi * (k1[:, None] * x2[None, :]) / 64.0
    both = np.stack([np.cos(angle), np.sin(angle)]) / 8.0
    return np.broadcast_to(both[..., None], (2, 8, 8, 128)).astype(np.float32)


def lane_product(lhs, mat, gain, outr, outi, at):
    for n in range(2):
        w = jnp.dot(lhs[...], mat[:, 256 * n : 256 * n + 256], precision=lax.Precision.HIGHEST,
                    preferred_element_type=jnp.float32)
        for f in range(2):
            pair = w[:, 128 * f : 128 * f + 128] * gain
            outr[at(2 * n + f)] = pair[:, :64].reshape(8, 32, 64)
            outi[at(2 * n + f)] = pair[:, 64:].reshape(8, 32, 64)


def kernel(ur, ui, gf, wz, tw, outr, outi, wv, last, gv, inr, ini, xbuf, b2, r2, tv, gs, asc, bsc, lsc,
           in_sem, q_sem, c_sem, s1, d1, s2, d2):
    row, col = lax.axis_index("row"), lax.axis_index("col")
    core = lax.rem(row, 2)
    dests = [1 + 2 * core, 3 - core, 2 - core]
    other = 1 - col

    barrier = pltpu.get_barrier_semaphore()
    for p in (1, 2, 3):
        pl.semaphore_signal(barrier, inc=1, device_id={"row": lax.rem(row + p, 4)}, device_id_type=MESH)
    pl.semaphore_signal(barrier, inc=1, device_id={"col": other}, device_id_type=MESH)

    def load(g, k):
        src, dst = ((ur, inr), (ui, ini))[k]
        return pltpu.make_async_copy(src.at[g], dst.at[lax.rem(g, RING)], in_sem.at[2 * lax.rem(g, RING) + k])

    def quarter(i, k):
        src, dst = ((ur, inr), (ui, ini))[k]
        part = (0, slice(None), pl.ds(4 * i, 4))
        return pltpu.make_async_copy(src.at[part], dst.at[part], q_sem.at[2 * i + k])

    consts = [
        pltpu.make_async_copy(tw, tv, c_sem.at[0]),
        pltpu.make_async_copy(wz.at[col], wv.at[pl.ds(0, 256)], c_sem.at[1]),
        pltpu.make_async_copy(wz.at[other], wv.at[pl.ds(256, 256)], c_sem.at[2]),
        pltpu.make_async_copy(gf, gs, c_sem.at[3]),
    ]
    for i in range(4):
        quarter(i, 0).start()
        quarter(i, 1).start()
        if i == 0:
            consts[0].start()

    def step_x(g, first, count):
        ring = lax.rem(g, RING)
        slots = [3 + lax.rem(k + 4 - row, 4) for k in range(4)]
        bases = [[(2 * g + t) * 7 + slots[k] for t in range(2)] for k in range(4)]

        def one(y, s):
            ar = inr[ring, :, y].reshape(PACK * 32, 64).T
            ai = ini[ring, :, y].reshape(PACK * 32, 64).T
            a = dft8([(ar[8 * j : 8 * j + 8], ai[8 * j : 8 * j + 8]) for j in range(8)])
            for k1 in range(8):
                vr, vi = times(a[k1], tv[0, k1], tv[1, k1])
                asc[s, 0, pl.ds(8 * k1, 8), :] = vr
                asc[s, 1, pl.ds(8 * k1, 8), :] = vi
            b = dft8([tuple(asc[s, q, pl.ds(x2, 8, stride=8), :] for q in range(2)) for x2 in range(8)])
            for k2 in range(8):
                for q in range(2):
                    xbuf[bases[k2 // 2][k2 % 2], y, q] = b[k2][q]

        @pl.loop(0, count // 2)
        def _(i):
            one(first + 2 * i, 0)
            one(first + 2 * i + 1, 1)

    def send_row(u, j, first=0, count=16):
        p = dests[j]
        return pltpu.make_async_remote_copy(
            src_ref=xbuf.at[u * 7 + 3 + p, pl.ds(first, count)], dst_ref=xbuf.at[u * 7 + 3 - p, pl.ds(first, count)],
            send_sem=s1.at[u * 3 + j], recv_sem=d1.at[u * 3 + 3 - p],
            device_id={"row": lax.rem(row + p, 4)}, device_id_type=MESH)

    def wait_row(u, slot):
        part = xbuf.at[u * 7 + slot]
        pltpu.make_async_remote_copy(
            src_ref=part, dst_ref=part, send_sem=s1.at[u * 3], recv_sem=d1.at[u * 3 + slot],
            device_id={"row": row}, device_id_type=MESH).wait_recv()

    def send_col(u):
        return pltpu.make_async_remote_copy(
            src_ref=b2.at[pl.ds(u * 4 + 2 * other, 2)], dst_ref=r2.at[pl.ds(u * 2, 2)],
            send_sem=s2.at[u], recv_sem=d2.at[u], device_id={"col": other}, device_id_type=MESH)

    def step_y(u):
        slots = [u * 7 + lax.rem(r + 7 - row, 4) for r in range(4)]
        for y2 in range(8):
            a = dft8([tuple(xbuf[slots[y1 // 2], 8 * (y1 % 2) + y2, q] for q in range(2)) for y1 in range(8)])
            for k1 in range(8):
                vr, vi = times(a[k1], *twiddle(k1 * y2))
                bsc[k1, y2, 0] = vr
                bsc[k1, y2, 1] = vi
        for k1 in range(8):
            b = dft8([(bsc[k1, y2, 0], bsc[k1, y2, 1]) for y2 in range(8)])
            for k2 in range(8):
                for q in range(2):
                    b2[u * 4 + 2 * (k2 // 4) + q, pl.ds(8 * (k1 + 8 * (k2 % 4)), 8), :] = b[k2][q]

    def gather_z(u, dst):
        for kx in range(8):
            for q in range(2):
                dst[pl.ds(32 * kx, 32), pl.ds(128 * q, 128)] = b2[u * 4 + 2 * col + q, pl.ds(kx, 32, stride=8), :]
                dst[pl.ds(32 * kx, 32), pl.ds(256 + 128 * q, 128)] = r2[u * 2 + q, pl.ds(kx, 32, stride=8), :]

    def step_z(u):
        gather_z(u, lsc)
        gain = gv[pl.ds(pl.multiple_of(256 * lax.rem(u, 2), 256), 256), :]
        lane_product(lsc, wv, gain, outr, outi, lambda f: (PACK * (u // 2) + f, pl.ds(8 * lax.rem(u, 2), 8)))

    consts[0].wait()
    for i in range(4):
        quarter(i, 0).wait()
        quarter(i, 1).wait()
        step_x(0, 4 * i, 4)
        if i == 0:
            pl.semaphore_wait(barrier, 4)
            send_row(0, 2, 0, 4).start()
        send_row(0, 1, 4 * i, 4).start()
    send_row(0, 0).start()
    send_row(0, 2, 4, 12).start()
    for j in range(3):
        send_row(1, j).start()

    @pl.loop(1, RING)
    def _(g):
        load(g, 0).start()
        load(g, 1).start()

    for copy in consts[1:]:
        copy.start()
    for k in range(2):
        load(RING, k).start()
        load(1, k).wait()
    step_x(1, 0, 16)
    for t in range(2):
        for j in range(3):
            send_row(2 + t, j).start()
    for k in range(2):
        load(RING + 1, k).start()

    for copy in consts[1:]:
        copy.wait()
    gain = gs[...].reshape(512, 64)
    gv[...] = jnp.concatenate([gain, gain], axis=1)

    @pl.loop(0, UNITS + LAG - 1)
    def _(t):
        @pl.when(t < UNITS)
        def _():
            for slot in range(3):
                wait_row(t, slot)
            step_y(t)
            send_col(t).start()

        g = t // 2 + 2

        @pl.when(g < GROUPS)
        def _():
            half = lax.rem(t, 2)

            @pl.when(half == 0)
            def _():
                load(g, 0).wait()
                load(g, 1).wait()

            step_x(g, 8 * half, 8)

            @pl.when(half == 1)
            def _():
                for k in range(2):
                    for j in range(3):
                        send_row(2 * g + k, j).start()

                @pl.when(g + RING < GROUPS)
                def _():
                    load(g + RING, 0).start()
                    load(g + RING, 1).start()

        @pl.when(t >= LAG)
        def _():
            u = t - LAG
            send_col(u).wait_recv()
            step_z(u)

    @pl.loop(0, UNITS)
    def _(u):
        for j in range(3):
            send_row(u, j).wait_send()

    @pl.loop(0, UNITS - 1)
    def _(u):
        send_col(u).wait_send()

    send_col(UNITS - 1).wait_recv()
    gather_z(UNITS - 1, last)
    send_col(UNITS - 1).wait_send()


def put(vr, vi, mat, last, gain, outr, outi, lr, li, sem):
    cuts = [(pl.ds(7 * i, 7), slice(None)) for i in range(4)] + [(pl.ds(28, 4), pl.ds(0, 8))]
    copies = [pltpu.make_async_copy(v.at[cut], o.at[cut], sem.at[2 * i + k])
              for i, cut in enumerate(cuts) for k, (v, o) in enumerate(((vr, outr), (vi, outi)))]
    for copy in copies:
        copy.start()
    lane_product(last, mat, gain[256:, :], lr, li, lambda f: f)
    cut = (pl.ds(28, 4), pl.ds(8, 8))
    tail = [pltpu.make_async_copy(v, o.at[cut], sem.at[10 + k]) for k, (v, o) in enumerate(((lr, outr), (li, outi)))]
    for copy in tail:
        copy.start()
    for copy in copies + tail:
        copy.wait()


def solution(mesh):
    f32 = jnp.float32

    def local_forward(u_real, u_imag, g_filter):
        parts = [jnp.transpose(v, (0, 2, 3, 1)).reshape(GROUPS, PACK, 16, 32, 64) for v in (u_real, u_imag)]
        spectrum = pl.pallas_call(
            kernel,
            out_shape=[pltpu.VMEM((32, 16, 32, 64), f32)] * 2 + [
                pltpu.VMEM((512, 512), f32), pltpu.VMEM((256, 512), f32), pltpu.VMEM((512, 128), f32)],
            in_specs=[pl.BlockSpec(memory_space=pltpu.HBM)] * 5,
            out_specs=[pl.BlockSpec(memory_space=pltpu.VMEM)] * 5,
            scratch_shapes=[
                pltpu.VMEM((RING, PACK, 16, 32, 64), f32),
                pltpu.VMEM((RING, PACK, 16, 32, 64), f32),
                pltpu.VMEM((UNITS * 7, 16, 2, 8, 128), f32),
                pltpu.VMEM((UNITS * 4, 256, 128), f32),
                pltpu.VMEM((UNITS * 2, 256, 128), f32),
                pltpu.VMEM((2, 8, 8, 128), f32),
                pltpu.VMEM((16, 32, 64), f32),
                pltpu.VMEM((2, 2, 64, 128), f32),
                pltpu.VMEM((8, 8, 2, 8, 128), f32),
                pltpu.VMEM((256, 512), f32),
                pltpu.SemaphoreType.DMA((2 * RING,)),
                pltpu.SemaphoreType.DMA((8,)),
                pltpu.SemaphoreType.DMA((4,)),
                pltpu.SemaphoreType.DMA((3 * UNITS,)),
                pltpu.SemaphoreType.DMA((3 * UNITS,)),
                pltpu.SemaphoreType.DMA((UNITS,)),
                pltpu.SemaphoreType.DMA((UNITS,)),
            ],
            compiler_params=pltpu.CompilerParams(
                collective_id=0, has_side_effects=True, vmem_limit_bytes=40 * 1024 * 1024),
            name="dft3",
        )(*parts, g_filter, jnp.asarray(lane_matrix()), jnp.asarray(sublane_twiddle()))
        return pl.pallas_call(
            put,
            out_shape=[jax.ShapeDtypeStruct((32, 16, 32, 64), f32)] * 2,
            in_specs=[pl.BlockSpec(memory_space=pltpu.VMEM)] * 5,
            out_specs=[pl.BlockSpec(memory_space=pltpu.HBM)] * 2,
            scratch_shapes=[pltpu.VMEM((PACK, 8, 32, 64), f32)] * 2 + [pltpu.SemaphoreType.DMA((12,))],
            compiler_params=pltpu.CompilerParams(vmem_limit_bytes=8 * 1024 * 1024),
            name="put",
        )(*spectrum)

    field_spec = P("fld", None, "row", "col")
    out_spec = P("fld", "row", "col", None)
    return jax.shard_map(local_forward, mesh=mesh, in_specs=(field_spec, field_spec, P("row", "col", None)),
                         out_specs=(out_spec, out_spec), check_vma=False)
```

```python
import functools
import math

import jax
import jax.numpy as jnp
import numpy as np
from jax import lax
from jax.experimental import pallas as pl
from jax.experimental.pallas import tpu as pltpu
from jax.sharding import PartitionSpec as P

MESH = pl.DeviceIdType.MESH
HALF = math.sqrt(0.5)
GROUPS, PACK, UNITS, LAG, RING = 8, 4, 16, 2, 4


def dft4(b):
    (r0, i0), (r1, i1), (r2, i2), (r3, i3) = b
    sr0, si0, sr1, si1 = r0 + r2, i0 + i2, r0 - r2, i0 - i2
    sr2, si2, sr3, si3 = r1 + r3, i1 + i3, r1 - r3, i1 - i3
    return [(sr0 + sr2, si0 + si2), (sr1 + si3, si1 - sr3), (sr0 - sr2, si0 - si2), (sr1 - si3, si1 + sr3)]


def dft8(a):
    even = [(a[j][0] + a[j + 4][0], a[j][1] + a[j + 4][1]) for j in range(4)]
    odd = [(a[j][0] - a[j + 4][0], a[j][1] - a[j + 4][1]) for j in range(4)]
    (r1, i1), (r2, i2), (r3, i3) = odd[1:]
    odd = [odd[0], ((r1 + i1) * HALF, (i1 - r1) * HALF), (i2, -r2), ((i3 - r3) * HALF, (r3 + i3) * -HALF)]
    even, odd = dft4(even), dft4(odd)
    return [(even if k % 2 == 0 else odd)[k // 2] for k in range(8)]


def times(a, tr, ti):
    return a[0] * tr - a[1] * ti, a[0] * ti + a[1] * tr


def twiddle(m):
    angle = -2.0 * math.pi * (m % 64) / 64.0
    return math.cos(angle) / 8.0, math.sin(angle) / 8.0


def lane_matrix():
    z, kz = np.arange(64), np.arange(64)
    angle = 2.0 * np.pi * ((z[:, None] * kz[None, :]) % 64) / 64.0
    cos, sin = np.cos(angle) / 8.0, np.sin(angle) / 8.0
    blocks = np.stack([np.concatenate([cos, -sin], 1), np.concatenate([sin, cos], 1)])
    out = np.zeros((2, 2, PACK, 32, PACK, 128))
    for c in range(2):
        for f in range(PACK):
            out[c, :, f, :, f, :] = blocks[:, 32 * c : 32 * c + 32]
    return out.reshape(2, 256, PACK * 128).astype(np.float32)


def sublane_twiddle():
    k1, x2 = np.arange(8), np.arange(8)
    angle = -2.0 * np.pi * (k1[:, None] * x2[None, :]) / 64.0
    both = np.stack([np.cos(angle), np.sin(angle)]) / 8.0
    return np.broadcast_to(both[..., None], (2, 8, 8, 128)).astype(np.float32)


def lane_product(lhs, mat, gain, outr, outi, at):
    for n in range(2):
        w = jnp.dot(lhs[...], mat[:, 256 * n : 256 * n + 256], precision=lax.Precision.HIGHEST,
                    preferred_element_type=jnp.float32)
        for f in range(2):
            pair = w[:, 128 * f : 128 * f + 128] * gain
            outr[at(2 * n + f)] = pair[:, :64].reshape(8, 32, 64)
            outi[at(2 * n + f)] = pair[:, 64:].reshape(8, 32, 64)


def kernel(ur, ui, gf, wz, tw, outr, outi, wv, last, gv, inr, ini, xbuf, b2, r2, tv, gs, asc, bsc, lsc,
           in_sem, q_sem, c_sem, s1, d1, s2, d2):
    row, col = lax.axis_index("row"), lax.axis_index("col")
    core = lax.rem(row, 2)
    dests = [1 + 2 * core, 2 - core, 3 - core]
    other = 1 - col

    barrier = pltpu.get_barrier_semaphore()
    for p in (1, 2, 3):
        pl.semaphore_signal(barrier, inc=1, device_id={"row": lax.rem(row + p, 4)}, device_id_type=MESH)
    pl.semaphore_signal(barrier, inc=1, device_id={"col": other}, device_id_type=MESH)

    def load(g, k):
        src, dst = ((ur, inr), (ui, ini))[k]
        return pltpu.make_async_copy(src.at[g], dst.at[lax.rem(g, RING)], in_sem.at[2 * lax.rem(g, RING) + k])

    def quarter(i, k):
        src, dst = ((ur, inr), (ui, ini))[k]
        part = (0, slice(None), pl.ds(4 * i, 4))
        return pltpu.make_async_copy(src.at[part], dst.at[part], q_sem.at[2 * i + k])

    consts = [
        pltpu.make_async_copy(tw, tv, c_sem.at[0]),
        pltpu.make_async_copy(wz.at[col], wv.at[pl.ds(0, 256)], c_sem.at[1]),
        pltpu.make_async_copy(wz.at[other], wv.at[pl.ds(256, 256)], c_sem.at[2]),
        pltpu.make_async_copy(gf, gs, c_sem.at[3]),
    ]
    for i in range(4):
        quarter(i, 0).start()
        quarter(i, 1).start()
        if i == 0:
            consts[0].start()

    def step_x(g, first, count):
        ring = lax.rem(g, RING)
        slots = [3 + lax.rem(k + 4 - row, 4) for k in range(4)]
        bases = [[(2 * g + t) * 7 + slots[k] for t in range(2)] for k in range(4)]

        def one(y, s):
            ar = inr[ring, :, y].reshape(PACK * 32, 64).T
            ai = ini[ring, :, y].reshape(PACK * 32, 64).T
            a = dft8([(ar[8 * j : 8 * j + 8], ai[8 * j : 8 * j + 8]) for j in range(8)])
            for k1 in range(8):
                vr, vi = times(a[k1], tv[0, k1], tv[1, k1])
                asc[s, 0, pl.ds(8 * k1, 8), :] = vr
                asc[s, 1, pl.ds(8 * k1, 8), :] = vi
            b = dft8([tuple(asc[s, q, pl.ds(x2, 8, stride=8), :] for q in range(2)) for x2 in range(8)])
            for k2 in range(8):
                for q in range(2):
                    xbuf[bases[k2 // 2][k2 % 2], y, q] = b[k2][q]

        @pl.loop(0, count // 2)
        def _(i):
            one(first + 2 * i, 0)
            one(first + 2 * i + 1, 1)

    def send_row(u, j, first=0, count=16):
        p = dests[j]
        return pltpu.make_async_remote_copy(
            src_ref=xbuf.at[u * 7 + 3 + p, pl.ds(first, count)], dst_ref=xbuf.at[u * 7 + 3 - p, pl.ds(first, count)],
            send_sem=s1.at[u * 3 + j], recv_sem=d1.at[u * 3 + 3 - p],
            device_id={"row": lax.rem(row + p, 4)}, device_id_type=MESH)

    def wait_row(u, slot):
        part = xbuf.at[u * 7 + slot]
        pltpu.make_async_remote_copy(
            src_ref=part, dst_ref=part, send_sem=s1.at[u * 3], recv_sem=d1.at[u * 3 + slot],
            device_id={"row": row}, device_id_type=MESH).wait_recv()

    def send_col(u):
        return pltpu.make_async_remote_copy(
            src_ref=b2.at[pl.ds(u * 4 + 2 * other, 2)], dst_ref=r2.at[pl.ds(u * 2, 2)],
            send_sem=s2.at[u], recv_sem=d2.at[u], device_id={"col": other}, device_id_type=MESH)

    def step_y(u):
        slots = [u * 7 + lax.rem(r + 7 - row, 4) for r in range(4)]
        for y2 in range(8):
            a = dft8([tuple(xbuf[slots[y1 // 2], 8 * (y1 % 2) + y2, q] for q in range(2)) for y1 in range(8)])
            for k1 in range(8):
                vr, vi = times(a[k1], *twiddle(k1 * y2))
                bsc[k1, y2, 0] = vr
                bsc[k1, y2, 1] = vi
        for k1 in range(8):
            b = dft8([(bsc[k1, y2, 0], bsc[k1, y2, 1]) for y2 in range(8)])
            for k2 in range(8):
                for q in range(2):
                    b2[u * 4 + 2 * (k2 // 4) + q, pl.ds(8 * (k1 + 8 * (k2 % 4)), 8), :] = b[k2][q]

    def gather_z(u, dst):
        for kx in range(8):
            for q in range(2):
                dst[pl.ds(32 * kx, 32), pl.ds(128 * q, 128)] = b2[u * 4 + 2 * col + q, pl.ds(kx, 32, stride=8), :]
                dst[pl.ds(32 * kx, 32), pl.ds(256 + 128 * q, 128)] = r2[u * 2 + q, pl.ds(kx, 32, stride=8), :]

    def step_z(u):
        gather_z(u, lsc)
        gain = gv[pl.ds(pl.multiple_of(256 * lax.rem(u, 2), 256), 256), :]
        lane_product(lsc, wv, gain, outr, outi, lambda f: (PACK * (u // 2) + f, pl.ds(8 * lax.rem(u, 2), 8)))

    consts[0].wait()
    for i in range(4):
        quarter(i, 0).wait()
        quarter(i, 1).wait()
        step_x(0, 4 * i, 4)
        if i == 0:
            pl.semaphore_wait(barrier, 4)
            send_row(0, 2, 0, 4).start()
        send_row(0, 1, 4 * i, 4).start()
    send_row(0, 0).start()
    send_row(0, 2, 4, 12).start()
    for j in range(3):
        send_row(1, j).start()

    @pl.loop(1, RING)
    def _(g):
        load(g, 0).start()
        load(g, 1).start()

    for copy in consts[1:]:
        copy.start()
    @pl.loop(0, UNITS + LAG - 1)
    def _(t):
        @pl.when(t < UNITS)
        def _():
            for slot in range(3):
                wait_row(t, slot)
            step_y(t)
            send_col(t).start()

        @pl.when(t == 0)
        def _():
            for k in range(2):
                load(RING, k).start()
                load(1, k).wait()
            step_x(1, 0, 16)
            for u in (2, 3):
                for j in range(3):
                    send_row(u, j).start()
            for k in range(2):
                load(RING + 1, k).start()
            for copy in consts[1:]:
                copy.wait()
            gain = gs[...].reshape(512, 64)
            gv[...] = jnp.concatenate([gain, gain], axis=1)

        g = (t + 3) // 2

        @pl.when((t >= 1) & (g < GROUPS))
        def _():
            half = lax.rem(t + 1, 2)

            @pl.when(half == 0)
            def _():
                load(g, 0).wait()
                load(g, 1).wait()

            step_x(g, 8 * half, 8)

            @pl.when(half == 1)
            def _():
                for k in range(2):
                    for j in range(3):
                        send_row(2 * g + k, j).start()

                @pl.when(g + RING < GROUPS)
                def _():
                    load(g + RING, 0).start()
                    load(g + RING, 1).start()

        @pl.when(t >= LAG)
        def _():
            u = t - LAG
            send_col(u).wait_recv()
            step_z(u)

    @pl.loop(0, UNITS)
    def _(u):
        for j in range(3):
            send_row(u, j).wait_send()

    @pl.loop(0, UNITS - 1)
    def _(u):
        send_col(u).wait_send()

    send_col(UNITS - 1).wait_recv()
    gather_z(UNITS - 1, last)
    send_col(UNITS - 1).wait_send()


def put(vr, vi, mat, last, gain, outr, outi, lr, li, sem):
    cuts = [(pl.ds(7 * i, 7), slice(None)) for i in range(4)] + [(pl.ds(28, 4), pl.ds(0, 8))]
    copies = [pltpu.make_async_copy(v.at[cut], o.at[cut], sem.at[2 * i + k])
              for i, cut in enumerate(cuts) for k, (v, o) in enumerate(((vr, outr), (vi, outi)))]
    for copy in copies:
        copy.start()
    lane_product(last, mat, gain[256:, :], lr, li, lambda f: f)
    cut = (pl.ds(28, 4), pl.ds(8, 8))
    tail = [pltpu.make_async_copy(v, o.at[cut], sem.at[10 + k]) for k, (v, o) in enumerate(((lr, outr), (li, outi)))]
    for copy in tail:
        copy.start()
    for copy in copies + tail:
        copy.wait()


def solution(mesh):
    f32 = jnp.float32

    def local_forward(u_real, u_imag, g_filter):
        parts = [jnp.transpose(v, (0, 2, 3, 1)).reshape(GROUPS, PACK, 16, 32, 64) for v in (u_real, u_imag)]
        spectrum = pl.pallas_call(
            kernel,
            out_shape=[pltpu.VMEM((32, 16, 32, 64), f32)] * 2 + [
                pltpu.VMEM((512, 512), f32), pltpu.VMEM((256, 512), f32), pltpu.VMEM((512, 128), f32)],
            in_specs=[pl.BlockSpec(memory_space=pltpu.HBM)] * 5,
            out_specs=[pl.BlockSpec(memory_space=pltpu.VMEM)] * 5,
            scratch_shapes=[
                pltpu.VMEM((RING, PACK, 16, 32, 64), f32),
                pltpu.VMEM((RING, PACK, 16, 32, 64), f32),
                pltpu.VMEM((UNITS * 7, 16, 2, 8, 128), f32),
                pltpu.VMEM((UNITS * 4, 256, 128), f32),
                pltpu.VMEM((UNITS * 2, 256, 128), f32),
                pltpu.VMEM((2, 8, 8, 128), f32),
                pltpu.VMEM((16, 32, 64), f32),
                pltpu.VMEM((2, 2, 64, 128), f32),
                pltpu.VMEM((8, 8, 2, 8, 128), f32),
                pltpu.VMEM((256, 512), f32),
                pltpu.SemaphoreType.DMA((2 * RING,)),
                pltpu.SemaphoreType.DMA((8,)),
                pltpu.SemaphoreType.DMA((4,)),
                pltpu.SemaphoreType.DMA((3 * UNITS,)),
                pltpu.SemaphoreType.DMA((3 * UNITS,)),
                pltpu.SemaphoreType.DMA((UNITS,)),
                pltpu.SemaphoreType.DMA((UNITS,)),
            ],
            compiler_params=pltpu.CompilerParams(
                collective_id=0, has_side_effects=True, vmem_limit_bytes=40 * 1024 * 1024),
            name="dft3",
        )(*parts, g_filter, jnp.asarray(lane_matrix()), jnp.asarray(sublane_twiddle()))
        return pl.pallas_call(
            put,
            out_shape=[jax.ShapeDtypeStruct((32, 16, 32, 64), f32)] * 2,
            in_specs=[pl.BlockSpec(memory_space=pltpu.VMEM)] * 5,
            out_specs=[pl.BlockSpec(memory_space=pltpu.HBM)] * 2,
            scratch_shapes=[pltpu.VMEM((PACK, 8, 32, 64), f32)] * 2 + [pltpu.SemaphoreType.DMA((12,))],
            compiler_params=pltpu.CompilerParams(vmem_limit_bytes=8 * 1024 * 1024),
            name="put",
        )(*spectrum)

    field_spec = P("fld", None, "row", "col")
    out_spec = P("fld", "row", "col", None)
    return jax.shard_map(local_forward, mesh=mesh, in_specs=(field_spec, field_spec, P("row", "col", None)),
                         out_specs=(out_spec, out_spec), check_vma=False)
```

```python
import functools
import math

import jax
import jax.numpy as jnp
import numpy as np
from jax import lax
from jax.experimental import pallas as pl
from jax.experimental.pallas import tpu as pltpu
from jax.sharding import PartitionSpec as P

MESH = pl.DeviceIdType.MESH
HALF = math.sqrt(0.5)
GROUPS, PACK, UNITS, LAG, RING = 8, 4, 16, 2, 4


def dft4(b):
    (r0, i0), (r1, i1), (r2, i2), (r3, i3) = b
    sr0, si0, sr1, si1 = r0 + r2, i0 + i2, r0 - r2, i0 - i2
    sr2, si2, sr3, si3 = r1 + r3, i1 + i3, r1 - r3, i1 - i3
    return [(sr0 + sr2, si0 + si2), (sr1 + si3, si1 - sr3), (sr0 - sr2, si0 - si2), (sr1 - si3, si1 + sr3)]


def dft8(a):
    even = [(a[j][0] + a[j + 4][0], a[j][1] + a[j + 4][1]) for j in range(4)]
    odd = [(a[j][0] - a[j + 4][0], a[j][1] - a[j + 4][1]) for j in range(4)]
    (r1, i1), (r2, i2), (r3, i3) = odd[1:]
    odd = [odd[0], ((r1 + i1) * HALF, (i1 - r1) * HALF), (i2, -r2), ((i3 - r3) * HALF, (r3 + i3) * -HALF)]
    even, odd = dft4(even), dft4(odd)
    return [(even if k % 2 == 0 else odd)[k // 2] for k in range(8)]


def times(a, tr, ti):
    return a[0] * tr - a[1] * ti, a[0] * ti + a[1] * tr


def twiddle(m):
    angle = -2.0 * math.pi * (m % 64) / 64.0
    return math.cos(angle) / 8.0, math.sin(angle) / 8.0


def lane_matrix():
    z, kz = np.arange(64), np.arange(64)
    angle = 2.0 * np.pi * ((z[:, None] * kz[None, :]) % 64) / 64.0
    cos, sin = np.cos(angle) / 8.0, np.sin(angle) / 8.0
    blocks = np.stack([np.concatenate([cos, -sin], 1), np.concatenate([sin, cos], 1)])
    out = np.zeros((2, 2, PACK, 32, PACK, 128))
    for c in range(2):
        for f in range(PACK):
            out[c, :, f, :, f, :] = blocks[:, 32 * c : 32 * c + 32]
    return out.reshape(2, 256, PACK * 128).astype(np.float32)


def sublane_twiddle():
    k1, x2 = np.arange(8), np.arange(8)
    angle = -2.0 * np.pi * (k1[:, None] * x2[None, :]) / 64.0
    both = np.stack([np.cos(angle), np.sin(angle)]) / 8.0
    return np.broadcast_to(both[..., None], (2, 8, 8, 128)).astype(np.float32)


def lane_product(lhs, mat, gain, outr, outi, at):
    for n in range(2):
        w = jnp.dot(lhs[...], mat[:, 256 * n : 256 * n + 256], precision=lax.Precision.HIGHEST,
                    preferred_element_type=jnp.float32)
        for f in range(2):
            pair = w[:, 128 * f : 128 * f + 128] * gain
            outr[at(2 * n + f)] = pair[:, :64].reshape(8, 32, 64)
            outi[at(2 * n + f)] = pair[:, 64:].reshape(8, 32, 64)


def kernel(ur, ui, gf, wz, tw, outr, outi, wv, last, gv, inr, ini, xbuf, b2, r2, tv, gs, asc, bsc, lsc,
           in_sem, q_sem, c_sem, s1, d1, s2, d2):
    row, col = lax.axis_index("row"), lax.axis_index("col")
    core = lax.rem(row, 2)
    dests = [1 + 2 * core, 2 - core, 3 - core]
    other = 1 - col

    barrier = pltpu.get_barrier_semaphore()
    for p in (1, 2, 3):
        pl.semaphore_signal(barrier, inc=1, device_id={"row": lax.rem(row + p, 4)}, device_id_type=MESH)
    pl.semaphore_signal(barrier, inc=1, device_id={"col": other}, device_id_type=MESH)

    def load(g, k):
        src, dst = ((ur, inr), (ui, ini))[k]
        return pltpu.make_async_copy(src.at[g], dst.at[lax.rem(g, RING)], in_sem.at[2 * lax.rem(g, RING) + k])

    pieces = ((0, 2), (2, 2), (4, 4), (8, 8))

    def piece(i, k):
        src, dst = ((ur, inr), (ui, ini))[k]
        part = (0, slice(None), pl.ds(*pieces[i]))
        return pltpu.make_async_copy(src.at[part], dst.at[part], q_sem.at[2 * i + k])

    consts = [
        pltpu.make_async_copy(tw, tv, c_sem.at[0]),
        pltpu.make_async_copy(wz.at[col], wv.at[pl.ds(0, 256)], c_sem.at[1]),
        pltpu.make_async_copy(wz.at[other], wv.at[pl.ds(256, 256)], c_sem.at[2]),
        pltpu.make_async_copy(gf, gs, c_sem.at[3]),
    ]
    for i in range(4):
        piece(i, 0).start()
        piece(i, 1).start()
        if i == 0:
            consts[0].start()

    def step_x(g, first, count):
        ring = lax.rem(g, RING)
        slots = [3 + lax.rem(k + 4 - row, 4) for k in range(4)]
        bases = [[(2 * g + t) * 7 + slots[k] for t in range(2)] for k in range(4)]

        def one(y, s):
            ar = inr[ring, :, y].reshape(PACK * 32, 64).T
            ai = ini[ring, :, y].reshape(PACK * 32, 64).T
            a = dft8([(ar[8 * j : 8 * j + 8], ai[8 * j : 8 * j + 8]) for j in range(8)])
            for k1 in range(8):
                vr, vi = times(a[k1], tv[0, k1], tv[1, k1])
                asc[s, 0, pl.ds(8 * k1, 8), :] = vr
                asc[s, 1, pl.ds(8 * k1, 8), :] = vi
            b = dft8([tuple(asc[s, q, pl.ds(x2, 8, stride=8), :] for q in range(2)) for x2 in range(8)])
            for k2 in range(8):
                for q in range(2):
                    xbuf[bases[k2 // 2][k2 % 2], y, q] = b[k2][q]

        @pl.loop(0, count // 2)
        def _(i):
            one(first + 2 * i, 0)
            one(first + 2 * i + 1, 1)

    def send_row(u, j, first=0, count=16):
        p = dests[j]
        return pltpu.make_async_remote_copy(
            src_ref=xbuf.at[u * 7 + 3 + p, pl.ds(first, count)], dst_ref=xbuf.at[u * 7 + 3 - p, pl.ds(first, count)],
            send_sem=s1.at[u * 3 + j], recv_sem=d1.at[u * 3 + 3 - p],
            device_id={"row": lax.rem(row + p, 4)}, device_id_type=MESH)

    def wait_row(u, slot):
        part = xbuf.at[u * 7 + slot]
        pltpu.make_async_remote_copy(
            src_ref=part, dst_ref=part, send_sem=s1.at[u * 3], recv_sem=d1.at[u * 3 + slot],
            device_id={"row": row}, device_id_type=MESH).wait_recv()

    def send_col(u):
        return pltpu.make_async_remote_copy(
            src_ref=b2.at[pl.ds(u * 4 + 2 * other, 2)], dst_ref=r2.at[pl.ds(u * 2, 2)],
            send_sem=s2.at[u], recv_sem=d2.at[u], device_id={"col": other}, device_id_type=MESH)

    def step_y(u):
        slots = [u * 7 + lax.rem(r + 7 - row, 4) for r in range(4)]
        for y2 in range(8):
            a = dft8([tuple(xbuf[slots[y1 // 2], 8 * (y1 % 2) + y2, q] for q in range(2)) for y1 in range(8)])
            for k1 in range(8):
                vr, vi = times(a[k1], *twiddle(k1 * y2))
                bsc[k1, y2, 0] = vr
                bsc[k1, y2, 1] = vi
        for k1 in range(8):
            b = dft8([(bsc[k1, y2, 0], bsc[k1, y2, 1]) for y2 in range(8)])
            for k2 in range(8):
                for q in range(2):
                    b2[u * 4 + 2 * (k2 // 4) + q, pl.ds(8 * (k1 + 8 * (k2 % 4)), 8), :] = b[k2][q]

    def gather_z(u, dst):
        for kx in range(8):
            for q in range(2):
                dst[pl.ds(32 * kx, 32), pl.ds(128 * q, 128)] = b2[u * 4 + 2 * col + q, pl.ds(kx, 32, stride=8), :]
                dst[pl.ds(32 * kx, 32), pl.ds(256 + 128 * q, 128)] = r2[u * 2 + q, pl.ds(kx, 32, stride=8), :]

    def step_z(u):
        gather_z(u, lsc)
        gain = gv[pl.ds(pl.multiple_of(256 * lax.rem(u, 2), 256), 256), :]
        lane_product(lsc, wv, gain, outr, outi, lambda f: (PACK * (u // 2) + f, pl.ds(8 * lax.rem(u, 2), 8)))

    consts[0].wait()
    for i, (first, count) in enumerate(pieces):
        piece(i, 0).wait()
        piece(i, 1).wait()
        step_x(0, first, count)
        if i == 0:
            pl.semaphore_wait(barrier, 4)
        send_row(0, 1, first, count).start()
    send_row(0, 0).start()
    send_row(0, 2).start()
    for j in range(3):
        send_row(1, j).start()

    @pl.loop(1, RING)
    def _(g):
        load(g, 0).start()
        load(g, 1).start()

    for copy in consts[1:]:
        copy.start()
    @pl.loop(0, UNITS + LAG - 1)
    def _(t):
        @pl.when(t < UNITS)
        def _():
            for slot in range(3):
                wait_row(t, slot)
            step_y(t)
            send_col(t).start()

        @pl.when(t == 0)
        def _():
            for k in range(2):
                load(RING, k).start()
                load(1, k).wait()
            step_x(1, 0, 16)
            for u in (2, 3):
                for j in range(3):
                    send_row(u, j).start()
            for k in range(2):
                load(RING + 1, k).start()
            for copy in consts[1:]:
                copy.wait()
            gain = gs[...].reshape(512, 64)
            gv[...] = jnp.concatenate([gain, gain], axis=1)

        g = (t + 3) // 2

        @pl.when((t >= 1) & (g < GROUPS))
        def _():
            half = lax.rem(t + 1, 2)

            @pl.when(half == 0)
            def _():
                load(g, 0).wait()
                load(g, 1).wait()

            step_x(g, 8 * half, 8)

            @pl.when(half == 1)
            def _():
                for k in range(2):
                    for j in range(3):
                        send_row(2 * g + k, j).start()

                @pl.when(g + RING < GROUPS)
                def _():
                    load(g + RING, 0).start()
                    load(g + RING, 1).start()

        @pl.when(t >= LAG)
        def _():
            u = t - LAG
            send_col(u).wait_recv()
            step_z(u)

    @pl.loop(0, UNITS)
    def _(u):
        for j in range(3):
            send_row(u, j).wait_send()

    @pl.loop(0, UNITS - 1)
    def _(u):
        send_col(u).wait_send()

    send_col(UNITS - 1).wait_recv()
    gather_z(UNITS - 1, last)
    send_col(UNITS - 1).wait_send()


def put(vr, vi, mat, last, gain, outr, outi, lr, li, sem):
    cuts = [(pl.ds(7 * i, 7), slice(None)) for i in range(4)] + [(pl.ds(28, 4), pl.ds(0, 8))]
    copies = [pltpu.make_async_copy(v.at[cut], o.at[cut], sem.at[2 * i + k])
              for i, cut in enumerate(cuts) for k, (v, o) in enumerate(((vr, outr), (vi, outi)))]
    for copy in copies:
        copy.start()
    lane_product(last, mat, gain[256:, :], lr, li, lambda f: f)
    cut = (pl.ds(28, 4), pl.ds(8, 8))
    tail = [pltpu.make_async_copy(v, o.at[cut], sem.at[10 + k]) for k, (v, o) in enumerate(((lr, outr), (li, outi)))]
    for copy in tail:
        copy.start()
    for copy in copies + tail:
        copy.wait()


def solution(mesh):
    f32 = jnp.float32

    def local_forward(u_real, u_imag, g_filter):
        parts = [jnp.transpose(v, (0, 2, 3, 1)).reshape(GROUPS, PACK, 16, 32, 64) for v in (u_real, u_imag)]
        spectrum = pl.pallas_call(
            kernel,
            out_shape=[pltpu.VMEM((32, 16, 32, 64), f32)] * 2 + [
                pltpu.VMEM((512, 512), f32), pltpu.VMEM((256, 512), f32), pltpu.VMEM((512, 128), f32)],
            in_specs=[pl.BlockSpec(memory_space=pltpu.HBM)] * 5,
            out_specs=[pl.BlockSpec(memory_space=pltpu.VMEM)] * 5,
            scratch_shapes=[
                pltpu.VMEM((RING, PACK, 16, 32, 64), f32),
                pltpu.VMEM((RING, PACK, 16, 32, 64), f32),
                pltpu.VMEM((UNITS * 7, 16, 2, 8, 128), f32),
                pltpu.VMEM((UNITS * 4, 256, 128), f32),
                pltpu.VMEM((UNITS * 2, 256, 128), f32),
                pltpu.VMEM((2, 8, 8, 128), f32),
                pltpu.VMEM((16, 32, 64), f32),
                pltpu.VMEM((2, 2, 64, 128), f32),
                pltpu.VMEM((8, 8, 2, 8, 128), f32),
                pltpu.VMEM((256, 512), f32),
                pltpu.SemaphoreType.DMA((2 * RING,)),
                pltpu.SemaphoreType.DMA((8,)),
                pltpu.SemaphoreType.DMA((4,)),
                pltpu.SemaphoreType.DMA((3 * UNITS,)),
                pltpu.SemaphoreType.DMA((3 * UNITS,)),
                pltpu.SemaphoreType.DMA((UNITS,)),
                pltpu.SemaphoreType.DMA((UNITS,)),
            ],
            compiler_params=pltpu.CompilerParams(
                collective_id=0, has_side_effects=True, vmem_limit_bytes=40 * 1024 * 1024),
            name="dft3",
        )(*parts, g_filter, jnp.asarray(lane_matrix()), jnp.asarray(sublane_twiddle()))
        return pl.pallas_call(
            put,
            out_shape=[jax.ShapeDtypeStruct((32, 16, 32, 64), f32)] * 2,
            in_specs=[pl.BlockSpec(memory_space=pltpu.VMEM)] * 5,
            out_specs=[pl.BlockSpec(memory_space=pltpu.HBM)] * 2,
            scratch_shapes=[pltpu.VMEM((PACK, 8, 32, 64), f32)] * 2 + [pltpu.SemaphoreType.DMA((12,))],
            compiler_params=pltpu.CompilerParams(vmem_limit_bytes=8 * 1024 * 1024),
            name="put",
        )(*spectrum)

    field_spec = P("fld", None, "row", "col")
    out_spec = P("fld", "row", "col", None)
    return jax.shard_map(local_forward, mesh=mesh, in_specs=(field_spec, field_spec, P("row", "col", None)),
                         out_specs=(out_spec, out_spec), check_vma=False)
```

```python
import functools
import math

import jax
import jax.numpy as jnp
import numpy as np
from jax import lax
from jax.experimental import pallas as pl
from jax.experimental.pallas import tpu as pltpu
from jax.sharding import PartitionSpec as P

MESH = pl.DeviceIdType.MESH
HALF = math.sqrt(0.5)
GROUPS, PACK, UNITS, LAG, RING = 8, 4, 16, 2, 4


def interleave(even, odd):
    return [v for pair in zip(even, odd) for v in pair]


def dft4(b):
    (r0, i0), (r1, i1), (r2, i2), (r3, i3) = b
    sr0, si0, sr1, si1 = r0 + r2, i0 + i2, r0 - r2, i0 - i2
    sr2, si2, sr3, si3 = r1 + r3, i1 + i3, r1 - r3, i1 - i3
    return [(sr0 + sr2, si0 + si2), (sr1 + si3, si1 - sr3), (sr0 - sr2, si0 - si2), (sr1 - si3, si1 + sr3)]


def dft8(a):
    pairs = list(zip(a[:4], a[4:]))
    even = [(vr + wr, vi + wi) for (vr, vi), (wr, wi) in pairs]
    odd = [(vr - wr, vi - wi) for (vr, vi), (wr, wi) in pairs]
    o0, (r1, i1), (r2, i2), (r3, i3) = odd
    odd = [o0, ((r1 + i1) * HALF, (i1 - r1) * HALF), (i2, -r2), ((i3 - r3) * HALF, (r3 + i3) * -HALF)]
    even, odd = dft4(even), dft4(odd)
    return interleave(even, odd)


def rotate(v):
    sign = jnp.where(lax.broadcasted_iota(jnp.int32, v.shape, 0) < 4, 1.0, -1.0)
    return pltpu.roll(v, 4, 0) * sign


def packed_dft4(b):
    b0, b1, b2, b3 = b
    s0, s1, s2, s3 = b0 + b2, b0 - b2, b1 + b3, rotate(b1 - b3)
    return [s0 + s2, s1 + s3, s0 - s2, s1 - s3]


def packed_dft8(a):
    pairs = list(zip(a[:4], a[4:]))
    even = packed_dft4([v + w for v, w in pairs])
    o0, o1, o2, o3 = [v - w for v, w in pairs]
    odd = packed_dft4([o0, (rotate(o1) + o1) * HALF, rotate(o2), (rotate(o3) - o3) * HALF])
    return interleave(even, odd)


def times(a, tr, ti):
    return a[0] * tr - a[1] * ti, a[0] * ti + a[1] * tr


def twiddle(m):
    angle = -2.0 * math.pi * (m % 64) / 64.0
    return math.cos(angle) / 8.0, math.sin(angle) / 8.0


def lane_matrix():
    z, kz = np.arange(64), np.arange(64)
    angle = 2.0 * np.pi * ((z[:, None] * kz[None, :]) % 64) / 64.0
    cos, sin = np.cos(angle) / 8.0, np.sin(angle) / 8.0
    blocks = np.stack([np.concatenate([cos, -sin], 1), np.concatenate([sin, cos], 1)])
    out = np.zeros((2, 2, PACK, 32, PACK, 128))
    for c in range(2):
        for f in range(PACK):
            out[c, :, f, :, f, :] = blocks[:, 32 * c : 32 * c + 32]
    return out.reshape(2, 256, PACK * 128).astype(np.float32)


def sublane_twiddle():
    k1, x2 = np.arange(8), np.arange(8)
    angle = -2.0 * np.pi * (k1[:, None] * x2[None, :]) / 64.0
    both = np.stack([np.cos(angle), np.sin(angle)]) / 8.0
    return np.broadcast_to(both[..., None], (2, 8, 8, 128)).astype(np.float32)


def lane_product(lhs, mat, gain, outr, outi, at):
    for n in range(2):
        w = jnp.dot(lhs[...], mat[:, 256 * n : 256 * n + 256], precision=lax.Precision.HIGHEST,
                    preferred_element_type=jnp.float32)
        for f in range(2):
            pair = w[:, 128 * f : 128 * f + 128] * gain
            outr[at(2 * n + f)] = pair[:, :64].reshape(8, 32, 64)
            outi[at(2 * n + f)] = pair[:, 64:].reshape(8, 32, 64)


def kernel(ur, ui, gf, wz, tw, outr, outi, wv, last, gv, inr, ini, xbuf, b2, r2, tv, gs, asc, bsc, lsc,
           in_sem, q_sem, c_sem, s1, d1, s2, d2):
    row, col = lax.axis_index("row"), lax.axis_index("col")
    core = lax.rem(row, 2)
    dests = [1 + 2 * core, 2 - core, 3 - core]
    other = 1 - col

    barrier = pltpu.get_barrier_semaphore()
    for p in (1, 2, 3):
        pl.semaphore_signal(barrier, inc=1, device_id={"row": lax.rem(row + p, 4)}, device_id_type=MESH)
    pl.semaphore_signal(barrier, inc=1, device_id={"col": other}, device_id_type=MESH)

    def load(g, k):
        src, dst = ((ur, inr), (ui, ini))[k]
        return pltpu.make_async_copy(src.at[g], dst.at[lax.rem(g, RING)], in_sem.at[2 * lax.rem(g, RING) + k])

    pieces = ((0, 2), (2, 2), (4, 4), (8, 8))

    def piece(i, k):
        src, dst = ((ur, inr), (ui, ini))[k]
        part = (0, slice(None), pl.ds(*pieces[i]))
        return pltpu.make_async_copy(src.at[part], dst.at[part], q_sem.at[2 * i + k])

    consts = [
        pltpu.make_async_copy(tw, tv, c_sem.at[0]),
        pltpu.make_async_copy(wz.at[col], wv.at[pl.ds(0, 256)], c_sem.at[1]),
        pltpu.make_async_copy(wz.at[other], wv.at[pl.ds(256, 256)], c_sem.at[2]),
        pltpu.make_async_copy(gf, gs, c_sem.at[3]),
    ]
    for i in range(4):
        piece(i, 0).start()
        piece(i, 1).start()
        if i == 0:
            consts[0].start()

    def step_x(g, first, count, packed=None):
        ring = lax.rem(g, RING)
        slots = [3 + lax.rem(k + 4 - row, 4) for k in range(4)]
        bases = [[(2 * g + t) * 7 + slots[k] for t in range(2)] for k in range(4)]

        def one(i, s):
            y = first + 2 * i + s
            ar = inr[ring, :, y].reshape(PACK * 32, 64).T
            ai = ini[ring, :, y].reshape(PACK * 32, 64).T
            a = dft8([(ar[8 * j : 8 * j + 8], ai[8 * j : 8 * j + 8]) for j in range(8)])
            for k1 in range(8):
                vr, vi = times(a[k1], tv[0, k1], tv[1, k1])
                asc[s, 0, pl.ds(8 * k1, 8), :] = vr
                asc[s, 1, pl.ds(8 * k1, 8), :] = vi
            b = dft8([tuple(asc[s, q, pl.ds(x2, 8, stride=8), :] for q in range(2)) for x2 in range(8)])
            for k2 in range(8):
                at, (vr, vi) = bases[k2 // 2][k2 % 2], b[k2]
                if k2 % 2 == packed:
                    top = lax.broadcasted_iota(jnp.int32, vr.shape, 0) < 4
                    xbuf[at, first // 2 + i, s] = jnp.where(top, vr, pltpu.roll(vi, 4, 0))
                    xbuf[at, 8 + first // 2 + i, s] = jnp.where(top, pltpu.roll(vr, 4, 0), vi)
                else:
                    xbuf[at, y, 0] = vr
                    xbuf[at, y, 1] = vi

        @pl.loop(0, count // 2)
        def _(i):
            one(i, 0)
            one(i, 1)

    def send_row(u, j, first=0, count=16):
        p = dests[j]
        return pltpu.make_async_remote_copy(
            src_ref=xbuf.at[u * 7 + 3 + p, pl.ds(first, count)], dst_ref=xbuf.at[u * 7 + 3 - p, pl.ds(first, count)],
            send_sem=s1.at[u * 3 + j], recv_sem=d1.at[u * 3 + 3 - p],
            device_id={"row": lax.rem(row + p, 4)}, device_id_type=MESH)

    def wait_row(u, slot):
        part = xbuf.at[u * 7 + slot]
        pltpu.make_async_remote_copy(
            src_ref=part, dst_ref=part, send_sem=s1.at[u * 3], recv_sem=d1.at[u * 3 + slot],
            device_id={"row": row}, device_id_type=MESH).wait_recv()

    def send_col(u):
        return pltpu.make_async_remote_copy(
            src_ref=b2.at[pl.ds(u * 4 + 2 * other, 2)], dst_ref=r2.at[pl.ds(u * 2, 2)],
            send_sem=s2.at[u], recv_sem=d2.at[u], device_id={"col": other}, device_id_type=MESH)

    def spare(u, h):
        return u if h == 0 else UNITS + u // (UNITS - 1)

    def send_half(u, h, j, first=0, count=16):
        p, at, rows = dests[j], spare(u, h), pl.ds(8 * h + first // 2, count // 2)
        return pltpu.make_async_remote_copy(
            src_ref=xbuf.at[u * 7 + 3 + p, rows], dst_ref=xbuf.at[u * 7 + 3 - p, rows],
            send_sem=s1.at[at * 3 + j], recv_sem=d1.at[at * 3 + 3 - p],
            device_id={"row": lax.rem(row + p, 4)}, device_id_type=MESH)

    def send_col_half(u, h):
        return pltpu.make_async_remote_copy(
            src_ref=b2.at[u * 4 + 2 * other + h], dst_ref=r2.at[u * 2 + h],
            send_sem=s2.at[spare(u, h)], recv_sem=d2.at[spare(u, h)], device_id={"col": other}, device_id_type=MESH)

    def step_y_half(u, h):
        for slot in range(3):
            part = xbuf.at[u * 7 + slot, pl.ds(8 * h, 8)]
            pltpu.make_async_remote_copy(
                src_ref=part, dst_ref=part, send_sem=s1.at[spare(u, h) * 3], recv_sem=d1.at[spare(u, h) * 3 + slot],
                device_id={"row": row}, device_id_type=MESH).wait_recv()
        slots = [u * 7 + lax.rem(r + 7 - row, 4) for r in range(4)]
        for y2 in range(8):
            a = packed_dft8([xbuf[slots[y1 // 2], 8 * h + 4 * (y1 % 2) + y2 // 2, y2 % 2] for y1 in range(8)])
            for k1 in range(8):
                tr, ti = twiddle(k1 * y2)
                bsc[k1, y2, 0] = a[k1] * tr - rotate(a[k1]) * ti if k1 * y2 else a[k1] * tr
        for k1 in range(8):
            b = packed_dft8([bsc[k1, y2, 0] for y2 in range(8)])
            for k2 in range(8):
                b2[u * 4 + 2 * (k2 // 4) + h, pl.ds(8 * (k1 + 8 * (k2 % 4)), 8), :] = b[k2]
        send_col_half(u, h).start()

    def step_y(u):
        slots = [u * 7 + lax.rem(r + 7 - row, 4) for r in range(4)]
        for y2 in range(8):
            a = dft8([tuple(xbuf[slots[y1 // 2], 8 * (y1 % 2) + y2, q] for q in range(2)) for y1 in range(8)])
            for k1 in range(8):
                vr, vi = times(a[k1], *twiddle(k1 * y2))
                bsc[k1, y2, 0] = vr
                bsc[k1, y2, 1] = vi
        for k1 in range(8):
            b = dft8([(bsc[k1, y2, 0], bsc[k1, y2, 1]) for y2 in range(8)])
            for k2 in range(8):
                for q in range(2):
                    b2[u * 4 + 2 * (k2 // 4) + q, pl.ds(8 * (k1 + 8 * (k2 % 4)), 8), :] = b[k2][q]

    def gather_z(u, dst, split, kxs=range(8)):
        for kx in kxs:
            for q in range(2):
                plane, first = (kx // 4, 4 * q + kx % 4) if split else (q, kx)
                dst[pl.ds(32 * kx, 32), pl.ds(128 * q, 128)] = b2[u * 4 + 2 * col + plane, pl.ds(first, 32, stride=8), :]
                dst[pl.ds(32 * kx, 32), pl.ds(256 + 128 * q, 128)] = r2[u * 2 + plane, pl.ds(first, 32, stride=8), :]

    def step_z(u):
        @pl.when(u == 0)
        def _():
            for h in range(2):
                send_col_half(0, h).wait_recv()
            gather_z(0, lsc, True)

        @pl.when(u > 0)
        def _():
            send_col(u).wait_recv()
            gather_z(u, lsc, False)

        gain = gv[pl.ds(pl.multiple_of(256 * lax.rem(u, 2), 256), 256), :]
        lane_product(lsc, wv, gain, outr, outi, lambda f: (PACK * (u // 2) + f, pl.ds(8 * lax.rem(u, 2), 8)))

    consts[0].wait()
    for i, (first, count) in enumerate(pieces):
        piece(i, 0).wait()
        piece(i, 1).wait()
        step_x(0, first, count, packed=0)
        if i == 0:
            pl.semaphore_wait(barrier, 4)
        send_half(0, 0, 1, first, count).start()
    send_half(0, 0, 0).start()
    send_half(0, 0, 2).start()
    for j in range(3):
        send_half(0, 1, j).start()
    for j in range(3):
        send_row(1, j).start()

    @pl.loop(1, RING)
    def _(g):
        load(g, 0).start()
        load(g, 1).start()

    for copy in consts[1:]:
        copy.start()
    for h in range(2):
        step_y_half(0, h)
    for k in range(2):
        load(RING, k).start()
        load(1, k).wait()
    step_x(1, 0, 16)
    for u in (2, 3):
        for j in range(3):
            send_row(u, j).start()
    for k in range(2):
        load(RING + 1, k).start()
    for copy in consts[1:]:
        copy.wait()
    gain = gs[...].reshape(512, 64)
    gv[...] = jnp.concatenate([gain, gain], axis=1)

    @pl.loop(1, UNITS + LAG - 1)
    def _(t):
        @pl.when(t < UNITS - 1)
        def _():
            for slot in range(3):
                wait_row(t, slot)
            step_y(t)
            send_col(t).start()

        @pl.when(t == UNITS - 1)
        def _():
            for h in range(2):
                step_y_half(UNITS - 1, h)

        g = (t + 3) // 2

        @pl.when(g < GROUPS)
        def _():
            half = lax.rem(t + 1, 2)

            @pl.when(half == 0)
            def _():
                load(g, 0).wait()
                load(g, 1).wait()

            @pl.when(g < GROUPS - 1)
            def _():
                step_x(g, 8 * half, 8)

            @pl.when(g == GROUPS - 1)
            def _():
                step_x(g, 8 * half, 8, packed=1)

            @pl.when(half == 1)
            def _():
                for j in range(3):
                    send_row(2 * g, j).start()

                @pl.when(g < GROUPS - 1)
                def _():
                    for j in range(3):
                        send_row(2 * g + 1, j).start()

                @pl.when(g == GROUPS - 1)
                def _():
                    for h in range(2):
                        for j in range(3):
                            send_half(UNITS - 1, h, j).start()

                @pl.when(g + RING < GROUPS)
                def _():
                    load(g + RING, 0).start()
                    load(g + RING, 1).start()

        @pl.when(t >= LAG)
        def _():
            u = t - LAG
            step_z(u)

    @pl.loop(1, UNITS - 1)
    def _(u):
        for j in range(3):
            send_row(u, j).wait_send()
        send_col(u).wait_send()

    for u in (0, UNITS - 1):
        for h in range(2):
            for j in range(3):
                send_half(u, h, j).wait_send()
    for h in range(2):
        send_col_half(0, h).wait_send()
    for h in range(2):
        send_col_half(UNITS - 1, h).wait_recv()
        gather_z(UNITS - 1, last, True, range(4 * h, 4 * h + 4))
    for h in range(2):
        send_col_half(UNITS - 1, h).wait_send()


def put(vr, vi, mat, last, gain, outr, outi, lr, li, sem):
    cuts = [(pl.ds(7 * i, 7), slice(None)) for i in range(4)] + [(pl.ds(28, 4), pl.ds(0, 8))]
    copies = [pltpu.make_async_copy(v.at[cut], o.at[cut], sem.at[2 * i + k])
              for i, cut in enumerate(cuts) for k, (v, o) in enumerate(((vr, outr), (vi, outi)))]
    for copy in copies:
        copy.start()
    lane_product(last, mat, gain[256:, :], lr, li, lambda f: f)
    cut = (pl.ds(28, 4), pl.ds(8, 8))
    tail = [pltpu.make_async_copy(v, o.at[cut], sem.at[10 + k]) for k, (v, o) in enumerate(((lr, outr), (li, outi)))]
    for copy in tail:
        copy.start()
    for copy in copies + tail:
        copy.wait()


def solution(mesh):
    f32 = jnp.float32

    def local_forward(u_real, u_imag, g_filter):
        parts = [jnp.transpose(v, (0, 2, 3, 1)).reshape(GROUPS, PACK, 16, 32, 64) for v in (u_real, u_imag)]
        spectrum = pl.pallas_call(
            kernel,
            out_shape=[pltpu.VMEM((32, 16, 32, 64), f32)] * 2 + [
                pltpu.VMEM((512, 512), f32), pltpu.VMEM((256, 512), f32), pltpu.VMEM((512, 128), f32)],
            in_specs=[pl.BlockSpec(memory_space=pltpu.HBM)] * 5,
            out_specs=[pl.BlockSpec(memory_space=pltpu.VMEM)] * 5,
            scratch_shapes=[
                pltpu.VMEM((RING, PACK, 16, 32, 64), f32),
                pltpu.VMEM((RING, PACK, 16, 32, 64), f32),
                pltpu.VMEM((UNITS * 7, 16, 2, 8, 128), f32),
                pltpu.VMEM((UNITS * 4, 256, 128), f32),
                pltpu.VMEM((UNITS * 2, 256, 128), f32),
                pltpu.VMEM((2, 8, 8, 128), f32),
                pltpu.VMEM((16, 32, 64), f32),
                pltpu.VMEM((2, 2, 64, 128), f32),
                pltpu.VMEM((8, 8, 2, 8, 128), f32),
                pltpu.VMEM((256, 512), f32),
                pltpu.SemaphoreType.DMA((2 * RING,)),
                pltpu.SemaphoreType.DMA((8,)),
                pltpu.SemaphoreType.DMA((4,)),
                pltpu.SemaphoreType.DMA((3 * UNITS + 6,)),
                pltpu.SemaphoreType.DMA((3 * UNITS + 6,)),
                pltpu.SemaphoreType.DMA((UNITS + 2,)),
                pltpu.SemaphoreType.DMA((UNITS + 2,)),
            ],
            compiler_params=pltpu.CompilerParams(
                collective_id=0, has_side_effects=True, vmem_limit_bytes=40 * 1024 * 1024),
            name="dft3",
        )(*parts, g_filter, jnp.asarray(lane_matrix()), jnp.asarray(sublane_twiddle()))
        return pl.pallas_call(
            put,
            out_shape=[jax.ShapeDtypeStruct((32, 16, 32, 64), f32)] * 2,
            in_specs=[pl.BlockSpec(memory_space=pltpu.VMEM)] * 5,
            out_specs=[pl.BlockSpec(memory_space=pltpu.HBM)] * 2,
            scratch_shapes=[pltpu.VMEM((PACK, 8, 32, 64), f32)] * 2 + [pltpu.SemaphoreType.DMA((12,))],
            compiler_params=pltpu.CompilerParams(vmem_limit_bytes=8 * 1024 * 1024),
            name="put",
        )(*spectrum)

    field_spec = P("fld", None, "row", "col")
    out_spec = P("fld", "row", "col", None)
    return jax.shard_map(local_forward, mesh=mesh, in_specs=(field_spec, field_spec, P("row", "col", None)),
                         out_specs=(out_spec, out_spec), check_vma=False)
```

```python
import functools
import math

import jax
import jax.numpy as jnp
import numpy as np
from jax import lax
from jax.experimental import pallas as pl
from jax.experimental.pallas import tpu as pltpu
from jax.sharding import PartitionSpec as P

MESH = pl.DeviceIdType.MESH
HALF = math.sqrt(0.5)
GROUPS, PACK, UNITS, RING = 8, 4, 32, 4


def interleave(even, odd):
    return [v for pair in zip(even, odd) for v in pair]


def dft4(b):
    (r0, i0), (r1, i1), (r2, i2), (r3, i3) = b
    sr0, si0, sr1, si1 = r0 + r2, i0 + i2, r0 - r2, i0 - i2
    sr2, si2, sr3, si3 = r1 + r3, i1 + i3, r1 - r3, i1 - i3
    return [(sr0 + sr2, si0 + si2), (sr1 + si3, si1 - sr3), (sr0 - sr2, si0 - si2), (sr1 - si3, si1 + sr3)]


def dft8(a):
    pairs = list(zip(a[:4], a[4:]))
    even = [(vr + wr, vi + wi) for (vr, vi), (wr, wi) in pairs]
    odd = [(vr - wr, vi - wi) for (vr, vi), (wr, wi) in pairs]
    o0, (r1, i1), (r2, i2), (r3, i3) = odd
    odd = [o0, ((r1 + i1) * HALF, (i1 - r1) * HALF), (i2, -r2), ((i3 - r3) * HALF, (r3 + i3) * -HALF)]
    even, odd = dft4(even), dft4(odd)
    return interleave(even, odd)


def rotate(v):
    sign = jnp.where(lax.broadcasted_iota(jnp.int32, v.shape, 0) < 4, 1.0, -1.0)
    return pltpu.roll(v, 4, 0) * sign


def packed_dft4(b):
    b0, b1, b2, b3 = b
    s0, s1, s2, s3 = b0 + b2, b0 - b2, b1 + b3, rotate(b1 - b3)
    return [s0 + s2, s1 + s3, s0 - s2, s1 - s3]


def packed_dft8(a):
    pairs = list(zip(a[:4], a[4:]))
    even = packed_dft4([v + w for v, w in pairs])
    o0, o1, o2, o3 = [v - w for v, w in pairs]
    odd = packed_dft4([o0, (rotate(o1) + o1) * HALF, rotate(o2), (rotate(o3) - o3) * HALF])
    return interleave(even, odd)


def times(a, tr, ti):
    return a[0] * tr - a[1] * ti, a[0] * ti + a[1] * tr


def twiddle(m):
    angle = -2.0 * math.pi * (m % 64) / 64.0
    return math.cos(angle) / 8.0, math.sin(angle) / 8.0


def lane_matrix():
    z, kz = np.arange(64), np.arange(64)
    angle = 2.0 * np.pi * ((z[:, None] * kz[None, :]) % 64) / 64.0
    cos, sin = np.cos(angle) / 8.0, np.sin(angle) / 8.0
    blocks = np.stack([np.concatenate([cos, -sin], 1), np.concatenate([sin, cos], 1)])
    out = np.zeros((2, 2, PACK, 32, PACK, 128))
    for c in range(2):
        for f in range(PACK):
            out[c, :, f, :, f, :] = blocks[:, 32 * c : 32 * c + 32]
    return out.reshape(2, 256, PACK * 128).astype(np.float32)


def sublane_twiddle():
    k1, x2 = np.arange(8), np.arange(8)
    angle = -2.0 * np.pi * (k1[:, None] * x2[None, :]) / 64.0
    both = np.stack([np.cos(angle), np.sin(angle)]) / 8.0
    return np.broadcast_to(both[..., None], (2, 8, 8, 128)).astype(np.float32)


def lane_product(lhs, mat, gain, outr, outi, at):
    for n in range(2):
        w = jnp.dot(lhs[...], mat[:, 256 * n : 256 * n + 256], precision=lax.Precision.HIGHEST,
                    preferred_element_type=jnp.float32)
        for f in range(2):
            pair = w[:, 128 * f : 128 * f + 128] * gain
            outr[at(2 * n + f)] = pair[:, :64].reshape(8, 32, 64)
            outi[at(2 * n + f)] = pair[:, 64:].reshape(8, 32, 64)


def kernel(ur, ui, gf, wz, tw, outr, outi, wv, last, gv, inr, ini, xbuf, b2, r2, tv, gs, asc, bsc, lsc,
           in_sem, q_sem, c_sem, s1, d1, s2, d2):
    row, col = lax.axis_index("row"), lax.axis_index("col")
    core = lax.rem(row, 2)
    dests = [1 + 2 * core, 2 - core, 3 - core]
    other = 1 - col

    barrier = pltpu.get_barrier_semaphore()
    for p in (1, 2, 3):
        pl.semaphore_signal(barrier, inc=1, device_id={"row": lax.rem(row + p, 4)}, device_id_type=MESH)
    pl.semaphore_signal(barrier, inc=1, device_id={"col": other}, device_id_type=MESH)

    def load(g, k):
        src, dst = ((ur, inr), (ui, ini))[k]
        return pltpu.make_async_copy(src.at[g], dst.at[lax.rem(g, RING)], in_sem.at[2 * lax.rem(g, RING) + k])

    pieces = ((0, 2), (2, 2), (4, 4), (8, 8))

    def piece(i, k):
        src, dst = ((ur, inr), (ui, ini))[k]
        part = (0, slice(None), pl.ds(*pieces[i]))
        return pltpu.make_async_copy(src.at[part], dst.at[part], q_sem.at[2 * i + k])

    consts = [
        pltpu.make_async_copy(tw, tv, c_sem.at[0]),
        pltpu.make_async_copy(wz.at[col], wv.at[pl.ds(0, 256)], c_sem.at[1]),
        pltpu.make_async_copy(wz.at[other], wv.at[pl.ds(256, 256)], c_sem.at[2]),
        pltpu.make_async_copy(gf, gs, c_sem.at[3]),
    ]
    for i in range(4):
        piece(i, 0).start()
        piece(i, 1).start()
        if i == 0:
            consts[0].start()

    def step_x(g, first, count):
        ring = lax.rem(g, RING)
        bases = [4 * g * 7 + 3 + lax.rem(k + 4 - row, 4) for k in range(4)]

        def one(i, s):
            y = first + 2 * i + s
            ar = inr[ring, :, y].reshape(PACK * 32, 64).T
            ai = ini[ring, :, y].reshape(PACK * 32, 64).T
            a = dft8([(ar[8 * j : 8 * j + 8], ai[8 * j : 8 * j + 8]) for j in range(8)])
            for k1 in range(8):
                vr, vi = times(a[k1], tv[0, k1], tv[1, k1])
                asc[s, 0, pl.ds(8 * k1, 8), :] = vr
                asc[s, 1, pl.ds(8 * k1, 8), :] = vi
            b = dft8([tuple(asc[s, q, pl.ds(x2, 8, stride=8), :] for q in range(2)) for x2 in range(8)])
            top = lax.broadcasted_iota(jnp.int32, (8, 128), 0) < 4
            for k2, (vr, vi) in enumerate(b):
                at = bases[k2 // 2] + 14 * (k2 % 2)
                xbuf[at, y] = jnp.where(top, vr, pltpu.roll(vi, 4, 0))
                xbuf[at + 7, y] = jnp.where(top, pltpu.roll(vr, 4, 0), vi)

        @pl.loop(0, count // 2)
        def _(i):
            one(i, 0)
            one(i, 1)

    def send_row(u, j, first=0, count=16):
        p = dests[j]
        return pltpu.make_async_remote_copy(
            src_ref=xbuf.at[u * 7 + 3 + p, pl.ds(first, count)], dst_ref=xbuf.at[u * 7 + 3 - p, pl.ds(first, count)],
            send_sem=s1.at[u * 3 + j], recv_sem=d1.at[u * 3 + 3 - p],
            device_id={"row": lax.rem(row + p, 4)}, device_id_type=MESH)

    def wait_row(u, slot):
        part = xbuf.at[u * 7 + slot]
        pltpu.make_async_remote_copy(
            src_ref=part, dst_ref=part, send_sem=s1.at[u * 3], recv_sem=d1.at[u * 3 + slot],
            device_id={"row": row}, device_id_type=MESH).wait_recv()

    def send_col(u):
        return pltpu.make_async_remote_copy(
            src_ref=b2.at[u * 2 + other], dst_ref=r2.at[u],
            send_sem=s2.at[u], recv_sem=d2.at[u], device_id={"col": other}, device_id_type=MESH)

    def step_y(u):
        for slot in range(3):
            wait_row(u, slot)
        slots = [u * 7 + lax.rem(r + 7 - row, 4) for r in range(4)]
        for y2 in range(8):
            a = packed_dft8([xbuf[slots[y1 // 2], 8 * (y1 % 2) + y2] for y1 in range(8)])
            for k1 in range(8):
                tr, ti = twiddle(k1 * y2)
                bsc[k1, y2] = a[k1] * tr - rotate(a[k1]) * ti if k1 * y2 else a[k1] * tr
        for k1 in range(8):
            b = packed_dft8([bsc[k1, y2] for y2 in range(8)])
            for k2 in range(8):
                b2[u * 2 + k2 // 4, pl.ds(8 * (k1 + 8 * (k2 % 4)), 8), :] = b[k2]
        send_col(u).start()

    def gather_z(u, dst):
        send_col(u).wait_recv()
        send_col(u + 1).wait_recv()
        for kx in range(8):
            v = u + kx // 4
            for q in range(2):
                rows = pl.ds(4 * q + kx % 4, 32, stride=8)
                dst[pl.ds(32 * kx, 32), pl.ds(128 * q, 128)] = b2[v * 2 + col, rows, :]
                dst[pl.ds(32 * kx, 32), pl.ds(256 + 128 * q, 128)] = r2[v, rows, :]

    def step_z(m):
        gather_z(2 * m, lsc)
        gain = gv[pl.ds(pl.multiple_of(256 * lax.rem(m, 2), 256), 256), :]
        lane_product(lsc, wv, gain, outr, outi, lambda f: (PACK * (m // 2) + f, pl.ds(8 * lax.rem(m, 2), 8)))

    consts[0].wait()
    for i, (first, count) in enumerate(pieces):
        piece(i, 0).wait()
        piece(i, 1).wait()
        step_x(0, first, count)
        if i == 0:
            pl.semaphore_wait(barrier, 4)
        send_row(0, 1, first, count).start()
    send_row(0, 0).start()
    send_row(0, 2).start()

    def send_rows(first, last):
        @pl.loop(first, last)
        def _(u):
            for j in range(3):
                send_row(u, j).start()

    send_rows(1, 4)

    @pl.loop(1, RING)
    def _(g):
        load(g, 0).start()
        load(g, 1).start()

    for copy in consts[1:]:
        copy.start()
    step_y(0)
    for k in range(2):
        load(RING, k).start()
        load(1, k).wait()
    step_x(1, 0, 16)
    send_rows(4, 8)
    for k in range(2):
        load(RING + 1, k).start()
    for copy in consts[1:]:
        copy.wait()
    gain = gs[...].reshape(512, 64)
    gv[...] = jnp.concatenate([gain, gain], axis=1)

    @pl.loop(1, UNITS)
    def _(t):
        step_y(t)
        g, i = (t + 7) // 4, lax.rem(t + 3, 4)

        @pl.when(g < GROUPS)
        def _():
            @pl.when(i == 0)
            def _():
                load(g, 0).wait()
                load(g, 1).wait()

            step_x(g, 4 * i, 4)

            @pl.when(i == 3)
            def _():
                send_rows(4 * g, 4 * g + 4)

                @pl.when(g + RING < GROUPS)
                def _():
                    load(g + RING, 0).start()
                    load(g + RING, 1).start()

        @pl.when((t >= 3) & (lax.rem(t, 2) == 1))
        def _():
            step_z((t - 3) // 2)

    @pl.loop(0, UNITS)
    def _(u):
        for j in range(3):
            send_row(u, j).wait_send()

    @pl.loop(0, UNITS - 2)
    def _(u):
        send_col(u).wait_send()

    gather_z(UNITS - 2, last)
    send_col(UNITS - 2).wait_send()
    send_col(UNITS - 1).wait_send()


def put(vr, vi, mat, last, gain, outr, outi, lr, li, sem):
    cuts = [(pl.ds(7 * i, 7), slice(None)) for i in range(4)] + [(pl.ds(28, 4), pl.ds(0, 8))]
    copies = [pltpu.make_async_copy(v.at[cut], o.at[cut], sem.at[2 * i + k])
              for i, cut in enumerate(cuts) for k, (v, o) in enumerate(((vr, outr), (vi, outi)))]
    for copy in copies:
        copy.start()
    lane_product(last, mat, gain[256:, :], lr, li, lambda f: f)
    cut = (pl.ds(28, 4), pl.ds(8, 8))
    tail = [pltpu.make_async_copy(v, o.at[cut], sem.at[10 + k]) for k, (v, o) in enumerate(((lr, outr), (li, outi)))]
    for copy in tail:
        copy.start()
    for copy in copies + tail:
        copy.wait()


def solution(mesh):
    f32 = jnp.float32

    def local_forward(u_real, u_imag, g_filter):
        parts = [jnp.transpose(v, (0, 2, 3, 1)).reshape(GROUPS, PACK, 16, 32, 64) for v in (u_real, u_imag)]
        spectrum = pl.pallas_call(
            kernel,
            out_shape=[pltpu.VMEM((32, 16, 32, 64), f32)] * 2 + [
                pltpu.VMEM((512, 512), f32), pltpu.VMEM((256, 512), f32), pltpu.VMEM((512, 128), f32)],
            in_specs=[pl.BlockSpec(memory_space=pltpu.HBM)] * 5,
            out_specs=[pl.BlockSpec(memory_space=pltpu.VMEM)] * 5,
            scratch_shapes=[
                pltpu.VMEM((RING, PACK, 16, 32, 64), f32),
                pltpu.VMEM((RING, PACK, 16, 32, 64), f32),
                pltpu.VMEM((UNITS * 7, 16, 8, 128), f32),
                pltpu.VMEM((UNITS * 2, 256, 128), f32),
                pltpu.VMEM((UNITS, 256, 128), f32),
                pltpu.VMEM((2, 8, 8, 128), f32),
                pltpu.VMEM((16, 32, 64), f32),
                pltpu.VMEM((2, 2, 64, 128), f32),
                pltpu.VMEM((8, 8, 8, 128), f32),
                pltpu.VMEM((256, 512), f32),
                pltpu.SemaphoreType.DMA((2 * RING,)),
                pltpu.SemaphoreType.DMA((8,)),
                pltpu.SemaphoreType.DMA((4,)),
                pltpu.SemaphoreType.DMA((3 * UNITS,)),
                pltpu.SemaphoreType.DMA((3 * UNITS,)),
                pltpu.SemaphoreType.DMA((UNITS,)),
                pltpu.SemaphoreType.DMA((UNITS,)),
            ],
            compiler_params=pltpu.CompilerParams(
                collective_id=0, has_side_effects=True, vmem_limit_bytes=40 * 1024 * 1024),
            name="dft3",
        )(*parts, g_filter, jnp.asarray(lane_matrix()), jnp.asarray(sublane_twiddle()))
        return pl.pallas_call(
            put,
            out_shape=[jax.ShapeDtypeStruct((32, 16, 32, 64), f32)] * 2,
            in_specs=[pl.BlockSpec(memory_space=pltpu.VMEM)] * 5,
            out_specs=[pl.BlockSpec(memory_space=pltpu.HBM)] * 2,
            scratch_shapes=[pltpu.VMEM((PACK, 8, 32, 64), f32)] * 2 + [pltpu.SemaphoreType.DMA((12,))],
            compiler_params=pltpu.CompilerParams(vmem_limit_bytes=8 * 1024 * 1024),
            name="put",
        )(*spectrum)

    field_spec = P("fld", None, "row", "col")
    out_spec = P("fld", "row", "col", None)
    return jax.shard_map(local_forward, mesh=mesh, in_specs=(field_spec, field_spec, P("row", "col", None)),
                         out_specs=(out_spec, out_spec), check_vma=False)
```

```python
import functools
import math

import jax
import jax.numpy as jnp
import numpy as np
from jax import lax
from jax.experimental import pallas as pl
from jax.experimental.pallas import tpu as pltpu
from jax.sharding import PartitionSpec as P

MESH = pl.DeviceIdType.MESH
HALF = math.sqrt(0.5)
GROUPS, PACK, UNITS, RING, LAG = 8, 4, 32, 4, 7


def interleave(even, odd):
    return [v for pair in zip(even, odd) for v in pair]


def dft4(b):
    (r0, i0), (r1, i1), (r2, i2), (r3, i3) = b
    sr0, si0, sr1, si1 = r0 + r2, i0 + i2, r0 - r2, i0 - i2
    sr2, si2, sr3, si3 = r1 + r3, i1 + i3, r1 - r3, i1 - i3
    return [(sr0 + sr2, si0 + si2), (sr1 + si3, si1 - sr3), (sr0 - sr2, si0 - si2), (sr1 - si3, si1 + sr3)]


def dft8(a):
    pairs = list(zip(a[:4], a[4:]))
    even = [(vr + wr, vi + wi) for (vr, vi), (wr, wi) in pairs]
    odd = [(vr - wr, vi - wi) for (vr, vi), (wr, wi) in pairs]
    o0, (r1, i1), (r2, i2), (r3, i3) = odd
    odd = [o0, ((r1 + i1) * HALF, (i1 - r1) * HALF), (i2, -r2), ((i3 - r3) * HALF, (r3 + i3) * -HALF)]
    even, odd = dft4(even), dft4(odd)
    return interleave(even, odd)


def rotate(v):
    sign = jnp.where(lax.broadcasted_iota(jnp.int32, v.shape, 0) < 4, 1.0, -1.0)
    return pltpu.roll(v, 4, 0) * sign


def packed_dft4(b):
    b0, b1, b2, b3 = b
    s0, s1, s2, s3 = b0 + b2, b0 - b2, b1 + b3, rotate(b1 - b3)
    return [s0 + s2, s1 + s3, s0 - s2, s1 - s3]


def packed_dft8(a):
    pairs = list(zip(a[:4], a[4:]))
    even = packed_dft4([v + w for v, w in pairs])
    o0, o1, o2, o3 = [v - w for v, w in pairs]
    odd = packed_dft4([o0, (rotate(o1) + o1) * HALF, rotate(o2), (rotate(o3) - o3) * HALF])
    return interleave(even, odd)


def times(a, tr, ti):
    return a[0] * tr - a[1] * ti, a[0] * ti + a[1] * tr


def twiddle(m):
    angle = -2.0 * math.pi * (m % 64) / 64.0
    return math.cos(angle) / 8.0, math.sin(angle) / 8.0


def lane_matrix():
    z, kz = np.arange(64), np.arange(64)
    angle = 2.0 * np.pi * ((z[:, None] * kz[None, :]) % 64) / 64.0
    cos, sin = np.cos(angle) / 8.0, np.sin(angle) / 8.0
    blocks = np.stack([np.concatenate([cos, -sin], 1), np.concatenate([sin, cos], 1)])
    out = np.zeros((2, 2, PACK, 32, PACK, 128))
    for c in range(2):
        for f in range(PACK):
            out[c, :, f, :, f, :] = blocks[:, 32 * c : 32 * c + 32]
    return out.reshape(2, 256, PACK * 128).astype(np.float32)


def sublane_twiddle():
    k1, x2 = np.arange(8), np.arange(8)
    angle = -2.0 * np.pi * (k1[:, None] * x2[None, :]) / 64.0
    both = np.stack([np.cos(angle), np.sin(angle)]) / 8.0
    return np.broadcast_to(both[..., None], (2, 8, 8, 128)).astype(np.float32)


def lane_product(lhs, mat, gain, outr, outi, at):
    for n in range(2):
        w = jnp.dot(lhs[...], mat[:, 256 * n : 256 * n + 256], precision=lax.Precision.HIGHEST,
                    preferred_element_type=jnp.float32)
        for f in range(2):
            pair = w[:, 128 * f : 128 * f + 128] * gain
            outr[at(2 * n + f)] = pair[:, :64].reshape(8, 32, 64)
            outi[at(2 * n + f)] = pair[:, 64:].reshape(8, 32, 64)


def kernel(ur, ui, gf, wz, tw, outr, outi, wv, last, gv, inr, ini, xbuf, b2, r2, tv, gs, asc, bsc, lsc,
           in_sem, q_sem, c_sem, s1, d1, s2, d2):
    row, col = lax.axis_index("row"), lax.axis_index("col")
    core = lax.rem(row, 2)
    dests = [1 + 2 * core, 2 - core, 3 - core]
    other = 1 - col

    barrier = pltpu.get_barrier_semaphore()
    for p in (1, 2, 3):
        pl.semaphore_signal(barrier, inc=1, device_id={"row": lax.rem(row + p, 4)}, device_id_type=MESH)
    pl.semaphore_signal(barrier, inc=1, device_id={"col": other}, device_id_type=MESH)

    def load(g, k):
        src, dst = ((ur, inr), (ui, ini))[k]
        return pltpu.make_async_copy(src.at[g], dst.at[lax.rem(g, RING)], in_sem.at[2 * lax.rem(g, RING) + k])

    pieces = ((0, 2), (2, 2), (4, 4), (8, 8))

    def piece(i, k):
        src, dst = ((ur, inr), (ui, ini))[k]
        part = (0, slice(None), pl.ds(*pieces[i]))
        return pltpu.make_async_copy(src.at[part], dst.at[part], q_sem.at[2 * i + k])

    consts = [
        pltpu.make_async_copy(tw, tv, c_sem.at[0]),
        pltpu.make_async_copy(wz.at[col], wv.at[pl.ds(0, 256)], c_sem.at[1]),
        pltpu.make_async_copy(wz.at[other], wv.at[pl.ds(256, 256)], c_sem.at[2]),
        pltpu.make_async_copy(gf, gs, c_sem.at[3]),
    ]
    for i in range(4):
        piece(i, 0).start()
        piece(i, 1).start()
        if i == 0:
            consts[0].start()

    def step_x(g, first, count):
        ring = lax.rem(g, RING)
        bases = [4 * g * 7 + 3 + lax.rem(k + 4 - row, 4) for k in range(4)]

        def one(i, s):
            y = first + 2 * i + s
            ar = inr[ring, :, y].reshape(PACK * 32, 64).T
            ai = ini[ring, :, y].reshape(PACK * 32, 64).T
            a = dft8([(ar[8 * j : 8 * j + 8], ai[8 * j : 8 * j + 8]) for j in range(8)])
            for k1 in range(8):
                vr, vi = times(a[k1], tv[0, k1], tv[1, k1])
                asc[s, 0, pl.ds(8 * k1, 8), :] = vr
                asc[s, 1, pl.ds(8 * k1, 8), :] = vi
            b = dft8([tuple(asc[s, q, pl.ds(x2, 8, stride=8), :] for q in range(2)) for x2 in range(8)])
            top = lax.broadcasted_iota(jnp.int32, (8, 128), 0) < 4
            for k2, (vr, vi) in enumerate(b):
                at = bases[k2 // 2] + 14 * (k2 % 2)
                xbuf[at, y] = jnp.where(top, vr, pltpu.roll(vi, 4, 0))
                xbuf[at + 7, y] = jnp.where(top, pltpu.roll(vr, 4, 0), vi)

        @pl.loop(0, count // 2)
        def _(i):
            one(i, 0)
            one(i, 1)

    def send_row(u, j, first=0, count=16):
        p = dests[j]
        return pltpu.make_async_remote_copy(
            src_ref=xbuf.at[u * 7 + 3 + p, pl.ds(first, count)], dst_ref=xbuf.at[u * 7 + 3 - p, pl.ds(first, count)],
            send_sem=s1.at[u * 3 + j], recv_sem=d1.at[u * 3 + 3 - p],
            device_id={"row": lax.rem(row + p, 4)}, device_id_type=MESH)

    def wait_row(u, slot):
        part = xbuf.at[u * 7 + slot]
        pltpu.make_async_remote_copy(
            src_ref=part, dst_ref=part, send_sem=s1.at[u * 3], recv_sem=d1.at[u * 3 + slot],
            device_id={"row": row}, device_id_type=MESH).wait_recv()

    def send_col(u):
        return pltpu.make_async_remote_copy(
            src_ref=b2.at[u * 2 + other], dst_ref=r2.at[u],
            send_sem=s2.at[u], recv_sem=d2.at[u], device_id={"col": other}, device_id_type=MESH)

    def step_y(u):
        for slot in range(3):
            wait_row(u, slot)
        slots = [u * 7 + lax.rem(r + 7 - row, 4) for r in range(4)]
        for y2 in range(8):
            a = packed_dft8([xbuf[slots[y1 // 2], 8 * (y1 % 2) + y2] for y1 in range(8)])
            for k1 in range(8):
                tr, ti = twiddle(k1 * y2)
                bsc[k1, y2] = a[k1] * tr - rotate(a[k1]) * ti if k1 * y2 else a[k1] * tr
        for k1 in range(8):
            b = packed_dft8([bsc[k1, y2] for y2 in range(8)])
            for k2 in range(8):
                b2[u * 2 + k2 // 4, pl.ds(8 * (k1 + 8 * (k2 % 4)), 8), :] = b[k2]
        send_col(u).start()

    def gather_z(u, dst):
        send_col(u).wait_recv()
        send_col(u + 1).wait_recv()
        for kx in range(8):
            v = u + kx // 4
            for q in range(2):
                rows = pl.ds(4 * q + kx % 4, 32, stride=8)
                dst[pl.ds(32 * kx, 32), pl.ds(128 * q, 128)] = b2[v * 2 + col, rows, :]
                dst[pl.ds(32 * kx, 32), pl.ds(256 + 128 * q, 128)] = r2[v, rows, :]

    def step_z(m):
        gather_z(2 * m, lsc)
        gain = gv[pl.ds(pl.multiple_of(256 * lax.rem(m, 2), 256), 256), :]
        lane_product(lsc, wv, gain, outr, outi, lambda f: (PACK * (m // 2) + f, pl.ds(8 * lax.rem(m, 2), 8)))

    consts[0].wait()
    for i, (first, count) in enumerate(pieces):
        piece(i, 0).wait()
        piece(i, 1).wait()
        step_x(0, first, count)
        if i == 0:
            pl.semaphore_wait(barrier, 4)
        send_row(0, 1, first, count).start()
    send_row(0, 0).start()
    send_row(0, 2).start()

    def send_rows(first, last):
        @pl.loop(first, last)
        def _(u):
            for j in range(3):
                send_row(u, j).start()

    send_rows(1, 4)

    @pl.loop(1, RING)
    def _(g):
        load(g, 0).start()
        load(g, 1).start()

    for copy in consts[1:]:
        copy.start()
    step_y(0)
    for k in range(2):
        load(RING, k).start()
        load(1, k).wait()
    step_x(1, 0, 16)
    send_rows(4, 8)
    for k in range(2):
        load(RING + 1, k).start()
    for copy in consts[1:]:
        copy.wait()
    gain = gs[...].reshape(512, 64)
    gv[...] = jnp.concatenate([gain, gain], axis=1)

    @pl.loop(1, UNITS + LAG - 3)
    def _(t):
        @pl.when(t < UNITS)
        def _():
            step_y(t)

        g, i = (t + 7) // 4, lax.rem(t + 3, 4)

        @pl.when(g < GROUPS)
        def _():
            @pl.when(i == 0)
            def _():
                load(g, 0).wait()
                load(g, 1).wait()

            step_x(g, 4 * i, 4)

            @pl.when(i == 3)
            def _():
                send_rows(4 * g, 4 * g + 4)

                @pl.when(g + RING < GROUPS)
                def _():
                    load(g + RING, 0).start()
                    load(g + RING, 1).start()

        @pl.when((t >= LAG) & (lax.rem(t - LAG, 2) == 0))
        def _():
            step_z((t - LAG) // 2)

    @pl.loop(0, UNITS)
    def _(u):
        for j in range(3):
            send_row(u, j).wait_send()

    @pl.loop(0, UNITS - 2)
    def _(u):
        send_col(u).wait_send()

    gather_z(UNITS - 2, last)
    send_col(UNITS - 2).wait_send()
    send_col(UNITS - 1).wait_send()


def put(vr, vi, mat, last, gain, outr, outi, lr, li, sem):
    cuts = [(pl.ds(7 * i, 7), slice(None)) for i in range(4)] + [(pl.ds(28, 4), pl.ds(0, 8))]
    copies = [pltpu.make_async_copy(v.at[cut], o.at[cut], sem.at[2 * i + k])
              for i, cut in enumerate(cuts) for k, (v, o) in enumerate(((vr, outr), (vi, outi)))]
    for copy in copies:
        copy.start()
    lane_product(last, mat, gain[256:, :], lr, li, lambda f: f)
    cut = (pl.ds(28, 4), pl.ds(8, 8))
    tail = [pltpu.make_async_copy(v, o.at[cut], sem.at[10 + k]) for k, (v, o) in enumerate(((lr, outr), (li, outi)))]
    for copy in tail:
        copy.start()
    for copy in copies + tail:
        copy.wait()


def solution(mesh):
    f32 = jnp.float32

    def local_forward(u_real, u_imag, g_filter):
        parts = [jnp.transpose(v, (0, 2, 3, 1)).reshape(GROUPS, PACK, 16, 32, 64) for v in (u_real, u_imag)]
        spectrum = pl.pallas_call(
            kernel,
            out_shape=[pltpu.VMEM((32, 16, 32, 64), f32)] * 2 + [
                pltpu.VMEM((512, 512), f32), pltpu.VMEM((256, 512), f32), pltpu.VMEM((512, 128), f32)],
            in_specs=[pl.BlockSpec(memory_space=pltpu.HBM)] * 5,
            out_specs=[pl.BlockSpec(memory_space=pltpu.VMEM)] * 5,
            scratch_shapes=[
                pltpu.VMEM((RING, PACK, 16, 32, 64), f32),
                pltpu.VMEM((RING, PACK, 16, 32, 64), f32),
                pltpu.VMEM((UNITS * 7, 16, 8, 128), f32),
                pltpu.VMEM((UNITS * 2, 256, 128), f32),
                pltpu.VMEM((UNITS, 256, 128), f32),
                pltpu.VMEM((2, 8, 8, 128), f32),
                pltpu.VMEM((16, 32, 64), f32),
                pltpu.VMEM((2, 2, 64, 128), f32),
                pltpu.VMEM((8, 8, 8, 128), f32),
                pltpu.VMEM((256, 512), f32),
                pltpu.SemaphoreType.DMA((2 * RING,)),
                pltpu.SemaphoreType.DMA((8,)),
                pltpu.SemaphoreType.DMA((4,)),
                pltpu.SemaphoreType.DMA((3 * UNITS,)),
                pltpu.SemaphoreType.DMA((3 * UNITS,)),
                pltpu.SemaphoreType.DMA((UNITS,)),
                pltpu.SemaphoreType.DMA((UNITS,)),
            ],
            compiler_params=pltpu.CompilerParams(
                collective_id=0, has_side_effects=True, vmem_limit_bytes=40 * 1024 * 1024),
            name="dft3",
        )(*parts, g_filter, jnp.asarray(lane_matrix()), jnp.asarray(sublane_twiddle()))
        return pl.pallas_call(
            put,
            out_shape=[jax.ShapeDtypeStruct((32, 16, 32, 64), f32)] * 2,
            in_specs=[pl.BlockSpec(memory_space=pltpu.VMEM)] * 5,
            out_specs=[pl.BlockSpec(memory_space=pltpu.HBM)] * 2,
            scratch_shapes=[pltpu.VMEM((PACK, 8, 32, 64), f32)] * 2 + [pltpu.SemaphoreType.DMA((12,))],
            compiler_params=pltpu.CompilerParams(vmem_limit_bytes=8 * 1024 * 1024),
            name="put",
        )(*spectrum)

    field_spec = P("fld", None, "row", "col")
    out_spec = P("fld", "row", "col", None)
    return jax.shard_map(local_forward, mesh=mesh, in_specs=(field_spec, field_spec, P("row", "col", None)),
                         out_specs=(out_spec, out_spec), check_vma=False)
```

```python
import functools
import math

import jax
import jax.numpy as jnp
import numpy as np
from jax import lax
from jax.experimental import pallas as pl
from jax.experimental.pallas import tpu as pltpu
from jax.sharding import PartitionSpec as P

MESH = pl.DeviceIdType.MESH
HALF = math.sqrt(0.5)
GROUPS, PACK, UNITS, RING, LAG = 8, 4, 32, 4, 7


def interleave(even, odd):
    return [v for pair in zip(even, odd) for v in pair]


def dft4(b):
    (r0, i0), (r1, i1), (r2, i2), (r3, i3) = b
    sr0, si0, sr1, si1 = r0 + r2, i0 + i2, r0 - r2, i0 - i2
    sr2, si2, sr3, si3 = r1 + r3, i1 + i3, r1 - r3, i1 - i3
    return [(sr0 + sr2, si0 + si2), (sr1 + si3, si1 - sr3), (sr0 - sr2, si0 - si2), (sr1 - si3, si1 + sr3)]


def dft8(a):
    pairs = list(zip(a[:4], a[4:]))
    even = [(vr + wr, vi + wi) for (vr, vi), (wr, wi) in pairs]
    odd = [(vr - wr, vi - wi) for (vr, vi), (wr, wi) in pairs]
    o0, (r1, i1), (r2, i2), (r3, i3) = odd
    odd = [o0, ((r1 + i1) * HALF, (i1 - r1) * HALF), (i2, -r2), ((i3 - r3) * HALF, (r3 + i3) * -HALF)]
    even, odd = dft4(even), dft4(odd)
    return interleave(even, odd)


def rotate(v):
    sign = jnp.where(lax.broadcasted_iota(jnp.int32, v.shape, 0) < 4, 1.0, -1.0)
    return pltpu.roll(v, 4, 0) * sign


def packed_dft4(b):
    b0, b1, b2, b3 = b
    s0, s1, s2, s3 = b0 + b2, b0 - b2, b1 + b3, rotate(b1 - b3)
    return [s0 + s2, s1 + s3, s0 - s2, s1 - s3]


def packed_dft8(a):
    pairs = list(zip(a[:4], a[4:]))
    even = packed_dft4([v + w for v, w in pairs])
    o0, o1, o2, o3 = [v - w for v, w in pairs]
    odd = packed_dft4([o0, (rotate(o1) + o1) * HALF, rotate(o2), (rotate(o3) - o3) * HALF])
    return interleave(even, odd)


def times(a, tr, ti):
    return a[0] * tr - a[1] * ti, a[0] * ti + a[1] * tr


def twiddle(m):
    angle = -2.0 * math.pi * (m % 64) / 64.0
    return math.cos(angle) / 8.0, math.sin(angle) / 8.0


def lane_matrix():
    z, kz = np.arange(64), np.arange(64)
    angle = 2.0 * np.pi * ((z[:, None] * kz[None, :]) % 64) / 64.0
    cos, sin = np.cos(angle) / 8.0, np.sin(angle) / 8.0
    blocks = np.stack([np.concatenate([cos, -sin], 1), np.concatenate([sin, cos], 1)])
    out = np.zeros((2, 2, PACK, 32, PACK, 128))
    for c in range(2):
        for f in range(PACK):
            out[c, :, f, :, f, :] = blocks[:, 32 * c : 32 * c + 32]
    return out.reshape(2, 256, PACK * 128).astype(np.float32)


def sublane_twiddle():
    k1, x2 = np.arange(8), np.arange(8)
    angle = -2.0 * np.pi * (k1[:, None] * x2[None, :]) / 64.0
    both = np.stack([np.cos(angle), np.sin(angle)]) / 8.0
    return np.broadcast_to(both[..., None], (2, 8, 8, 128)).astype(np.float32)


def lane_product(lhs, mat, gain, outr, outi, at):
    for n in range(2):
        w = jnp.dot(lhs[...], mat[:, 256 * n : 256 * n + 256], precision=lax.Precision.HIGHEST,
                    preferred_element_type=jnp.float32)
        for f in range(2):
            pair = w[:, 128 * f : 128 * f + 128] * gain
            outr[at(2 * n + f)] = pair[:, :64].reshape(8, 32, 64)
            outi[at(2 * n + f)] = pair[:, 64:].reshape(8, 32, 64)


def kernel(ur, ui, gf, wz, tw, outr, outi, wv, last, gv, inr, ini, xbuf, b2, r2, tv, gs, asc, bsc, lsc,
           in_sem, q_sem, c_sem, s1, d1, s2, d2):
    row, col = lax.axis_index("row"), lax.axis_index("col")
    core = lax.rem(row, 2)
    dests = [1 + 2 * core, 2 - core, 3 - core]
    other = 1 - col

    barrier = pltpu.get_barrier_semaphore()
    for p in (1, 2, 3):
        pl.semaphore_signal(barrier, inc=1, device_id={"row": lax.rem(row + p, 4)}, device_id_type=MESH)
    pl.semaphore_signal(barrier, inc=1, device_id={"col": other}, device_id_type=MESH)

    def load(g, k):
        src, dst = ((ur, inr), (ui, ini))[k]
        return pltpu.make_async_copy(src.at[g], dst.at[lax.rem(g, RING)], in_sem.at[2 * lax.rem(g, RING) + k])

    pieces = ((0, 2), (2, 2), (4, 4), (8, 8))

    def piece(i, k):
        src, dst = ((ur, inr), (ui, ini))[k]
        part = (0, slice(None), pl.ds(*pieces[i]))
        return pltpu.make_async_copy(src.at[part], dst.at[part], q_sem.at[2 * i + k])

    consts = [
        pltpu.make_async_copy(tw, tv, c_sem.at[0]),
        pltpu.make_async_copy(wz.at[col], wv.at[pl.ds(0, 256)], c_sem.at[1]),
        pltpu.make_async_copy(wz.at[other], wv.at[pl.ds(256, 256)], c_sem.at[2]),
        pltpu.make_async_copy(gf, gs, c_sem.at[3]),
    ]
    for i in range(4):
        piece(i, 0).start()
        piece(i, 1).start()
        if i == 0:
            consts[0].start()

    def step_x(g, first, count):
        ring = lax.rem(g, RING)
        bases = [4 * g * 7 + 3 + lax.rem(k + 4 - row, 4) for k in range(4)]

        def one(i, s):
            y = first + 2 * i + s
            ar = inr[ring, :, y].reshape(PACK * 32, 64).T
            ai = ini[ring, :, y].reshape(PACK * 32, 64).T
            a = dft8([(ar[8 * j : 8 * j + 8], ai[8 * j : 8 * j + 8]) for j in range(8)])
            for k1 in range(8):
                vr, vi = times(a[k1], tv[0, k1], tv[1, k1])
                asc[s, 0, pl.ds(8 * k1, 8), :] = vr
                asc[s, 1, pl.ds(8 * k1, 8), :] = vi
            b = dft8([tuple(asc[s, q, pl.ds(x2, 8, stride=8), :] for q in range(2)) for x2 in range(8)])
            top = lax.broadcasted_iota(jnp.int32, (8, 128), 0) < 4
            for k2, (vr, vi) in enumerate(b):
                at = bases[k2 // 2] + 14 * (k2 % 2)
                xbuf[at, y] = jnp.where(top, vr, pltpu.roll(vi, 4, 0))
                xbuf[at + 7, y] = jnp.where(top, pltpu.roll(vr, 4, 0), vi)

        @pl.loop(0, count // 2)
        def _(i):
            one(i, 0)
            one(i, 1)

    def send_row(u, j, first=0, count=16):
        p = dests[j]
        return pltpu.make_async_remote_copy(
            src_ref=xbuf.at[u * 7 + 3 + p, pl.ds(first, count)], dst_ref=xbuf.at[u * 7 + 3 - p, pl.ds(first, count)],
            send_sem=s1.at[u * 3 + j], recv_sem=d1.at[u * 3 + 3 - p],
            device_id={"row": lax.rem(row + p, 4)}, device_id_type=MESH)

    def wait_row(u, slot):
        part = xbuf.at[u * 7 + slot]
        pltpu.make_async_remote_copy(
            src_ref=part, dst_ref=part, send_sem=s1.at[u * 3], recv_sem=d1.at[u * 3 + slot],
            device_id={"row": row}, device_id_type=MESH).wait_recv()

    def send_col(u):
        return pltpu.make_async_remote_copy(
            src_ref=b2.at[u * 2 + other], dst_ref=r2.at[u],
            send_sem=s2.at[u], recv_sem=d2.at[u], device_id={"col": other}, device_id_type=MESH)

    def step_y(u):
        for slot in range(3):
            wait_row(u, slot)
        slots = [u * 7 + lax.rem(r + 7 - row, 4) for r in range(4)]
        for y2 in range(8):
            a = packed_dft8([xbuf[slots[y1 // 2], 8 * (y1 % 2) + y2] for y1 in range(8)])
            for k1 in range(8):
                tr, ti = twiddle(k1 * y2)
                bsc[k1, y2] = a[k1] * tr - rotate(a[k1]) * ti if k1 * y2 else a[k1] * tr
        for k1 in range(8):
            b = packed_dft8([bsc[k1, y2] for y2 in range(8)])
            for k2 in range(8):
                b2[u * 2 + k2 // 4, pl.ds(8 * (k1 + 8 * (k2 % 4)), 8), :] = b[k2]
        send_col(u).start()

    def gather_z(u, dst):
        send_col(u).wait_recv()
        send_col(u + 1).wait_recv()
        for kx in range(8):
            v = u + kx // 4
            for q in range(2):
                rows = pl.ds(4 * q + kx % 4, 32, stride=8)
                dst[pl.ds(32 * kx, 32), pl.ds(128 * q, 128)] = b2[v * 2 + col, rows, :]
                dst[pl.ds(32 * kx, 32), pl.ds(256 + 128 * q, 128)] = r2[v, rows, :]

    def step_z(m):
        gather_z(2 * m, lsc)
        gain = gv[pl.ds(pl.multiple_of(256 * lax.rem(m, 2), 256), 256), :]
        lane_product(lsc, wv, gain, outr, outi, lambda f: (PACK * (m // 2) + f, pl.ds(8 * lax.rem(m, 2), 8)))

    consts[0].wait()
    for i, (first, count) in enumerate(pieces):
        piece(i, 0).wait()
        piece(i, 1).wait()
        step_x(0, first, count)
        if i == 0:
            pl.semaphore_wait(barrier, 4)
        send_row(0, 1, first, count).start()
        send_row(0, 2, first, count).start()
    send_row(0, 0).start()

    def send_rows(first, last):
        @pl.loop(first, last)
        def _(u):
            for j in range(3):
                send_row(u, j).start()

    send_rows(1, 4)

    @pl.loop(1, RING)
    def _(g):
        load(g, 0).start()
        load(g, 1).start()

    for copy in consts[1:]:
        copy.start()
    step_y(0)
    for k in range(2):
        load(RING, k).start()
        load(1, k).wait()
    step_x(1, 0, 16)
    for k in range(2):
        load(RING + 1, k).start()
    for copy in consts[1:]:
        copy.wait()
    gain = gs[...].reshape(512, 64)
    gv[...] = jnp.concatenate([gain, gain], axis=1)

    @pl.loop(1, UNITS + LAG - 3)
    def _(t):
        @pl.when(t < UNITS)
        def _():
            step_y(t)

        @pl.when(t < UNITS - 3)
        def _():
            send_rows(t + 3, t + 4)

        g, i = (t + 7) // 4, lax.rem(t + 3, 4)

        @pl.when(g < GROUPS)
        def _():
            @pl.when(i == 0)
            def _():
                load(g, 0).wait()
                load(g, 1).wait()

            step_x(g, 4 * i, 4)

            @pl.when(i == 3)
            def _():
                @pl.when(g + RING < GROUPS)
                def _():
                    load(g + RING, 0).start()
                    load(g + RING, 1).start()

        @pl.when((t >= LAG) & (lax.rem(t - LAG, 2) == 0))
        def _():
            step_z((t - LAG) // 2)

    @pl.loop(0, UNITS)
    def _(u):
        for j in range(3):
            send_row(u, j).wait_send()

    @pl.loop(0, UNITS - 2)
    def _(u):
        send_col(u).wait_send()

    gather_z(UNITS - 2, last)
    send_col(UNITS - 2).wait_send()
    send_col(UNITS - 1).wait_send()


def put(vr, vi, mat, last, gain, outr, outi, lr, li, sem):
    cuts = [(pl.ds(7 * i, 7), slice(None)) for i in range(4)] + [(pl.ds(28, 4), pl.ds(0, 8))]
    copies = [pltpu.make_async_copy(v.at[cut], o.at[cut], sem.at[2 * i + k])
              for i, cut in enumerate(cuts) for k, (v, o) in enumerate(((vr, outr), (vi, outi)))]
    for copy in copies:
        copy.start()
    lane_product(last, mat, gain[256:, :], lr, li, lambda f: f)
    cut = (pl.ds(28, 4), pl.ds(8, 8))
    tail = [pltpu.make_async_copy(v, o.at[cut], sem.at[10 + k]) for k, (v, o) in enumerate(((lr, outr), (li, outi)))]
    for copy in tail:
        copy.start()
    for copy in copies + tail:
        copy.wait()


def solution(mesh):
    f32 = jnp.float32

    def local_forward(u_real, u_imag, g_filter):
        parts = [jnp.transpose(v, (0, 2, 3, 1)).reshape(GROUPS, PACK, 16, 32, 64) for v in (u_real, u_imag)]
        spectrum = pl.pallas_call(
            kernel,
            out_shape=[pltpu.VMEM((32, 16, 32, 64), f32)] * 2 + [
                pltpu.VMEM((512, 512), f32), pltpu.VMEM((256, 512), f32), pltpu.VMEM((512, 128), f32)],
            in_specs=[pl.BlockSpec(memory_space=pltpu.HBM)] * 5,
            out_specs=[pl.BlockSpec(memory_space=pltpu.VMEM)] * 5,
            scratch_shapes=[
                pltpu.VMEM((RING, PACK, 16, 32, 64), f32),
                pltpu.VMEM((RING, PACK, 16, 32, 64), f32),
                pltpu.VMEM((UNITS * 7, 16, 8, 128), f32),
                pltpu.VMEM((UNITS * 2, 256, 128), f32),
                pltpu.VMEM((UNITS, 256, 128), f32),
                pltpu.VMEM((2, 8, 8, 128), f32),
                pltpu.VMEM((16, 32, 64), f32),
                pltpu.VMEM((2, 2, 64, 128), f32),
                pltpu.VMEM((8, 8, 8, 128), f32),
                pltpu.VMEM((256, 512), f32),
                pltpu.SemaphoreType.DMA((2 * RING,)),
                pltpu.SemaphoreType.DMA((8,)),
                pltpu.SemaphoreType.DMA((4,)),
                pltpu.SemaphoreType.DMA((3 * UNITS,)),
                pltpu.SemaphoreType.DMA((3 * UNITS,)),
                pltpu.SemaphoreType.DMA((UNITS,)),
                pltpu.SemaphoreType.DMA((UNITS,)),
            ],
            compiler_params=pltpu.CompilerParams(
                collective_id=0, has_side_effects=True, vmem_limit_bytes=40 * 1024 * 1024),
            name="dft3",
        )(*parts, g_filter, jnp.asarray(lane_matrix()), jnp.asarray(sublane_twiddle()))
        return pl.pallas_call(
            put,
            out_shape=[jax.ShapeDtypeStruct((32, 16, 32, 64), f32)] * 2,
            in_specs=[pl.BlockSpec(memory_space=pltpu.VMEM)] * 5,
            out_specs=[pl.BlockSpec(memory_space=pltpu.HBM)] * 2,
            scratch_shapes=[pltpu.VMEM((PACK, 8, 32, 64), f32)] * 2 + [pltpu.SemaphoreType.DMA((12,))],
            compiler_params=pltpu.CompilerParams(vmem_limit_bytes=8 * 1024 * 1024),
            name="put",
        )(*spectrum)

    field_spec = P("fld", None, "row", "col")
    out_spec = P("fld", "row", "col", None)
    return jax.shard_map(local_forward, mesh=mesh, in_specs=(field_spec, field_spec, P("row", "col", None)),
                         out_specs=(out_spec, out_spec), check_vma=False)
```

```python
import functools
import math

import jax
import jax.numpy as jnp
import numpy as np
from jax import lax
from jax.experimental import pallas as pl
from jax.experimental.pallas import tpu as pltpu
from jax.sharding import PartitionSpec as P

MESH = pl.DeviceIdType.MESH
HALF = math.sqrt(0.5)
GROUPS, PACK, UNITS, LAG, RING = 8, 4, 16, 2, 4


def dft4(b):
    (r0, i0), (r1, i1), (r2, i2), (r3, i3) = b
    sr0, si0, sr1, si1 = r0 + r2, i0 + i2, r0 - r2, i0 - i2
    sr2, si2, sr3, si3 = r1 + r3, i1 + i3, r1 - r3, i1 - i3
    return [(sr0 + sr2, si0 + si2), (sr1 + si3, si1 - sr3), (sr0 - sr2, si0 - si2), (sr1 - si3, si1 + sr3)]


def dft8(a):
    even = [(a[j][0] + a[j + 4][0], a[j][1] + a[j + 4][1]) for j in range(4)]
    odd = [(a[j][0] - a[j + 4][0], a[j][1] - a[j + 4][1]) for j in range(4)]
    (r1, i1), (r2, i2), (r3, i3) = odd[1:]
    odd = [odd[0], ((r1 + i1) * HALF, (i1 - r1) * HALF), (i2, -r2), ((i3 - r3) * HALF, (r3 + i3) * -HALF)]
    even, odd = dft4(even), dft4(odd)
    return [(even if k % 2 == 0 else odd)[k // 2] for k in range(8)]


def times(a, tr, ti):
    return a[0] * tr - a[1] * ti, a[0] * ti + a[1] * tr


def twiddle(m):
    angle = -2.0 * math.pi * (m % 64) / 64.0
    return math.cos(angle) / 8.0, math.sin(angle) / 8.0


def lane_matrix():
    z, kz = np.arange(64), np.arange(64)
    angle = 2.0 * np.pi * ((z[:, None] * kz[None, :]) % 64) / 64.0
    cos, sin = np.cos(angle) / 8.0, np.sin(angle) / 8.0
    blocks = np.stack([np.concatenate([cos, -sin], 1), np.concatenate([sin, cos], 1)])
    out = np.zeros((2, 2, PACK, 32, PACK, 128))
    for c in range(2):
        for f in range(PACK):
            out[c, :, f, :, f, :] = blocks[:, 32 * c : 32 * c + 32]
    return out.reshape(2, 256, PACK * 128).astype(np.float32)


def sublane_twiddle():
    k1, x2 = np.arange(8), np.arange(8)
    angle = -2.0 * np.pi * (k1[:, None] * x2[None, :]) / 64.0
    both = np.stack([np.cos(angle), np.sin(angle)]) / 8.0
    return np.broadcast_to(both[..., None], (2, 8, 8, 128)).astype(np.float32)


def lane_product(lhs, mat, gain, outr, outi, at):
    for n in range(2):
        w = jnp.dot(lhs[...], mat[:, 256 * n : 256 * n + 256], precision=lax.Precision.HIGHEST,
                    preferred_element_type=jnp.float32)
        for f in range(2):
            pair = w[:, 128 * f : 128 * f + 128] * gain
            outr[at(2 * n + f)] = pair[:, :64].reshape(8, 32, 64)
            outi[at(2 * n + f)] = pair[:, 64:].reshape(8, 32, 64)


def kernel(ur, ui, gf, wz, tw, outr, outi, wv, last, gv, inp, xbuf, b2, r2, tv, gs, asc, bsc, lsc,
           in_sem, q_sem, c_sem, s1, d1, s2, d2):
    row, col = lax.axis_index("row"), lax.axis_index("col")
    core = lax.rem(row, 2)
    dests = [1 + 2 * core, 2 - core, 3 - core]
    other = 1 - col

    def arrived(ref, sem):
        pltpu.make_async_remote_copy(src_ref=ref, dst_ref=ref, send_sem=sem, recv_sem=sem,
                                     device_id={"row": row}, device_id_type=MESH).wait_recv()

    def load(g, k):
        src, dst = (ur, ui)[k], inp.at[k]
        return pltpu.make_async_copy(src.at[g], dst.at[lax.rem(g, RING)], in_sem.at[lax.rem(g, RING)])

    pieces = ((0, 2), (2, 2), (4, 4), (8, 8))

    def piece(i, k):
        src, dst = (ur, ui)[k], inp.at[k]
        part = (0, slice(None), pl.ds(*pieces[i]))
        return pltpu.make_async_copy(src.at[part], dst.at[part], q_sem.at[i])

    consts = [
        pltpu.make_async_copy(tw, tv, c_sem.at[0]),
        pltpu.make_async_copy(wz.at[col], wv.at[pl.ds(0, 256)], c_sem.at[1]),
        pltpu.make_async_copy(wz.at[other], wv.at[pl.ds(256, 256)], c_sem.at[1]),
        pltpu.make_async_copy(gf, gs, c_sem.at[2]),
    ]
    for i in range(4):
        piece(i, 0).start()
        piece(i, 1).start()
        if i == 0:
            consts[0].start()

    barrier = pltpu.get_barrier_semaphore()
    for p in (1, 2, 3):
        pl.semaphore_signal(barrier, inc=1, device_id={"row": lax.rem(row + p, 4)}, device_id_type=MESH)
    pl.semaphore_signal(barrier, inc=1, device_id={"col": other}, device_id_type=MESH)

    def step_x(g, first, count):
        ring = lax.rem(g, RING)
        slots = [3 + lax.rem(k + 4 - row, 4) for k in range(4)]
        bases = [[(2 * g + t) * 7 + slots[k] for t in range(2)] for k in range(4)]

        def one(y, s):
            ar = inp[0, ring, :, y].reshape(PACK * 32, 64).T
            ai = inp[1, ring, :, y].reshape(PACK * 32, 64).T
            a = dft8([(ar[8 * j : 8 * j + 8], ai[8 * j : 8 * j + 8]) for j in range(8)])
            for k1 in range(8):
                vr, vi = times(a[k1], tv[0, k1], tv[1, k1])
                asc[s, 0, pl.ds(8 * k1, 8), :] = vr
                asc[s, 1, pl.ds(8 * k1, 8), :] = vi
            b = dft8([tuple(asc[s, q, pl.ds(x2, 8, stride=8), :] for q in range(2)) for x2 in range(8)])
            for k2 in range(8):
                for q in range(2):
                    xbuf[bases[k2 // 2][k2 % 2], y, q] = b[k2][q]

        @pl.loop(0, count // 2)
        def _(i):
            one(first + 2 * i, 0)
            one(first + 2 * i + 1, 1)

    def send_row(u, j, first=0, count=16):
        p = dests[j]
        return pltpu.make_async_remote_copy(
            src_ref=xbuf.at[u * 7 + 3 + p, pl.ds(first, count)], dst_ref=xbuf.at[u * 7 + 3 - p, pl.ds(first, count)],
            send_sem=s1, recv_sem=d1.at[u],
            device_id={"row": lax.rem(row + p, 4)}, device_id_type=MESH)

    def send_col(u):
        return pltpu.make_async_remote_copy(
            src_ref=b2.at[pl.ds(u * 4 + 2 * other, 2)], dst_ref=r2.at[pl.ds(u * 2, 2)],
            send_sem=s2, recv_sem=d2.at[u], device_id={"col": other}, device_id_type=MESH)

    def step_y(u):
        slots = [u * 7 + lax.rem(r + 7 - row, 4) for r in range(4)]
        for y2 in range(8):
            a = dft8([tuple(xbuf[slots[y1 // 2], 8 * (y1 % 2) + y2, q] for q in range(2)) for y1 in range(8)])
            for k1 in range(8):
                vr, vi = times(a[k1], *twiddle(k1 * y2))
                bsc[k1, y2, 0] = vr
                bsc[k1, y2, 1] = vi
        for k1 in range(8):
            b = dft8([(bsc[k1, y2, 0], bsc[k1, y2, 1]) for y2 in range(8)])
            for k2 in range(8):
                for q in range(2):
                    b2[u * 4 + 2 * (k2 // 4) + q, pl.ds(8 * (k1 + 8 * (k2 % 4)), 8), :] = b[k2][q]

    def gather_z(u, dst):
        for kx in range(8):
            for q in range(2):
                dst[pl.ds(32 * kx, 32), pl.ds(128 * q, 128)] = b2[u * 4 + 2 * col + q, pl.ds(kx, 32, stride=8), :]
                dst[pl.ds(32 * kx, 32), pl.ds(256 + 128 * q, 128)] = r2[u * 2 + q, pl.ds(kx, 32, stride=8), :]

    def step_z(u):
        gather_z(u, lsc)
        gain = gv[pl.ds(pl.multiple_of(256 * lax.rem(u, 2), 256), 256), :]
        lane_product(lsc, wv, gain, outr, outi, lambda f: (PACK * (u // 2) + f, pl.ds(8 * lax.rem(u, 2), 8)))

    consts[0].wait()
    for i, (first, count) in enumerate(pieces):
        arrived(inp.at[:, 0, :, pl.ds(first, count)], q_sem.at[i])
        step_x(0, first, count)
        if i == 0:
            pl.semaphore_wait(barrier, 4)
        send_row(0, 1, first, count).start()
    send_row(0, 0).start()
    send_row(0, 2).start()
    for j in range(3):
        send_row(1, j).start()

    @pl.loop(1, RING)
    def _(g):
        load(g, 0).start()
        load(g, 1).start()

    for copy in consts[1:]:
        copy.start()
    @pl.loop(0, UNITS + LAG - 1)
    def _(t):
        @pl.when(t < UNITS)
        def _():
            arrived(xbuf.at[pl.ds(t * 7, 3)], d1.at[t])
            step_y(t)
            send_col(t).start()

        @pl.when(t == 0)
        def _():
            for k in range(2):
                load(RING, k).start()
            arrived(inp.at[:, 1], in_sem.at[1])
            step_x(1, 0, 16)
            for u in (2, 3):
                for j in range(3):
                    send_row(u, j).start()
            for k in range(2):
                load(RING + 1, k).start()
            arrived(wv, c_sem.at[1])
            consts[3].wait()
            gain = gs[...].reshape(512, 64)
            gv[...] = jnp.concatenate([gain, gain], axis=1)

        g = (t + 3) // 2

        @pl.when((t >= 1) & (g < GROUPS))
        def _():
            half = lax.rem(t + 1, 2)

            @pl.when(half == 0)
            def _():
                arrived(inp.at[:, lax.rem(g, RING)], in_sem.at[lax.rem(g, RING)])

            step_x(g, 8 * half, 8)

            @pl.when(half == 1)
            def _():
                for k in range(2):
                    for j in range(3):
                        send_row(2 * g + k, j).start()

                @pl.when(g + RING < GROUPS)
                def _():
                    load(g + RING, 0).start()
                    load(g + RING, 1).start()

        @pl.when(t >= LAG)
        def _():
            u = t - LAG
            send_col(u).wait_recv()
            step_z(u)

    arrived(xbuf.at[pl.ds(0, 3 * UNITS)], s1)
    send_col(UNITS - 1).wait_recv()
    gather_z(UNITS - 1, last)
    arrived(b2.at[pl.ds(0, 2 * UNITS)], s2)


def put(vr, vi, mat, last, gain, outr, outi, lr, li, sem):
    cuts = [(pl.ds(7 * i, 7), slice(None)) for i in range(4)] + [(pl.ds(28, 4), pl.ds(0, 8))]
    copies = [pltpu.make_async_copy(v.at[cut], o.at[cut], sem) for cut in cuts for v, o in ((vr, outr), (vi, outi))]
    for copy in copies:
        copy.start()
    lane_product(last, mat, gain[256:, :], lr, li, lambda f: f)
    cut = (pl.ds(28, 4), pl.ds(8, 8))
    tail = [pltpu.make_async_copy(v, o.at[cut], sem) for v, o in ((lr, outr), (li, outi))]
    for copy in tail:
        copy.start()
    for copy in copies + tail:
        copy.wait()


def solution(mesh):
    f32 = jnp.float32

    def local_forward(u_real, u_imag, g_filter):
        parts = [jnp.transpose(v, (0, 2, 3, 1)).reshape(GROUPS, PACK, 16, 32, 64) for v in (u_real, u_imag)]
        spectrum = pl.pallas_call(
            kernel,
            out_shape=[pltpu.VMEM((32, 16, 32, 64), f32)] * 2 + [
                pltpu.VMEM((512, 512), f32), pltpu.VMEM((256, 512), f32), pltpu.VMEM((512, 128), f32)],
            in_specs=[pl.BlockSpec(memory_space=pltpu.HBM)] * 5,
            out_specs=[pl.BlockSpec(memory_space=pltpu.VMEM)] * 5,
            scratch_shapes=[
                pltpu.VMEM((2, RING, PACK, 16, 32, 64), f32),
                pltpu.VMEM((UNITS * 7, 16, 2, 8, 128), f32),
                pltpu.VMEM((UNITS * 4, 256, 128), f32),
                pltpu.VMEM((UNITS * 2, 256, 128), f32),
                pltpu.VMEM((2, 8, 8, 128), f32),
                pltpu.VMEM((16, 32, 64), f32),
                pltpu.VMEM((2, 2, 64, 128), f32),
                pltpu.VMEM((8, 8, 2, 8, 128), f32),
                pltpu.VMEM((256, 512), f32),
                pltpu.SemaphoreType.DMA((RING,)),
                pltpu.SemaphoreType.DMA((4,)),
                pltpu.SemaphoreType.DMA((3,)),
                pltpu.SemaphoreType.DMA,
                pltpu.SemaphoreType.DMA((UNITS,)),
                pltpu.SemaphoreType.DMA,
                pltpu.SemaphoreType.DMA((UNITS,)),
            ],
            compiler_params=pltpu.CompilerParams(
                collective_id=0, has_side_effects=True, vmem_limit_bytes=40 * 1024 * 1024),
            name="dft3",
        )(*parts, g_filter, jnp.asarray(lane_matrix()), jnp.asarray(sublane_twiddle()))
        return pl.pallas_call(
            put,
            out_shape=[jax.ShapeDtypeStruct((32, 16, 32, 64), f32)] * 2,
            in_specs=[pl.BlockSpec(memory_space=pltpu.VMEM)] * 5,
            out_specs=[pl.BlockSpec(memory_space=pltpu.HBM)] * 2,
            scratch_shapes=[pltpu.VMEM((PACK, 8, 32, 64), f32)] * 2 + [pltpu.SemaphoreType.DMA],
            compiler_params=pltpu.CompilerParams(vmem_limit_bytes=8 * 1024 * 1024),
            name="put",
        )(*spectrum)

    field_spec = P("fld", None, "row", "col")
    out_spec = P("fld", "row", "col", None)
    return jax.shard_map(local_forward, mesh=mesh, in_specs=(field_spec, field_spec, P("row", "col", None)),
                         out_specs=(out_spec, out_spec), check_vma=False)
```

```python
import functools
import math

import jax
import jax.numpy as jnp
import numpy as np
from jax import lax
from jax.experimental import pallas as pl
from jax.experimental.pallas import tpu as pltpu
from jax.sharding import PartitionSpec as P

MESH = pl.DeviceIdType.MESH
HALF = math.sqrt(0.5)
GROUPS, PACK, UNITS, RING, LAG = 8, 4, 32, 4, 7


def interleave(even, odd):
    return [v for pair in zip(even, odd) for v in pair]


def dft4(b):
    (r0, i0), (r1, i1), (r2, i2), (r3, i3) = b
    sr0, si0, sr1, si1 = r0 + r2, i0 + i2, r0 - r2, i0 - i2
    sr2, si2, sr3, si3 = r1 + r3, i1 + i3, r1 - r3, i1 - i3
    return [(sr0 + sr2, si0 + si2), (sr1 + si3, si1 - sr3), (sr0 - sr2, si0 - si2), (sr1 - si3, si1 + sr3)]


def dft8(a):
    pairs = list(zip(a[:4], a[4:]))
    even = [(vr + wr, vi + wi) for (vr, vi), (wr, wi) in pairs]
    odd = [(vr - wr, vi - wi) for (vr, vi), (wr, wi) in pairs]
    o0, (r1, i1), (r2, i2), (r3, i3) = odd
    odd = [o0, ((r1 + i1) * HALF, (i1 - r1) * HALF), (i2, -r2), ((i3 - r3) * HALF, (r3 + i3) * -HALF)]
    even, odd = dft4(even), dft4(odd)
    return interleave(even, odd)


def rotate(v):
    sign = jnp.where(lax.broadcasted_iota(jnp.int32, v.shape, 0) < 4, 1.0, -1.0)
    return pltpu.roll(v, 4, 0) * sign


def packed_dft4(b):
    b0, b1, b2, b3 = b
    s0, s1, s2, s3 = b0 + b2, b0 - b2, b1 + b3, rotate(b1 - b3)
    return [s0 + s2, s1 + s3, s0 - s2, s1 - s3]


def packed_dft8(a):
    pairs = list(zip(a[:4], a[4:]))
    even = packed_dft4([v + w for v, w in pairs])
    o0, o1, o2, o3 = [v - w for v, w in pairs]
    odd = packed_dft4([o0, (rotate(o1) + o1) * HALF, rotate(o2), (rotate(o3) - o3) * HALF])
    return interleave(even, odd)


def times(a, tr, ti):
    return a[0] * tr - a[1] * ti, a[0] * ti + a[1] * tr


def twiddle(m):
    angle = -2.0 * math.pi * (m % 64) / 64.0
    return math.cos(angle) / 8.0, math.sin(angle) / 8.0


def lane_matrix():
    z, kz = np.arange(64), np.arange(64)
    angle = 2.0 * np.pi * ((z[:, None] * kz[None, :]) % 64) / 64.0
    cos, sin = np.cos(angle) / 8.0, np.sin(angle) / 8.0
    blocks = np.stack([np.concatenate([cos, -sin], 1), np.concatenate([sin, cos], 1)])
    out = np.zeros((2, 2, PACK, 32, PACK, 128))
    for c in range(2):
        for f in range(PACK):
            out[c, :, f, :, f, :] = blocks[:, 32 * c : 32 * c + 32]
    return out.reshape(2, 256, PACK * 128).astype(np.float32)


def sublane_twiddle():
    k1, x2 = np.arange(8), np.arange(8)
    angle = -2.0 * np.pi * (k1[:, None] * x2[None, :]) / 64.0
    both = np.stack([np.cos(angle), np.sin(angle)]) / 8.0
    return np.broadcast_to(both[..., None], (2, 8, 8, 128)).astype(np.float32)


def lane_product(lhs, mat, gain, outr, outi, at):
    for n in range(2):
        w = jnp.dot(lhs[...], mat[:, 256 * n : 256 * n + 256], precision=lax.Precision.HIGHEST,
                    preferred_element_type=jnp.float32)
        for f in range(2):
            pair = w[:, 128 * f : 128 * f + 128] * gain
            outr[at(2 * n + f)] = pair[:, :64].reshape(8, 32, 64)
            outi[at(2 * n + f)] = pair[:, 64:].reshape(8, 32, 64)


def kernel(ur, ui, gf, wz, tw, outr, outi, wv, last, gv, inp, xbuf, b2, r2, tv, gs, asc, bsc, lsc,
           in_sem, q_sem, c_sem, s1, d1, s2, d2):
    row, col = lax.axis_index("row"), lax.axis_index("col")
    core = lax.rem(row, 2)
    dests = [1 + 2 * core, 2 - core, 3 - core]
    other = 1 - col

    def arrived(ref, sem):
        pltpu.make_async_remote_copy(src_ref=ref, dst_ref=ref, send_sem=sem, recv_sem=sem,
                                     device_id={"row": row}, device_id_type=MESH).wait_recv()

    def load(g, k):
        src, dst = (ur, ui)[k], inp.at[k]
        return pltpu.make_async_copy(src.at[g], dst.at[lax.rem(g, RING)], in_sem.at[lax.rem(g, RING)])

    pieces = ((0, 2), (2, 2), (4, 4), (8, 8))

    def piece(i, k):
        src, dst = (ur, ui)[k], inp.at[k]
        part = (0, slice(None), pl.ds(*pieces[i]))
        return pltpu.make_async_copy(src.at[part], dst.at[part], q_sem.at[i])

    consts = [
        pltpu.make_async_copy(tw, tv, c_sem.at[0]),
        pltpu.make_async_copy(wz.at[col], wv.at[pl.ds(0, 256)], c_sem.at[1]),
        pltpu.make_async_copy(wz.at[other], wv.at[pl.ds(256, 256)], c_sem.at[1]),
        pltpu.make_async_copy(gf, gs, c_sem.at[2]),
    ]
    for i in range(4):
        piece(i, 0).start()
        piece(i, 1).start()
        if i == 0:
            consts[0].start()

    barrier = pltpu.get_barrier_semaphore()
    for p in (1, 2, 3):
        pl.semaphore_signal(barrier, inc=1, device_id={"row": lax.rem(row + p, 4)}, device_id_type=MESH)
    pl.semaphore_signal(barrier, inc=1, device_id={"col": other}, device_id_type=MESH)

    def step_x(g, first, count):
        ring = lax.rem(g, RING)
        bases = [4 * g * 7 + 3 + lax.rem(k + 4 - row, 4) for k in range(4)]

        def one(i, s):
            y = first + 2 * i + s
            ar = inp[0, ring, :, y].reshape(PACK * 32, 64).T
            ai = inp[1, ring, :, y].reshape(PACK * 32, 64).T
            a = dft8([(ar[8 * j : 8 * j + 8], ai[8 * j : 8 * j + 8]) for j in range(8)])
            for k1 in range(8):
                vr, vi = times(a[k1], tv[0, k1], tv[1, k1])
                asc[s, 0, pl.ds(8 * k1, 8), :] = vr
                asc[s, 1, pl.ds(8 * k1, 8), :] = vi
            b = dft8([tuple(asc[s, q, pl.ds(x2, 8, stride=8), :] for q in range(2)) for x2 in range(8)])
            top = lax.broadcasted_iota(jnp.int32, (8, 128), 0) < 4
            for k2, (vr, vi) in enumerate(b):
                at = bases[k2 // 2] + 14 * (k2 % 2)
                xbuf[at, y] = jnp.where(top, vr, pltpu.roll(vi, 4, 0))
                xbuf[at + 7, y] = jnp.where(top, pltpu.roll(vr, 4, 0), vi)

        @pl.loop(0, count // 2)
        def _(i):
            one(i, 0)
            one(i, 1)

    def send_row(u, j, first=0, count=16):
        p = dests[j]
        return pltpu.make_async_remote_copy(
            src_ref=xbuf.at[u * 7 + 3 + p, pl.ds(first, count)], dst_ref=xbuf.at[u * 7 + 3 - p, pl.ds(first, count)],
            send_sem=s1, recv_sem=d1.at[u],
            device_id={"row": lax.rem(row + p, 4)}, device_id_type=MESH)

    def send_col(u):
        return pltpu.make_async_remote_copy(
            src_ref=b2.at[u * 2 + other], dst_ref=r2.at[u],
            send_sem=s2, recv_sem=d2.at[u], device_id={"col": other}, device_id_type=MESH)

    def step_y(u):
        arrived(xbuf.at[pl.ds(u * 7, 3)], d1.at[u])
        slots = [u * 7 + lax.rem(r + 7 - row, 4) for r in range(4)]
        for y2 in range(8):
            a = packed_dft8([xbuf[slots[y1 // 2], 8 * (y1 % 2) + y2] for y1 in range(8)])
            for k1 in range(8):
                tr, ti = twiddle(k1 * y2)
                bsc[k1, y2] = a[k1] * tr - rotate(a[k1]) * ti if k1 * y2 else a[k1] * tr
        for k1 in range(8):
            b = packed_dft8([bsc[k1, y2] for y2 in range(8)])
            for k2 in range(8):
                b2[u * 2 + k2 // 4, pl.ds(8 * (k1 + 8 * (k2 % 4)), 8), :] = b[k2]
        send_col(u).start()

    def gather_z(u, dst):
        send_col(u).wait_recv()
        send_col(u + 1).wait_recv()
        for kx in range(8):
            v = u + kx // 4
            for q in range(2):
                rows = pl.ds(4 * q + kx % 4, 32, stride=8)
                dst[pl.ds(32 * kx, 32), pl.ds(128 * q, 128)] = b2[v * 2 + col, rows, :]
                dst[pl.ds(32 * kx, 32), pl.ds(256 + 128 * q, 128)] = r2[v, rows, :]

    def step_z(m):
        gather_z(2 * m, lsc)
        gain = gv[pl.ds(pl.multiple_of(256 * lax.rem(m, 2), 256), 256), :]
        lane_product(lsc, wv, gain, outr, outi, lambda f: (PACK * (m // 2) + f, pl.ds(8 * lax.rem(m, 2), 8)))

    consts[0].wait()
    for i, (first, count) in enumerate(pieces):
        arrived(inp.at[:, 0, :, pl.ds(first, count)], q_sem.at[i])
        step_x(0, first, count)
        if i == 0:
            pl.semaphore_wait(barrier, 4)
        send_row(0, 1, first, count).start()
    send_row(0, 0).start()
    send_row(0, 2).start()

    def send_rows(first, last):
        @pl.loop(first, last)
        def _(u):
            for j in range(3):
                send_row(u, j).start()

    send_rows(1, 4)

    @pl.loop(1, RING)
    def _(g):
        load(g, 0).start()
        load(g, 1).start()

    for copy in consts[1:]:
        copy.start()
    step_y(0)
    for k in range(2):
        load(RING, k).start()
    arrived(inp.at[:, 1], in_sem.at[1])
    step_x(1, 0, 16)
    send_rows(4, 8)
    for k in range(2):
        load(RING + 1, k).start()
    arrived(wv, c_sem.at[1])
    consts[3].wait()
    gain = gs[...].reshape(512, 64)
    gv[...] = jnp.concatenate([gain, gain], axis=1)

    @pl.loop(1, UNITS + LAG - 3)
    def _(t):
        @pl.when(t < UNITS)
        def _():
            step_y(t)

        g, i = (t + 7) // 4, lax.rem(t + 3, 4)

        @pl.when(g < GROUPS)
        def _():
            @pl.when(i == 0)
            def _():
                arrived(inp.at[:, lax.rem(g, RING)], in_sem.at[lax.rem(g, RING)])

            step_x(g, 4 * i, 4)

            @pl.when(i == 3)
            def _():
                send_rows(4 * g, 4 * g + 4)

                @pl.when(g + RING < GROUPS)
                def _():
                    load(g + RING, 0).start()
                    load(g + RING, 1).start()

        @pl.when((t >= LAG) & (lax.rem(t - LAG, 2) == 0))
        def _():
            step_z((t - LAG) // 2)

    arrived(xbuf.at[pl.ds(0, 3 * UNITS)], s1)
    gather_z(UNITS - 2, last)
    arrived(b2.at[pl.ds(0, UNITS)], s2)


def put(vr, vi, mat, last, gain, outr, outi, lr, li, sem):
    cuts = [(pl.ds(7 * i, 7), slice(None)) for i in range(4)] + [(pl.ds(28, 4), pl.ds(0, 8))]
    copies = [pltpu.make_async_copy(v.at[cut], o.at[cut], sem) for cut in cuts for v, o in ((vr, outr), (vi, outi))]
    for copy in copies:
        copy.start()
    lane_product(last, mat, gain[256:, :], lr, li, lambda f: f)
    cut = (pl.ds(28, 4), pl.ds(8, 8))
    tail = [pltpu.make_async_copy(v, o.at[cut], sem) for v, o in ((lr, outr), (li, outi))]
    for copy in tail:
        copy.start()
    for copy in copies + tail:
        copy.wait()


def solution(mesh):
    f32 = jnp.float32

    def local_forward(u_real, u_imag, g_filter):
        parts = [jnp.transpose(v, (0, 2, 3, 1)).reshape(GROUPS, PACK, 16, 32, 64) for v in (u_real, u_imag)]
        spectrum = pl.pallas_call(
            kernel,
            out_shape=[pltpu.VMEM((32, 16, 32, 64), f32)] * 2 + [
                pltpu.VMEM((512, 512), f32), pltpu.VMEM((256, 512), f32), pltpu.VMEM((512, 128), f32)],
            in_specs=[pl.BlockSpec(memory_space=pltpu.HBM)] * 5,
            out_specs=[pl.BlockSpec(memory_space=pltpu.VMEM)] * 5,
            scratch_shapes=[
                pltpu.VMEM((2, RING, PACK, 16, 32, 64), f32),
                pltpu.VMEM((UNITS * 7, 16, 8, 128), f32),
                pltpu.VMEM((UNITS * 2, 256, 128), f32),
                pltpu.VMEM((UNITS, 256, 128), f32),
                pltpu.VMEM((2, 8, 8, 128), f32),
                pltpu.VMEM((16, 32, 64), f32),
                pltpu.VMEM((2, 2, 64, 128), f32),
                pltpu.VMEM((8, 8, 8, 128), f32),
                pltpu.VMEM((256, 512), f32),
                pltpu.SemaphoreType.DMA((RING,)),
                pltpu.SemaphoreType.DMA((4,)),
                pltpu.SemaphoreType.DMA((3,)),
                pltpu.SemaphoreType.DMA,
                pltpu.SemaphoreType.DMA((UNITS,)),
                pltpu.SemaphoreType.DMA,
                pltpu.SemaphoreType.DMA((UNITS,)),
            ],
            compiler_params=pltpu.CompilerParams(
                collective_id=0, has_side_effects=True, vmem_limit_bytes=40 * 1024 * 1024),
            name="dft3",
        )(*parts, g_filter, jnp.asarray(lane_matrix()), jnp.asarray(sublane_twiddle()))
        return pl.pallas_call(
            put,
            out_shape=[jax.ShapeDtypeStruct((32, 16, 32, 64), f32)] * 2,
            in_specs=[pl.BlockSpec(memory_space=pltpu.VMEM)] * 5,
            out_specs=[pl.BlockSpec(memory_space=pltpu.HBM)] * 2,
            scratch_shapes=[pltpu.VMEM((PACK, 8, 32, 64), f32)] * 2 + [pltpu.SemaphoreType.DMA],
            compiler_params=pltpu.CompilerParams(vmem_limit_bytes=8 * 1024 * 1024),
            name="put",
        )(*spectrum)

    field_spec = P("fld", None, "row", "col")
    out_spec = P("fld", "row", "col", None)
    return jax.shard_map(local_forward, mesh=mesh, in_specs=(field_spec, field_spec, P("row", "col", None)),
                         out_specs=(out_spec, out_spec), check_vma=False)
```

```python
import functools
import math

import jax
import jax.numpy as jnp
import numpy as np
from jax import lax
from jax.experimental import pallas as pl
from jax.experimental.pallas import tpu as pltpu
from jax.sharding import PartitionSpec as P

MESH = pl.DeviceIdType.MESH
HALF = math.sqrt(0.5)
GROUPS, PACK, UNITS, RING, LAG = 8, 4, 32, 4, 5


def interleave(even, odd):
    return [v for pair in zip(even, odd) for v in pair]


def dft4(b):
    (r0, i0), (r1, i1), (r2, i2), (r3, i3) = b
    sr0, si0, sr1, si1 = r0 + r2, i0 + i2, r0 - r2, i0 - i2
    sr2, si2, sr3, si3 = r1 + r3, i1 + i3, r1 - r3, i1 - i3
    return [(sr0 + sr2, si0 + si2), (sr1 + si3, si1 - sr3), (sr0 - sr2, si0 - si2), (sr1 - si3, si1 + sr3)]


def dft8(a):
    pairs = list(zip(a[:4], a[4:]))
    even = [(vr + wr, vi + wi) for (vr, vi), (wr, wi) in pairs]
    odd = [(vr - wr, vi - wi) for (vr, vi), (wr, wi) in pairs]
    o0, (r1, i1), (r2, i2), (r3, i3) = odd
    odd = [o0, ((r1 + i1) * HALF, (i1 - r1) * HALF), (i2, -r2), ((i3 - r3) * HALF, (r3 + i3) * -HALF)]
    even, odd = dft4(even), dft4(odd)
    return interleave(even, odd)


def rotate(v):
    sign = jnp.where(lax.broadcasted_iota(jnp.int32, v.shape, 0) < 4, 1.0, -1.0)
    return pltpu.roll(v, 4, 0) * sign


def packed_dft4(b):
    b0, b1, b2, b3 = b
    s0, s1, s2, s3 = b0 + b2, b0 - b2, b1 + b3, rotate(b1 - b3)
    return [s0 + s2, s1 + s3, s0 - s2, s1 - s3]


def packed_dft8(a):
    pairs = list(zip(a[:4], a[4:]))
    even = packed_dft4([v + w for v, w in pairs])
    o0, o1, o2, o3 = [v - w for v, w in pairs]
    odd = packed_dft4([o0, (rotate(o1) + o1) * HALF, rotate(o2), (rotate(o3) - o3) * HALF])
    return interleave(even, odd)


def times(a, tr, ti):
    return a[0] * tr - a[1] * ti, a[0] * ti + a[1] * tr


def twiddle(m):
    angle = -2.0 * math.pi * (m % 64) / 64.0
    return math.cos(angle) / 8.0, math.sin(angle) / 8.0


def lane_matrix():
    z, kz = np.arange(64), np.arange(64)
    angle = 2.0 * np.pi * ((z[:, None] * kz[None, :]) % 64) / 64.0
    cos, sin = np.cos(angle) / 8.0, np.sin(angle) / 8.0
    blocks = np.stack([np.concatenate([cos, -sin], 1), np.concatenate([sin, cos], 1)])
    out = np.zeros((2, 2, PACK, 32, PACK, 128))
    for c in range(2):
        for f in range(PACK):
            out[c, :, f, :, f, :] = blocks[:, 32 * c : 32 * c + 32]
    return out.reshape(2, 256, PACK * 128).astype(np.float32)


def sublane_twiddle():
    k1, x2 = np.arange(8), np.arange(8)
    angle = -2.0 * np.pi * (k1[:, None] * x2[None, :]) / 64.0
    both = np.stack([np.cos(angle), np.sin(angle)]) / 8.0
    return np.broadcast_to(both[..., None], (2, 8, 8, 128)).astype(np.float32)


def lane_product(lhs, mat, gain, outr, outi, at):
    for n in range(2):
        w = jnp.dot(lhs[...], mat[:, 256 * n : 256 * n + 256], precision=lax.Precision.HIGHEST,
                    preferred_element_type=jnp.float32)
        for f in range(2):
            pair = w[:, 128 * f : 128 * f + 128] * gain
            outr[at(2 * n + f)] = pair[:, :64].reshape(8, 32, 64)
            outi[at(2 * n + f)] = pair[:, 64:].reshape(8, 32, 64)


def kernel(ur, ui, gf, wz, tw, outr, outi, wv, last, gv, inp, xbuf, b2, r2, tv, gs, asc, bsc, lsc,
           in_sem, q_sem, c_sem, s1, d1, s2, d2):
    row, col = lax.axis_index("row"), lax.axis_index("col")
    core = lax.rem(row, 2)
    dests = [1 + 2 * core, 2 - core, 3 - core]
    other = 1 - col

    def arrived(ref, sem):
        pltpu.make_async_remote_copy(src_ref=ref, dst_ref=ref, send_sem=sem, recv_sem=sem,
                                     device_id={"row": row}, device_id_type=MESH).wait_recv()

    def load(g, k):
        src, dst = (ur, ui)[k], inp.at[k]
        return pltpu.make_async_copy(src.at[g], dst.at[lax.rem(g, RING)], in_sem.at[lax.rem(g, RING)])

    pieces = ((0, 2), (2, 2), (4, 4), (8, 8))

    def piece(i, k):
        src, dst = (ur, ui)[k], inp.at[k]
        part = (0, slice(None), pl.ds(*pieces[i]))
        return pltpu.make_async_copy(src.at[part], dst.at[part], q_sem.at[i])

    consts = [
        pltpu.make_async_copy(tw, tv, c_sem.at[0]),
        pltpu.make_async_copy(wz.at[col], wv.at[pl.ds(0, 256)], c_sem.at[1]),
        pltpu.make_async_copy(wz.at[other], wv.at[pl.ds(256, 256)], c_sem.at[1]),
        pltpu.make_async_copy(gf, gs, c_sem.at[2]),
    ]
    for i in range(4):
        piece(i, 0).start()
        piece(i, 1).start()
        if i == 0:
            consts[0].start()

    barrier = pltpu.get_barrier_semaphore()
    for p in (1, 2, 3):
        pl.semaphore_signal(barrier, inc=1, device_id={"row": lax.rem(row + p, 4)}, device_id_type=MESH)
    pl.semaphore_signal(barrier, inc=1, device_id={"col": other}, device_id_type=MESH)

    def step_x(g, first, count):
        ring = lax.rem(g, RING)
        bases = [4 * g * 7 + 3 + lax.rem(k + 4 - row, 4) for k in range(4)]

        def one(i, s):
            y = first + 2 * i + s
            ar = inp[0, ring, :, y].reshape(PACK * 32, 64).T
            ai = inp[1, ring, :, y].reshape(PACK * 32, 64).T
            a = dft8([(ar[8 * j : 8 * j + 8], ai[8 * j : 8 * j + 8]) for j in range(8)])
            for k1 in range(8):
                vr, vi = times(a[k1], tv[0, k1], tv[1, k1])
                asc[s, 0, pl.ds(8 * k1, 8), :] = vr
                asc[s, 1, pl.ds(8 * k1, 8), :] = vi
            b = dft8([tuple(asc[s, q, pl.ds(x2, 8, stride=8), :] for q in range(2)) for x2 in range(8)])
            top = lax.broadcasted_iota(jnp.int32, (8, 128), 0) < 4
            for k2, (vr, vi) in enumerate(b):
                at = bases[k2 // 2] + 14 * (k2 % 2)
                xbuf[at, y] = jnp.where(top, vr, pltpu.roll(vi, 4, 0))
                xbuf[at + 7, y] = jnp.where(top, pltpu.roll(vr, 4, 0), vi)

        @pl.loop(0, count // 2)
        def _(i):
            one(i, 0)
            one(i, 1)

    def send_row(u, j, first=0, count=16):
        p = dests[j]
        return pltpu.make_async_remote_copy(
            src_ref=xbuf.at[u * 7 + 3 + p, pl.ds(first, count)], dst_ref=xbuf.at[u * 7 + 3 - p, pl.ds(first, count)],
            send_sem=s1, recv_sem=d1.at[u],
            device_id={"row": lax.rem(row + p, 4)}, device_id_type=MESH)

    def send_col(u):
        return pltpu.make_async_remote_copy(
            src_ref=b2.at[u * 2 + other], dst_ref=r2.at[u],
            send_sem=s2, recv_sem=d2.at[u // 2], device_id={"col": other}, device_id_type=MESH)

    def step_y(u):
        arrived(xbuf.at[pl.ds(u * 7, 3)], d1.at[u])
        slots = [u * 7 + lax.rem(r + 7 - row, 4) for r in range(4)]
        for y2 in range(8):
            a = packed_dft8([xbuf[slots[y1 // 2], 8 * (y1 % 2) + y2] for y1 in range(8)])
            for k1 in range(8):
                tr, ti = twiddle(k1 * y2)
                bsc[k1, y2] = a[k1] * tr - rotate(a[k1]) * ti if k1 * y2 else a[k1] * tr
        for k1 in range(8):
            b = packed_dft8([bsc[k1, y2] for y2 in range(8)])
            for k2 in range(8):
                b2[u * 2 + k2 // 4, pl.ds(8 * (k1 + 8 * (k2 % 4)), 8), :] = b[k2]
        send_col(u).start()

    def gather_z(m, dst):
        def part(lane, plane):
            for kx in range(8):
                for q in range(2):
                    dst[pl.ds(32 * kx, 32), pl.ds(lane + 128 * q, 128)] = plane(2 * m + kx // 4, pl.ds(4 * q + kx % 4, 32, stride=8))

        part(0, lambda u, rows: b2[u * 2 + col, rows, :])
        arrived(r2.at[pl.ds(2 * m, 2)], d2.at[m])
        part(256, lambda u, rows: r2[u, rows, :])

    def step_z(m):
        gather_z(m, lsc)
        gain = gv[pl.ds(pl.multiple_of(256 * lax.rem(m, 2), 256), 256), :]
        lane_product(lsc, wv, gain, outr, outi, lambda f: (PACK * (m // 2) + f, pl.ds(8 * lax.rem(m, 2), 8)))

    consts[0].wait()
    for i, (first, count) in enumerate(pieces):
        arrived(inp.at[:, 0, :, pl.ds(first, count)], q_sem.at[i])
        step_x(0, first, count)
        if i == 0:
            pl.semaphore_wait(barrier, 4)
        send_row(0, 1, first, count).start()
        if i == 1:
            send_row(1, 1, 0, first + count).start()
    send_row(0, 0).start()
    send_row(1, 1, 4, 12).start()
    send_row(1, 0).start()
    send_row(0, 2).start()

    def send_rows(first, last):
        @pl.loop(first, last)
        def _(u):
            send_row(u, 1).start()
            send_row(u, 0).start()
            send_row(u - 1, 2).start()

    send_rows(2, 4)

    @pl.loop(1, RING)
    def _(g):
        load(g, 0).start()
        load(g, 1).start()

    for copy in consts[1:]:
        copy.start()
    step_y(0)
    for k in range(2):
        load(RING, k).start()
    arrived(inp.at[:, 1], in_sem.at[1])
    step_x(1, 0, 16)
    send_rows(4, 8)
    for k in range(2):
        load(RING + 1, k).start()
    arrived(wv, c_sem.at[1])
    consts[3].wait()
    gain = gs[...].reshape(512, 64)
    gv[...] = jnp.concatenate([gain, gain], axis=1)

    @pl.loop(1, UNITS + LAG - 3)
    def _(t):
        @pl.when(t < UNITS)
        def _():
            step_y(t)

        g, i = (t + 7) // 4, lax.rem(t + 3, 4)

        @pl.when(g < GROUPS)
        def _():
            @pl.when(i == 0)
            def _():
                arrived(inp.at[:, lax.rem(g, RING)], in_sem.at[lax.rem(g, RING)])

            step_x(g, 4 * i, 4)

            @pl.when(i == 3)
            def _():
                send_rows(4 * g, 4 * g + 4)

                @pl.when(g == GROUPS - 1)
                def _():
                    send_row(UNITS - 1, 2).start()

                @pl.when(g + RING < GROUPS)
                def _():
                    load(g + RING, 0).start()
                    load(g + RING, 1).start()

        @pl.when((t >= LAG) & (lax.rem(t - LAG, 2) == 0))
        def _():
            step_z((t - LAG) // 2)

    arrived(xbuf.at[pl.ds(0, 3 * UNITS)], s1)
    gather_z(UNITS // 2 - 1, last)
    arrived(b2.at[pl.ds(0, UNITS)], s2)


def put(vr, vi, mat, last, gain, outr, outi, lr, li, sem):
    cuts = [(pl.ds(7 * i, 7), slice(None)) for i in range(4)] + [(pl.ds(28, 4), pl.ds(0, 8))]
    copies = [pltpu.make_async_copy(v.at[cut], o.at[cut], sem) for cut in cuts for v, o in ((vr, outr), (vi, outi))]
    for copy in copies:
        copy.start()
    lane_product(last, mat, gain[256:, :], lr, li, lambda f: f)
    cut = (pl.ds(28, 4), pl.ds(8, 8))
    tail = [pltpu.make_async_copy(v, o.at[cut], sem) for v, o in ((lr, outr), (li, outi))]
    for copy in tail:
        copy.start()
    for copy in copies + tail:
        copy.wait()


def solution(mesh):
    f32 = jnp.float32

    def local_forward(u_real, u_imag, g_filter):
        parts = [jnp.transpose(v, (0, 2, 3, 1)).reshape(GROUPS, PACK, 16, 32, 64) for v in (u_real, u_imag)]
        spectrum = pl.pallas_call(
            kernel,
            out_shape=[pltpu.VMEM((32, 16, 32, 64), f32)] * 2 + [
                pltpu.VMEM((512, 512), f32), pltpu.VMEM((256, 512), f32), pltpu.VMEM((512, 128), f32)],
            in_specs=[pl.BlockSpec(memory_space=pltpu.HBM)] * 5,
            out_specs=[pl.BlockSpec(memory_space=pltpu.VMEM)] * 5,
            scratch_shapes=[
                pltpu.VMEM((2, RING, PACK, 16, 32, 64), f32),
                pltpu.VMEM((UNITS * 7, 16, 8, 128), f32),
                pltpu.VMEM((UNITS * 2, 256, 128), f32),
                pltpu.VMEM((UNITS, 256, 128), f32),
                pltpu.VMEM((2, 8, 8, 128), f32),
                pltpu.VMEM((16, 32, 64), f32),
                pltpu.VMEM((2, 2, 64, 128), f32),
                pltpu.VMEM((8, 8, 8, 128), f32),
                pltpu.VMEM((256, 512), f32),
                pltpu.SemaphoreType.DMA((RING,)),
                pltpu.SemaphoreType.DMA((4,)),
                pltpu.SemaphoreType.DMA((3,)),
                pltpu.SemaphoreType.DMA,
                pltpu.SemaphoreType.DMA((UNITS,)),
                pltpu.SemaphoreType.DMA,
                pltpu.SemaphoreType.DMA((UNITS // 2,)),
            ],
            compiler_params=pltpu.CompilerParams(
                collective_id=0, has_side_effects=True, vmem_limit_bytes=40 * 1024 * 1024),
            name="dft3",
        )(*parts, g_filter, jnp.asarray(lane_matrix()), jnp.asarray(sublane_twiddle()))
        return pl.pallas_call(
            put,
            out_shape=[jax.ShapeDtypeStruct((32, 16, 32, 64), f32)] * 2,
            in_specs=[pl.BlockSpec(memory_space=pltpu.VMEM)] * 5,
            out_specs=[pl.BlockSpec(memory_space=pltpu.HBM)] * 2,
            scratch_shapes=[pltpu.VMEM((PACK, 8, 32, 64), f32)] * 2 + [pltpu.SemaphoreType.DMA],
            compiler_params=pltpu.CompilerParams(vmem_limit_bytes=8 * 1024 * 1024),
            name="put",
        )(*spectrum)

    field_spec = P("fld", None, "row", "col")
    out_spec = P("fld", "row", "col", None)
    return jax.shard_map(local_forward, mesh=mesh, in_specs=(field_spec, field_spec, P("row", "col", None)),
                         out_specs=(out_spec, out_spec), check_vma=False)
```

```python
import functools
import math

import jax
import jax.numpy as jnp
import numpy as np
from jax import lax
from jax.experimental import pallas as pl
from jax.experimental.pallas import tpu as pltpu
from jax.sharding import PartitionSpec as P

MESH = pl.DeviceIdType.MESH
HALF = math.sqrt(0.5)
GROUPS, PACK, UNITS, RING, LAG = 8, 4, 32, 4, 5


def interleave(even, odd):
    return [v for pair in zip(even, odd) for v in pair]


def dft4(b):
    (r0, i0), (r1, i1), (r2, i2), (r3, i3) = b
    sr0, si0, sr1, si1 = r0 + r2, i0 + i2, r0 - r2, i0 - i2
    sr2, si2, sr3, si3 = r1 + r3, i1 + i3, r1 - r3, i1 - i3
    return [(sr0 + sr2, si0 + si2), (sr1 + si3, si1 - sr3), (sr0 - sr2, si0 - si2), (sr1 - si3, si1 + sr3)]


def dft8(a):
    pairs = list(zip(a[:4], a[4:]))
    even = [(vr + wr, vi + wi) for (vr, vi), (wr, wi) in pairs]
    odd = [(vr - wr, vi - wi) for (vr, vi), (wr, wi) in pairs]
    o0, (r1, i1), (r2, i2), (r3, i3) = odd
    odd = [o0, ((r1 + i1) * HALF, (i1 - r1) * HALF), (i2, -r2), ((i3 - r3) * HALF, (r3 + i3) * -HALF)]
    even, odd = dft4(even), dft4(odd)
    return interleave(even, odd)


def rotate(v):
    sign = jnp.where(lax.broadcasted_iota(jnp.int32, v.shape, 0) < 4, 1.0, -1.0)
    return pltpu.roll(v, 4, 0) * sign


def packed_dft4(b):
    b0, b1, b2, b3 = b
    s0, s1, s2, s3 = b0 + b2, b0 - b2, b1 + b3, rotate(b1 - b3)
    return [s0 + s2, s1 + s3, s0 - s2, s1 - s3]


def packed_dft8(a):
    pairs = list(zip(a[:4], a[4:]))
    even = packed_dft4([v + w for v, w in pairs])
    o0, o1, o2, o3 = [v - w for v, w in pairs]
    odd = packed_dft4([o0, (rotate(o1) + o1) * HALF, rotate(o2), (rotate(o3) - o3) * HALF])
    return interleave(even, odd)


def times(a, tr, ti):
    return a[0] * tr - a[1] * ti, a[0] * ti + a[1] * tr


def twiddle(m):
    angle = -2.0 * math.pi * (m % 64) / 64.0
    return math.cos(angle) / 8.0, math.sin(angle) / 8.0


def lane_matrix():
    z, kz = np.arange(64), np.arange(64)
    angle = 2.0 * np.pi * ((z[:, None] * kz[None, :]) % 64) / 64.0
    cos, sin = np.cos(angle) / 8.0, np.sin(angle) / 8.0
    blocks = np.stack([np.concatenate([cos, -sin], 1), np.concatenate([sin, cos], 1)])
    out = np.zeros((2, 2, PACK, 32, PACK, 128))
    for c in range(2):
        for f in range(PACK):
            out[c, :, f, :, f, :] = blocks[:, 32 * c : 32 * c + 32]
    return out.reshape(2, 256, PACK * 128).astype(np.float32)


def sublane_twiddle():
    k1, x2 = np.arange(8), np.arange(8)
    angle = -2.0 * np.pi * (k1[:, None] * x2[None, :]) / 64.0
    both = np.stack([np.cos(angle), np.sin(angle)]) / 8.0
    return np.broadcast_to(both[..., None], (2, 8, 8, 128)).astype(np.float32)


def lane_product(lhs, mat, gain, outr, outi, at):
    for n in range(2):
        w = jnp.dot(lhs[...], mat[:, 256 * n : 256 * n + 256], precision=lax.Precision.HIGHEST,
                    preferred_element_type=jnp.float32)
        for f in range(2):
            pair = w[:, 128 * f : 128 * f + 128] * gain
            outr[at(2 * n + f)] = pair[:, :64].reshape(8, 32, 64)
            outi[at(2 * n + f)] = pair[:, 64:].reshape(8, 32, 64)


def body(ur, ui, gf, wz, tw, outr, outi, wv, last, gv, inp, xbuf, b2, r2, tv, gs, asc, bsc, lsc,
           in_sem, q_sem, c_sem, s1, d1, s2, d2):
    row, col = lax.axis_index("row"), lax.axis_index("col")
    core = lax.rem(row, 2)
    dests = [1 + 2 * core, 2 - core, 3 - core]
    other = 1 - col

    def arrived(ref, sem):
        pltpu.make_async_remote_copy(src_ref=ref, dst_ref=ref, send_sem=sem, recv_sem=sem,
                                     device_id={"row": row}, device_id_type=MESH).wait_recv()

    def load(g, k):
        src, dst = (ur, ui)[k], inp.at[k]
        return pltpu.make_async_copy(src.at[g], dst.at[lax.rem(g, RING)], in_sem.at[lax.rem(g, RING)])

    pieces = ((0, 2), (2, 2), (4, 4), (8, 8))

    def piece(i, k):
        src, dst = (ur, ui)[k], inp.at[k]
        part = (0, slice(None), pl.ds(*pieces[i]))
        return pltpu.make_async_copy(src.at[part], dst.at[part], q_sem.at[i])

    consts = [
        pltpu.make_async_copy(tw, tv, c_sem.at[0]),
        pltpu.make_async_copy(wz.at[col], wv.at[pl.ds(0, 256)], c_sem.at[1]),
        pltpu.make_async_copy(wz.at[other], wv.at[pl.ds(256, 256)], c_sem.at[1]),
        pltpu.make_async_copy(gf, gs, c_sem.at[2]),
    ]
    for i in range(4):
        piece(i, 0).start()
        piece(i, 1).start()
        if i == 0:
            consts[0].start()

    barrier = pltpu.get_barrier_semaphore()
    for p in (1, 2, 3):
        pl.semaphore_signal(barrier, inc=1, device_id={"row": lax.rem(row + p, 4)}, device_id_type=MESH)
    pl.semaphore_signal(barrier, inc=1, device_id={"col": other}, device_id_type=MESH)

    def step_x(g, first, count):
        ring = lax.rem(g, RING)
        bases = [4 * g * 7 + 3 + lax.rem(k + 4 - row, 4) for k in range(4)]

        def one(i, s):
            y = first + 2 * i + s
            ar = inp[0, ring, :, y].reshape(PACK * 32, 64).T
            ai = inp[1, ring, :, y].reshape(PACK * 32, 64).T
            a = dft8([(ar[8 * j : 8 * j + 8], ai[8 * j : 8 * j + 8]) for j in range(8)])
            for k1 in range(8):
                vr, vi = times(a[k1], tv[0, k1], tv[1, k1])
                asc[s, 0, pl.ds(8 * k1, 8), :] = vr
                asc[s, 1, pl.ds(8 * k1, 8), :] = vi
            b = dft8([tuple(asc[s, q, pl.ds(x2, 8, stride=8), :] for q in range(2)) for x2 in range(8)])
            top = lax.broadcasted_iota(jnp.int32, (8, 128), 0) < 4
            for k2, (vr, vi) in enumerate(b):
                at = bases[k2 // 2] + 14 * (k2 % 2)
                xbuf[at, y] = jnp.where(top, vr, pltpu.roll(vi, 4, 0))
                xbuf[at + 7, y] = jnp.where(top, pltpu.roll(vr, 4, 0), vi)

        @pl.loop(0, count // 2)
        def _(i):
            one(i, 0)
            one(i, 1)

    def send_row(u, j, first=0, count=16):
        p = dests[j]
        return pltpu.make_async_remote_copy(
            src_ref=xbuf.at[u * 7 + 3 + p, pl.ds(first, count)], dst_ref=xbuf.at[u * 7 + 3 - p, pl.ds(first, count)],
            send_sem=s1, recv_sem=d1.at[u],
            device_id={"row": lax.rem(row + p, 4)}, device_id_type=MESH)

    def send_col(u):
        return pltpu.make_async_remote_copy(
            src_ref=b2.at[u * 2 + other], dst_ref=r2.at[u],
            send_sem=s2, recv_sem=d2.at[u // 2], device_id={"col": other}, device_id_type=MESH)

    def step_y(u):
        arrived(xbuf.at[pl.ds(u * 7, 3)], d1.at[u])
        slots = [u * 7 + lax.rem(r + 7 - row, 4) for r in range(4)]
        for y2 in range(8):
            a = packed_dft8([xbuf[slots[y1 // 2], 8 * (y1 % 2) + y2] for y1 in range(8)])
            for k1 in range(8):
                tr, ti = twiddle(k1 * y2)
                bsc[k1, y2] = a[k1] * tr - rotate(a[k1]) * ti if k1 * y2 else a[k1] * tr
        for k1 in range(8):
            b = packed_dft8([bsc[k1, y2] for y2 in range(8)])
            for k2 in range(8):
                b2[u * 2 + k2 // 4, pl.ds(8 * (k1 + 8 * (k2 % 4)), 8), :] = b[k2]
        send_col(u).start()

    def gather_z(m, dst):
        def part(lane, plane):
            for kx in range(8):
                for q in range(2):
                    dst[pl.ds(32 * kx, 32), pl.ds(lane + 128 * q, 128)] = plane(2 * m + kx // 4, pl.ds(4 * q + kx % 4, 32, stride=8))

        part(0, lambda u, rows: b2[u * 2 + col, rows, :])
        arrived(r2.at[pl.ds(2 * m, 2)], d2.at[m])
        part(256, lambda u, rows: r2[u, rows, :])

    def step_z(m):
        gather_z(m, lsc)
        gain = gv[pl.ds(pl.multiple_of(256 * lax.rem(m, 2), 256), 256), :]
        lane_product(lsc, wv, gain, outr, outi, lambda f: (PACK * (m // 2) + f, pl.ds(8 * lax.rem(m, 2), 8)))

    consts[0].wait()
    for i, (first, count) in enumerate(pieces):
        arrived(inp.at[:, 0, :, pl.ds(first, count)], q_sem.at[i])
        step_x(0, first, count)
        if i == 0:
            pl.semaphore_wait(barrier, 4)
        send_row(0, 1, first, count).start()
        if i == 1:
            send_row(1, 1, 0, first + count).start()
    send_row(0, 0).start()
    send_row(1, 1, 4, 12).start()
    send_row(1, 0).start()
    send_row(0, 2).start()

    def send_rows(first, last):
        @pl.loop(first, last)
        def _(u):
            send_row(u, 1).start()
            send_row(u, 0).start()
            send_row(u - 1, 2).start()

    send_rows(2, 4)

    @pl.loop(1, RING)
    def _(g):
        load(g, 0).start()
        load(g, 1).start()

    for copy in consts[1:]:
        copy.start()
    step_y(0)
    for k in range(2):
        load(RING, k).start()
    arrived(inp.at[:, 1], in_sem.at[1])
    step_x(1, 0, 16)
    send_rows(4, 8)
    for k in range(2):
        load(RING + 1, k).start()
    arrived(wv, c_sem.at[1])
    consts[3].wait()
    gain = gs[...].reshape(512, 64)
    gv[...] = jnp.concatenate([gain, gain], axis=1)

    @pl.loop(1, UNITS + LAG - 3)
    def _(t):
        @pl.when(t < UNITS)
        def _():
            step_y(t)

        g, i = (t + 7) // 4, lax.rem(t + 3, 4)

        @pl.when(g < GROUPS)
        def _():
            @pl.when(i == 0)
            def _():
                arrived(inp.at[:, lax.rem(g, RING)], in_sem.at[lax.rem(g, RING)])

            step_x(g, 4 * i, 4)

            @pl.when(i == 3)
            def _():
                send_rows(4 * g, 4 * g + 4)

                @pl.when(g == GROUPS - 1)
                def _():
                    send_row(UNITS - 1, 2).start()

                @pl.when(g + RING < GROUPS)
                def _():
                    load(g + RING, 0).start()
                    load(g + RING, 1).start()

        @pl.when((t >= LAG) & (lax.rem(t - LAG, 2) == 0))
        def _():
            step_z((t - LAG) // 2)

    arrived(xbuf.at[pl.ds(0, 3 * UNITS)], s1)
    gather_z(UNITS // 2 - 1, last)
    arrived(b2.at[pl.ds(0, UNITS)], s2)


def kernel(*refs):
    dma = pltpu.SemaphoreType.DMA
    pl.run_scoped(functools.partial(body, *refs), in_sem=dma((RING,)), q_sem=dma((4,)), c_sem=dma((3,)), s1=dma,
                  d1=dma((UNITS,)), s2=dma, d2=dma((UNITS // 2,)))


def put(vr, vi, mat, last, gain, outr, outi, lr, li, sem):
    cuts = [(pl.ds(7 * i, 7), slice(None)) for i in range(4)] + [(pl.ds(28, 4), pl.ds(0, 8))]
    copies = [pltpu.make_async_copy(v.at[cut], o.at[cut], sem) for cut in cuts for v, o in ((vr, outr), (vi, outi))]
    for copy in copies:
        copy.start()
    lane_product(last, mat, gain[256:, :], lr, li, lambda f: f)
    cut = (pl.ds(28, 4), pl.ds(8, 8))
    tail = [pltpu.make_async_copy(v, o.at[cut], sem) for v, o in ((lr, outr), (li, outi))]
    for copy in tail:
        copy.start()
    for copy in copies + tail:
        copy.wait()


def solution(mesh):
    f32 = jnp.float32

    def local_forward(u_real, u_imag, g_filter):
        parts = [jnp.transpose(v, (0, 2, 3, 1)).reshape(GROUPS, PACK, 16, 32, 64) for v in (u_real, u_imag)]
        spectrum = pl.pallas_call(
            kernel,
            out_shape=[pltpu.VMEM((32, 16, 32, 64), f32)] * 2 + [
                pltpu.VMEM((512, 512), f32), pltpu.VMEM((256, 512), f32), pltpu.VMEM((512, 128), f32)],
            in_specs=[pl.BlockSpec(memory_space=pltpu.HBM)] * 5,
            out_specs=[pl.BlockSpec(memory_space=pltpu.VMEM)] * 5,
            scratch_shapes=[
                pltpu.VMEM((2, RING, PACK, 16, 32, 64), f32),
                pltpu.VMEM((UNITS * 7, 16, 8, 128), f32),
                pltpu.VMEM((UNITS * 2, 256, 128), f32),
                pltpu.VMEM((UNITS, 256, 128), f32),
                pltpu.VMEM((2, 8, 8, 128), f32),
                pltpu.VMEM((16, 32, 64), f32),
                pltpu.VMEM((2, 2, 64, 128), f32),
                pltpu.VMEM((8, 8, 8, 128), f32),
                pltpu.VMEM((256, 512), f32),
            ],
            compiler_params=pltpu.CompilerParams(
                collective_id=0, has_side_effects=True, vmem_limit_bytes=40 * 1024 * 1024),
            name="dft3",
        )(*parts, g_filter, jnp.asarray(lane_matrix()), jnp.asarray(sublane_twiddle()))
        return pl.pallas_call(
            put,
            out_shape=[jax.ShapeDtypeStruct((32, 16, 32, 64), f32)] * 2,
            in_specs=[pl.BlockSpec(memory_space=pltpu.VMEM)] * 5,
            out_specs=[pl.BlockSpec(memory_space=pltpu.HBM)] * 2,
            scratch_shapes=[pltpu.VMEM((PACK, 8, 32, 64), f32)] * 2 + [pltpu.SemaphoreType.DMA],
            compiler_params=pltpu.CompilerParams(vmem_limit_bytes=8 * 1024 * 1024),
            name="put",
        )(*spectrum)

    field_spec = P("fld", None, "row", "col")
    out_spec = P("fld", "row", "col", None)
    return jax.shard_map(local_forward, mesh=mesh, in_specs=(field_spec, field_spec, P("row", "col", None)),
                         out_specs=(out_spec, out_spec), check_vma=False)
```

```python
import functools
import math

import jax
import jax.numpy as jnp
import numpy as np
from jax import lax
from jax.experimental import pallas as pl
from jax.experimental.pallas import tpu as pltpu
from jax.sharding import PartitionSpec as P

MESH = pl.DeviceIdType.MESH
HALF = math.sqrt(0.5)
GROUPS, PACK, UNITS, RING, LAG = 8, 4, 32, 4, 5


def interleave(even, odd):
    return [v for pair in zip(even, odd) for v in pair]


def dft4(b):
    (r0, i0), (r1, i1), (r2, i2), (r3, i3) = b
    sr0, si0, sr1, si1 = r0 + r2, i0 + i2, r0 - r2, i0 - i2
    sr2, si2, sr3, si3 = r1 + r3, i1 + i3, r1 - r3, i1 - i3
    return [(sr0 + sr2, si0 + si2), (sr1 + si3, si1 - sr3), (sr0 - sr2, si0 - si2), (sr1 - si3, si1 + sr3)]


def dft8(a):
    pairs = list(zip(a[:4], a[4:]))
    even = [(vr + wr, vi + wi) for (vr, vi), (wr, wi) in pairs]
    odd = [(vr - wr, vi - wi) for (vr, vi), (wr, wi) in pairs]
    o0, (r1, i1), (r2, i2), (r3, i3) = odd
    odd = [o0, ((r1 + i1) * HALF, (i1 - r1) * HALF), (i2, -r2), ((i3 - r3) * HALF, (r3 + i3) * -HALF)]
    even, odd = dft4(even), dft4(odd)
    return interleave(even, odd)


def rotate(v):
    sign = jnp.where(lax.broadcasted_iota(jnp.int32, v.shape, 0) < 4, 1.0, -1.0)
    return pltpu.roll(v, 4, 0) * sign


def packed_dft4(b):
    b0, b1, b2, b3 = b
    s0, s1, s2, s3 = b0 + b2, b0 - b2, b1 + b3, rotate(b1 - b3)
    return [s0 + s2, s1 + s3, s0 - s2, s1 - s3]


def packed_dft8(a):
    pairs = list(zip(a[:4], a[4:]))
    even = packed_dft4([v + w for v, w in pairs])
    o0, o1, o2, o3 = [v - w for v, w in pairs]
    odd = packed_dft4([o0, (rotate(o1) + o1) * HALF, rotate(o2), (rotate(o3) - o3) * HALF])
    return interleave(even, odd)


def times(a, tr, ti):
    return a[0] * tr - a[1] * ti, a[0] * ti + a[1] * tr


def twiddle(m):
    angle = -2.0 * math.pi * (m % 64) / 64.0
    return math.cos(angle) / 8.0, math.sin(angle) / 8.0


def lane_matrix():
    z, kz = np.arange(64), np.arange(64)
    angle = 2.0 * np.pi * ((z[:, None] * kz[None, :]) % 64) / 64.0
    cos, sin = np.cos(angle) / 8.0, np.sin(angle) / 8.0
    blocks = np.stack([np.concatenate([cos, -sin], 1), np.concatenate([sin, cos], 1)])
    out = np.zeros((2, 2, PACK, 32, PACK, 128))
    for c in range(2):
        for f in range(PACK):
            out[c, :, f, :, f, :] = blocks[:, 32 * c : 32 * c + 32]
    return out.reshape(2, 256, PACK * 128).astype(np.float32)


def sublane_twiddle():
    k1, x2 = np.arange(8), np.arange(8)
    angle = -2.0 * np.pi * (k1[:, None] * x2[None, :]) / 64.0
    both = np.stack([np.cos(angle), np.sin(angle)]) / 8.0
    return np.broadcast_to(both[..., None], (2, 8, 8, 128)).astype(np.float32)


def lane_product(lhs, mat, gain, outr, outi, at):
    for n in range(2):
        w = jnp.dot(lhs[...], mat[:, 256 * n : 256 * n + 256], precision=lax.Precision.HIGHEST,
                    preferred_element_type=jnp.float32)
        for f in range(2):
            pair = w[:, 128 * f : 128 * f + 128] * gain
            outr[at(2 * n + f)] = pair[:, :64].reshape(8, 32, 64)
            outi[at(2 * n + f)] = pair[:, 64:].reshape(8, 32, 64)


def body(ur, ui, gf, wz, tw, outr, outi, wv, last, gv, inp, xbuf, b2, r2, tv, gs, asc, bsc, lsc,
           in_sem, q_sem, c_sem, s1, d1, s2, d2):
    row, col = lax.axis_index("row"), lax.axis_index("col")
    core = lax.rem(row, 2)
    dests = [1 + 2 * core, 2 - core, 3 - core]
    other = 1 - col

    def arrived(ref, sem):
        pltpu.make_async_remote_copy(src_ref=ref, dst_ref=ref, send_sem=sem, recv_sem=sem,
                                     device_id={"row": row}, device_id_type=MESH).wait_recv()

    def load(g, k):
        src, dst = (ur, ui)[k], inp.at[k]
        return pltpu.make_async_copy(src.at[g], dst.at[lax.rem(g, RING)], in_sem.at[lax.rem(g, RING)])

    pieces = ((0, 2), (2, 2), (4, 4), (8, 8))

    def piece(i, k):
        src, dst = (ur, ui)[k], inp.at[k]
        part = (0, slice(None), pl.ds(*pieces[i]))
        return pltpu.make_async_copy(src.at[part], dst.at[part], q_sem.at[i])

    consts = [
        pltpu.make_async_copy(tw, tv, c_sem.at[0]),
        pltpu.make_async_copy(wz.at[col], wv.at[pl.ds(0, 256)], c_sem.at[1]),
        pltpu.make_async_copy(wz.at[other], wv.at[pl.ds(256, 256)], c_sem.at[1]),
        pltpu.make_async_copy(gf, gs, c_sem.at[2]),
    ]
    def start_piece(i):
        piece(i, 0).start()
        piece(i, 1).start()

    consts[0].start()
    start_piece(0)
    barrier = pltpu.get_barrier_semaphore()
    for p in (1, 2, 3):
        pl.semaphore_signal(barrier, inc=1, device_id={"row": lax.rem(row + p, 4)}, device_id_type=MESH)
    pl.semaphore_signal(barrier, inc=1, device_id={"col": other}, device_id_type=MESH)
    for i in range(1, 4):
        start_piece(i)

    def step_x(g, first, count):
        ring = lax.rem(g, RING)
        bases = [4 * g * 7 + 3 + lax.rem(k + 4 - row, 4) for k in range(4)]

        def one(i, s):
            y = first + 2 * i + s
            ar = inp[0, ring, :, y].reshape(PACK * 32, 64).T
            ai = inp[1, ring, :, y].reshape(PACK * 32, 64).T
            a = dft8([(ar[8 * j : 8 * j + 8], ai[8 * j : 8 * j + 8]) for j in range(8)])
            for k1 in range(8):
                vr, vi = times(a[k1], tv[0, k1], tv[1, k1])
                asc[s, 0, pl.ds(8 * k1, 8), :] = vr
                asc[s, 1, pl.ds(8 * k1, 8), :] = vi
            b = dft8([tuple(asc[s, q, pl.ds(x2, 8, stride=8), :] for q in range(2)) for x2 in range(8)])
            top = lax.broadcasted_iota(jnp.int32, (8, 128), 0) < 4
            for k2, (vr, vi) in enumerate(b):
                at = bases[k2 // 2] + 14 * (k2 % 2)
                xbuf[at, y] = jnp.where(top, vr, pltpu.roll(vi, 4, 0))
                xbuf[at + 7, y] = jnp.where(top, pltpu.roll(vr, 4, 0), vi)

        @pl.loop(0, count // 2)
        def _(i):
            one(i, 0)
            one(i, 1)

    def send_row(u, j, first=0, count=16):
        p = dests[j]
        return pltpu.make_async_remote_copy(
            src_ref=xbuf.at[u * 7 + 3 + p, pl.ds(first, count)], dst_ref=xbuf.at[u * 7 + 3 - p, pl.ds(first, count)],
            send_sem=s1, recv_sem=d1.at[u],
            device_id={"row": lax.rem(row + p, 4)}, device_id_type=MESH)

    def send_col(u):
        return pltpu.make_async_remote_copy(
            src_ref=b2.at[u * 2 + other], dst_ref=r2.at[u],
            send_sem=s2, recv_sem=d2.at[u // 2], device_id={"col": other}, device_id_type=MESH)

    def step_y(u):
        arrived(xbuf.at[pl.ds(u * 7, 3)], d1.at[u])
        slots = [u * 7 + lax.rem(r + 7 - row, 4) for r in range(4)]
        for y2 in range(8):
            a = packed_dft8([xbuf[slots[y1 // 2], 8 * (y1 % 2) + y2] for y1 in range(8)])
            for k1 in range(8):
                tr, ti = twiddle(k1 * y2)
                bsc[k1, y2] = a[k1] * tr - rotate(a[k1]) * ti if k1 * y2 else a[k1] * tr
        for k1 in range(8):
            b = packed_dft8([bsc[k1, y2] for y2 in range(8)])
            for k2 in range(8):
                b2[u * 2 + k2 // 4, pl.ds(8 * (k1 + 8 * (k2 % 4)), 8), :] = b[k2]
        send_col(u).start()

    def gather_z(m, dst):
        def part(lane, plane):
            for kx in range(8):
                for q in range(2):
                    dst[pl.ds(32 * kx, 32), pl.ds(lane + 128 * q, 128)] = plane(2 * m + kx // 4, pl.ds(4 * q + kx % 4, 32, stride=8))

        part(0, lambda u, rows: b2[u * 2 + col, rows, :])
        arrived(r2.at[pl.ds(2 * m, 2)], d2.at[m])
        part(256, lambda u, rows: r2[u, rows, :])

    def step_z(m):
        gather_z(m, lsc)
        gain = gv[pl.ds(pl.multiple_of(256 * lax.rem(m, 2), 256), 256), :]
        lane_product(lsc, wv, gain, outr, outi, lambda f: (PACK * (m // 2) + f, pl.ds(8 * lax.rem(m, 2), 8)))

    consts[0].wait()
    for i, (first, count) in enumerate(pieces):
        arrived(inp.at[:, 0, :, pl.ds(first, count)], q_sem.at[i])
        step_x(0, first, count)
        if i == 0:
            pl.semaphore_wait(barrier, 4)
        send_row(0, 1, first, count).start()
        if i == 1:
            send_row(1, 1, 0, first + count).start()
    send_row(0, 0).start()
    send_row(1, 1, 4, 12).start()
    send_row(1, 0).start()
    send_row(0, 2).start()

    def send_rows(first, last):
        @pl.loop(first, last)
        def _(u):
            send_row(u, 1).start()
            send_row(u, 0).start()
            send_row(u - 1, 2).start()

    send_rows(2, 4)

    @pl.loop(1, RING)
    def _(g):
        load(g, 0).start()
        load(g, 1).start()

    for copy in consts[1:]:
        copy.start()
    step_y(0)
    for k in range(2):
        load(RING, k).start()
    arrived(inp.at[:, 1], in_sem.at[1])
    step_x(1, 0, 16)
    send_rows(4, 8)
    for k in range(2):
        load(RING + 1, k).start()
    arrived(wv, c_sem.at[1])
    consts[3].wait()
    gain = gs[...].reshape(512, 64)
    gv[...] = jnp.concatenate([gain, gain], axis=1)

    @pl.loop(1, UNITS + LAG - 3)
    def _(t):
        @pl.when(t < UNITS)
        def _():
            step_y(t)

        g, i = (t + 7) // 4, lax.rem(t + 3, 4)

        @pl.when(g < GROUPS)
        def _():
            @pl.when(i == 0)
            def _():
                arrived(inp.at[:, lax.rem(g, RING)], in_sem.at[lax.rem(g, RING)])

            step_x(g, 4 * i, 4)

            @pl.when(i == 3)
            def _():
                send_rows(4 * g, 4 * g + 4)

                @pl.when(g == GROUPS - 1)
                def _():
                    send_row(UNITS - 1, 2).start()

                @pl.when(g + RING < GROUPS)
                def _():
                    load(g + RING, 0).start()
                    load(g + RING, 1).start()

        @pl.when((t >= LAG) & (lax.rem(t - LAG, 2) == 0))
        def _():
            step_z((t - LAG) // 2)

    arrived(xbuf.at[pl.ds(0, 3 * UNITS)], s1)
    gather_z(UNITS // 2 - 1, last)
    arrived(b2.at[pl.ds(0, UNITS)], s2)


def kernel(*refs):
    dma = pltpu.SemaphoreType.DMA
    pl.run_scoped(functools.partial(body, *refs), in_sem=dma((RING,)), q_sem=dma((4,)), c_sem=dma((3,)), s1=dma,
                  d1=dma((UNITS,)), s2=dma, d2=dma((UNITS // 2,)))


def put(vr, vi, mat, last, gain, outr, outi, lr, li, sem):
    cuts = [(pl.ds(7 * i, 7), slice(None)) for i in range(4)] + [(pl.ds(28, 4), pl.ds(0, 8))]
    copies = [pltpu.make_async_copy(v.at[cut], o.at[cut], sem) for cut in cuts for v, o in ((vr, outr), (vi, outi))]
    for copy in copies:
        copy.start()
    lane_product(last, mat, gain[256:, :], lr, li, lambda f: f)
    cut = (pl.ds(28, 4), pl.ds(8, 8))
    tail = [pltpu.make_async_copy(v, o.at[cut], sem) for v, o in ((lr, outr), (li, outi))]
    for copy in tail:
        copy.start()
    for copy in copies + tail:
        copy.wait()


def solution(mesh):
    f32 = jnp.float32

    def local_forward(u_real, u_imag, g_filter):
        parts = [jnp.transpose(v, (0, 2, 3, 1)).reshape(GROUPS, PACK, 16, 32, 64) for v in (u_real, u_imag)]
        spectrum = pl.pallas_call(
            kernel,
            out_shape=[pltpu.VMEM((32, 16, 32, 64), f32)] * 2 + [
                pltpu.VMEM((512, 512), f32), pltpu.VMEM((256, 512), f32), pltpu.VMEM((512, 128), f32)],
            in_specs=[pl.BlockSpec(memory_space=pltpu.HBM)] * 5,
            out_specs=[pl.BlockSpec(memory_space=pltpu.VMEM)] * 5,
            scratch_shapes=[
                pltpu.VMEM((2, RING, PACK, 16, 32, 64), f32),
                pltpu.VMEM((UNITS * 7, 16, 8, 128), f32),
                pltpu.VMEM((UNITS * 2, 256, 128), f32),
                pltpu.VMEM((UNITS, 256, 128), f32),
                pltpu.VMEM((2, 8, 8, 128), f32),
                pltpu.VMEM((16, 32, 64), f32),
                pltpu.VMEM((2, 2, 64, 128), f32),
                pltpu.VMEM((8, 8, 8, 128), f32),
                pltpu.VMEM((256, 512), f32),
            ],
            compiler_params=pltpu.CompilerParams(
                collective_id=0, has_side_effects=True, vmem_limit_bytes=40 * 1024 * 1024),
            name="dft3",
        )(*parts, g_filter, jnp.asarray(lane_matrix()), jnp.asarray(sublane_twiddle()))
        return pl.pallas_call(
            put,
            out_shape=[jax.ShapeDtypeStruct((32, 16, 32, 64), f32)] * 2,
            in_specs=[pl.BlockSpec(memory_space=pltpu.VMEM)] * 5,
            out_specs=[pl.BlockSpec(memory_space=pltpu.HBM)] * 2,
            scratch_shapes=[pltpu.VMEM((PACK, 8, 32, 64), f32)] * 2 + [pltpu.SemaphoreType.DMA],
            compiler_params=pltpu.CompilerParams(vmem_limit_bytes=8 * 1024 * 1024),
            name="put",
        )(*spectrum)

    field_spec = P("fld", None, "row", "col")
    out_spec = P("fld", "row", "col", None)
    return jax.shard_map(local_forward, mesh=mesh, in_specs=(field_spec, field_spec, P("row", "col", None)),
                         out_specs=(out_spec, out_spec), check_vma=False)
```

```python
import functools
import math

import jax
import jax.numpy as jnp
import numpy as np
from jax import lax
from jax.experimental import pallas as pl
from jax.experimental.pallas import tpu as pltpu
from jax.sharding import PartitionSpec as P

MESH = pl.DeviceIdType.MESH
HALF = math.sqrt(0.5)
GROUPS, PACK, UNITS, RING, LAG = 8, 4, 32, 4, 5


def interleave(even, odd):
    return [v for pair in zip(even, odd) for v in pair]


def dft4(b):
    (r0, i0), (r1, i1), (r2, i2), (r3, i3) = b
    sr0, si0, sr1, si1 = r0 + r2, i0 + i2, r0 - r2, i0 - i2
    sr2, si2, sr3, si3 = r1 + r3, i1 + i3, r1 - r3, i1 - i3
    return [(sr0 + sr2, si0 + si2), (sr1 + si3, si1 - sr3), (sr0 - sr2, si0 - si2), (sr1 - si3, si1 + sr3)]


def dft8(a):
    pairs = list(zip(a[:4], a[4:]))
    even = [(vr + wr, vi + wi) for (vr, vi), (wr, wi) in pairs]
    odd = [(vr - wr, vi - wi) for (vr, vi), (wr, wi) in pairs]
    o0, (r1, i1), (r2, i2), (r3, i3) = odd
    odd = [o0, ((r1 + i1) * HALF, (i1 - r1) * HALF), (i2, -r2), ((i3 - r3) * HALF, (r3 + i3) * -HALF)]
    even, odd = dft4(even), dft4(odd)
    return interleave(even, odd)


def rotate(v):
    sign = jnp.where(lax.broadcasted_iota(jnp.int32, v.shape, 0) < 4, 1.0, -1.0)
    return pltpu.roll(v, 4, 0) * sign


def packed_dft4(b):
    b0, b1, b2, b3 = b
    s0, s1, s2, s3 = b0 + b2, b0 - b2, b1 + b3, rotate(b1 - b3)
    return [s0 + s2, s1 + s3, s0 - s2, s1 - s3]


def packed_dft8(a):
    pairs = list(zip(a[:4], a[4:]))
    even = packed_dft4([v + w for v, w in pairs])
    o0, o1, o2, o3 = [v - w for v, w in pairs]
    odd = packed_dft4([o0, (rotate(o1) + o1) * HALF, rotate(o2), (rotate(o3) - o3) * HALF])
    return interleave(even, odd)


def times(a, tr, ti):
    return a[0] * tr - a[1] * ti, a[0] * ti + a[1] * tr


def twiddle(m):
    angle = -2.0 * math.pi * (m % 64) / 64.0
    return math.cos(angle) / 8.0, math.sin(angle) / 8.0


def lane_matrix():
    z, kz = np.arange(64), np.arange(64)
    angle = 2.0 * np.pi * ((z[:, None] * kz[None, :]) % 64) / 64.0
    cos, sin = np.cos(angle) / 8.0, np.sin(angle) / 8.0
    blocks = np.stack([np.concatenate([cos, -sin], 1), np.concatenate([sin, cos], 1)])
    out = np.zeros((2, 2, PACK, 32, PACK, 128))
    for c in range(2):
        for f in range(PACK):
            out[c, :, f, :, f, :] = blocks[:, 32 * c : 32 * c + 32]
    return out.reshape(2, 256, PACK * 128).astype(np.float32)


def sublane_twiddle():
    k1, x2 = np.arange(8), np.arange(8)
    angle = -2.0 * np.pi * (k1[:, None] * x2[None, :]) / 64.0
    both = np.stack([np.cos(angle), np.sin(angle)]) / 8.0
    return np.broadcast_to(both[..., None], (2, 8, 8, 128)).astype(np.float32)


def lane_product(lhs, mat, gain, outr, outi, at):
    for n in range(2):
        w = jnp.dot(lhs[...], mat[:, 256 * n : 256 * n + 256], precision=lax.Precision.HIGHEST,
                    preferred_element_type=jnp.float32)
        for f in range(2):
            pair = w[:, 128 * f : 128 * f + 128] * gain
            outr[at(2 * n + f)] = pair[:, :64].reshape(8, 32, 64)
            outi[at(2 * n + f)] = pair[:, 64:].reshape(8, 32, 64)


def body(ur, ui, gf, wz, tw, outr, outi, wv, last, gv, inp, xbuf, b2, r2, tv, gs, asc, bsc, lsc,
           in_sem, q_sem, c_sem, s1, d1, s2, d2):
    row, col = lax.axis_index("row"), lax.axis_index("col")
    core = lax.rem(row, 2)
    dests = [1 + 2 * core, 2 - core, 3 - core]
    other = 1 - col

    def arrived(ref, sem):
        pltpu.make_async_remote_copy(src_ref=ref, dst_ref=ref, send_sem=sem, recv_sem=sem,
                                     device_id={"row": row}, device_id_type=MESH).wait_recv()

    def load(g, k):
        src, dst = (ur, ui)[k], inp.at[k]
        return pltpu.make_async_copy(src.at[g], dst.at[lax.rem(g, RING)], in_sem.at[lax.rem(g, RING)])

    pieces = ((0, 2), (2, 2), (4, 4), (8, 4), (12, 4))

    def piece(i, k):
        src, dst = (ur, ui)[k], inp.at[k]
        part = (0, slice(None), pl.ds(*pieces[i]))
        return pltpu.make_async_copy(src.at[part], dst.at[part], q_sem.at[i])

    consts = [
        pltpu.make_async_copy(tw, tv, c_sem.at[0]),
        pltpu.make_async_copy(wz.at[col], wv.at[pl.ds(0, 256)], c_sem.at[1]),
        pltpu.make_async_copy(wz.at[other], wv.at[pl.ds(256, 256)], c_sem.at[1]),
        pltpu.make_async_copy(gf, gs, c_sem.at[2]),
    ]
    def start_piece(i):
        piece(i, 0).start()
        piece(i, 1).start()

    consts[0].start()
    start_piece(0)
    barrier = pltpu.get_barrier_semaphore()
    for p in (1, 2, 3):
        pl.semaphore_signal(barrier, inc=1, device_id={"row": lax.rem(row + p, 4)}, device_id_type=MESH)
    pl.semaphore_signal(barrier, inc=1, device_id={"col": other}, device_id_type=MESH)
    for i in range(1, len(pieces)):
        start_piece(i)

    def step_x(g, first, count):
        ring = lax.rem(g, RING)
        bases = [4 * g * 7 + 3 + lax.rem(k + 4 - row, 4) for k in range(4)]

        def one(i, s):
            y = first + 2 * i + s
            ar = inp[0, ring, :, y].reshape(PACK * 32, 64).T
            ai = inp[1, ring, :, y].reshape(PACK * 32, 64).T
            a = dft8([(ar[8 * j : 8 * j + 8], ai[8 * j : 8 * j + 8]) for j in range(8)])
            for k1 in range(8):
                vr, vi = times(a[k1], tv[0, k1], tv[1, k1])
                asc[s, 0, pl.ds(8 * k1, 8), :] = vr
                asc[s, 1, pl.ds(8 * k1, 8), :] = vi
            b = dft8([tuple(asc[s, q, pl.ds(x2, 8, stride=8), :] for q in range(2)) for x2 in range(8)])
            top = lax.broadcasted_iota(jnp.int32, (8, 128), 0) < 4
            for k2, (vr, vi) in enumerate(b):
                at = bases[k2 // 2] + 14 * (k2 % 2)
                xbuf[at, y] = jnp.where(top, vr, pltpu.roll(vi, 4, 0))
                xbuf[at + 7, y] = jnp.where(top, pltpu.roll(vr, 4, 0), vi)

        @pl.loop(0, count // 2)
        def _(i):
            one(i, 0)
            one(i, 1)

    def send_row(u, j, first=0, count=16):
        p = dests[j]
        return pltpu.make_async_remote_copy(
            src_ref=xbuf.at[u * 7 + 3 + p, pl.ds(first, count)], dst_ref=xbuf.at[u * 7 + 3 - p, pl.ds(first, count)],
            send_sem=s1, recv_sem=d1.at[u],
            device_id={"row": lax.rem(row + p, 4)}, device_id_type=MESH)

    def send_col(u):
        return pltpu.make_async_remote_copy(
            src_ref=b2.at[u * 2 + other], dst_ref=r2.at[u],
            send_sem=s2, recv_sem=d2.at[u // 2], device_id={"col": other}, device_id_type=MESH)

    def step_y(u):
        arrived(xbuf.at[pl.ds(u * 7, 3)], d1.at[u])
        slots = [u * 7 + lax.rem(r + 7 - row, 4) for r in range(4)]
        for y2 in range(8):
            a = packed_dft8([xbuf[slots[y1 // 2], 8 * (y1 % 2) + y2] for y1 in range(8)])
            for k1 in range(8):
                tr, ti = twiddle(k1 * y2)
                bsc[k1, y2] = a[k1] * tr - rotate(a[k1]) * ti if k1 * y2 else a[k1] * tr
        for k1 in range(8):
            b = packed_dft8([bsc[k1, y2] for y2 in range(8)])
            for k2 in range(8):
                b2[u * 2 + k2 // 4, pl.ds(8 * (k1 + 8 * (k2 % 4)), 8), :] = b[k2]
        send_col(u).start()

    def gather_z(m, dst):
        def part(lane, plane):
            for kx in range(8):
                for q in range(2):
                    dst[pl.ds(32 * kx, 32), pl.ds(lane + 128 * q, 128)] = plane(2 * m + kx // 4, pl.ds(4 * q + kx % 4, 32, stride=8))

        part(0, lambda u, rows: b2[u * 2 + col, rows, :])
        arrived(r2.at[pl.ds(2 * m, 2)], d2.at[m])
        part(256, lambda u, rows: r2[u, rows, :])

    def step_z(m):
        gather_z(m, lsc)
        gain = gv[pl.ds(pl.multiple_of(256 * lax.rem(m, 2), 256), 256), :]
        lane_product(lsc, wv, gain, outr, outi, lambda f: (PACK * (m // 2) + f, pl.ds(8 * lax.rem(m, 2), 8)))

    consts[0].wait()
    for i, (first, count) in enumerate(pieces):
        arrived(inp.at[:, 0, :, pl.ds(first, count)], q_sem.at[i])
        step_x(0, first, count)
        if i == 0:
            pl.semaphore_wait(barrier, 4)
        send_row(0, 1, first, count).start()
    send_row(0, 0).start()
    send_row(1, 1).start()
    send_row(1, 0).start()
    send_row(0, 2).start()

    def send_rows(first, last):
        @pl.loop(first, last)
        def _(u):
            send_row(u, 1).start()
            send_row(u, 0).start()
            send_row(u - 1, 2).start()

    send_rows(2, 4)

    @pl.loop(1, RING)
    def _(g):
        load(g, 0).start()
        load(g, 1).start()

    for copy in consts[1:]:
        copy.start()
    step_y(0)
    for k in range(2):
        load(RING, k).start()
    arrived(inp.at[:, 1], in_sem.at[1])
    step_x(1, 0, 16)
    send_rows(4, 8)
    for k in range(2):
        load(RING + 1, k).start()
    arrived(wv, c_sem.at[1])
    consts[3].wait()
    gain = gs[...].reshape(512, 64)
    gv[...] = jnp.concatenate([gain, gain], axis=1)

    @pl.loop(1, UNITS + LAG - 3)
    def _(t):
        @pl.when(t < UNITS)
        def _():
            step_y(t)

        g, i = (t + 7) // 4, lax.rem(t + 3, 4)

        @pl.when(g < GROUPS)
        def _():
            @pl.when(i == 0)
            def _():
                arrived(inp.at[:, lax.rem(g, RING)], in_sem.at[lax.rem(g, RING)])

            step_x(g, 4 * i, 4)

            @pl.when(i == 3)
            def _():
                send_rows(4 * g, 4 * g + 4)

                @pl.when(g == GROUPS - 1)
                def _():
                    send_row(UNITS - 1, 2).start()

                @pl.when(g + RING < GROUPS)
                def _():
                    load(g + RING, 0).start()
                    load(g + RING, 1).start()

        @pl.when((t >= LAG) & (lax.rem(t - LAG, 2) == 0))
        def _():
            step_z((t - LAG) // 2)

    arrived(xbuf.at[pl.ds(0, 3 * UNITS)], s1)
    gather_z(UNITS // 2 - 1, last)
    arrived(b2.at[pl.ds(0, UNITS)], s2)


def kernel(*refs):
    dma = pltpu.SemaphoreType.DMA
    pl.run_scoped(functools.partial(body, *refs), in_sem=dma((RING,)), q_sem=dma((5,)), c_sem=dma((3,)), s1=dma,
                  d1=dma((UNITS,)), s2=dma, d2=dma((UNITS // 2,)))


def put(vr, vi, mat, last, gain, outr, outi, lr, li, sem):
    cuts = [(pl.ds(7 * i, 7), slice(None)) for i in range(4)] + [(pl.ds(28, 4), pl.ds(0, 8))]
    copies = [pltpu.make_async_copy(v.at[cut], o.at[cut], sem) for cut in cuts for v, o in ((vr, outr), (vi, outi))]
    for copy in copies:
        copy.start()
    lane_product(last, mat, gain[256:, :], lr, li, lambda f: f)
    cut = (pl.ds(28, 4), pl.ds(8, 8))
    tail = [pltpu.make_async_copy(v, o.at[cut], sem) for v, o in ((lr, outr), (li, outi))]
    for copy in tail:
        copy.start()
    for copy in copies + tail:
        copy.wait()


def solution(mesh):
    f32 = jnp.float32

    def local_forward(u_real, u_imag, g_filter):
        parts = [jnp.transpose(v, (0, 2, 3, 1)).reshape(GROUPS, PACK, 16, 32, 64) for v in (u_real, u_imag)]
        spectrum = pl.pallas_call(
            kernel,
            out_shape=[pltpu.VMEM((32, 16, 32, 64), f32)] * 2 + [
                pltpu.VMEM((512, 512), f32), pltpu.VMEM((256, 512), f32), pltpu.VMEM((512, 128), f32)],
            in_specs=[pl.BlockSpec(memory_space=pltpu.HBM)] * 5,
            out_specs=[pl.BlockSpec(memory_space=pltpu.VMEM)] * 5,
            scratch_shapes=[
                pltpu.VMEM((2, RING, PACK, 16, 32, 64), f32),
                pltpu.VMEM((UNITS * 7, 16, 8, 128), f32),
                pltpu.VMEM((UNITS * 2, 256, 128), f32),
                pltpu.VMEM((UNITS, 256, 128), f32),
                pltpu.VMEM((2, 8, 8, 128), f32),
                pltpu.VMEM((16, 32, 64), f32),
                pltpu.VMEM((2, 2, 64, 128), f32),
                pltpu.VMEM((8, 8, 8, 128), f32),
                pltpu.VMEM((256, 512), f32),
            ],
            compiler_params=pltpu.CompilerParams(
                collective_id=0, has_side_effects=True, vmem_limit_bytes=40 * 1024 * 1024),
            name="dft3",
        )(*parts, g_filter, jnp.asarray(lane_matrix()), jnp.asarray(sublane_twiddle()))
        return pl.pallas_call(
            put,
            out_shape=[jax.ShapeDtypeStruct((32, 16, 32, 64), f32)] * 2,
            in_specs=[pl.BlockSpec(memory_space=pltpu.VMEM)] * 5,
            out_specs=[pl.BlockSpec(memory_space=pltpu.HBM)] * 2,
            scratch_shapes=[pltpu.VMEM((PACK, 8, 32, 64), f32)] * 2 + [pltpu.SemaphoreType.DMA],
            compiler_params=pltpu.CompilerParams(vmem_limit_bytes=8 * 1024 * 1024),
            name="put",
        )(*spectrum)

    field_spec = P("fld", None, "row", "col")
    out_spec = P("fld", "row", "col", None)
    return jax.shard_map(local_forward, mesh=mesh, in_specs=(field_spec, field_spec, P("row", "col", None)),
                         out_specs=(out_spec, out_spec), check_vma=False)
```

```python
import functools
import math

import jax
import jax.numpy as jnp
import numpy as np
from jax import lax
from jax.experimental import pallas as pl
from jax.experimental.pallas import tpu as pltpu
from jax.sharding import PartitionSpec as P

MESH = pl.DeviceIdType.MESH
HALF = math.sqrt(0.5)
GROUPS, PACK, UNITS, RING, LAG = 8, 4, 32, 4, 5


def interleave(even, odd):
    return [v for pair in zip(even, odd) for v in pair]


def dft4(b):
    (r0, i0), (r1, i1), (r2, i2), (r3, i3) = b
    sr0, si0, sr1, si1 = r0 + r2, i0 + i2, r0 - r2, i0 - i2
    sr2, si2, sr3, si3 = r1 + r3, i1 + i3, r1 - r3, i1 - i3
    return [(sr0 + sr2, si0 + si2), (sr1 + si3, si1 - sr3), (sr0 - sr2, si0 - si2), (sr1 - si3, si1 + sr3)]


def dft8(a):
    pairs = list(zip(a[:4], a[4:]))
    even = [(vr + wr, vi + wi) for (vr, vi), (wr, wi) in pairs]
    odd = [(vr - wr, vi - wi) for (vr, vi), (wr, wi) in pairs]
    o0, (r1, i1), (r2, i2), (r3, i3) = odd
    odd = [o0, ((r1 + i1) * HALF, (i1 - r1) * HALF), (i2, -r2), ((i3 - r3) * HALF, (r3 + i3) * -HALF)]
    even, odd = dft4(even), dft4(odd)
    return interleave(even, odd)


def rotate(v):
    sign = jnp.where(lax.broadcasted_iota(jnp.int32, v.shape, 0) < 4, 1.0, -1.0)
    return pltpu.roll(v, 4, 0) * sign


def packed_dft4(b):
    b0, b1, b2, b3 = b
    s0, s1, s2, s3 = b0 + b2, b0 - b2, b1 + b3, rotate(b1 - b3)
    return [s0 + s2, s1 + s3, s0 - s2, s1 - s3]


def packed_dft8(a):
    pairs = list(zip(a[:4], a[4:]))
    even = packed_dft4([v + w for v, w in pairs])
    o0, o1, o2, o3 = [v - w for v, w in pairs]
    odd = packed_dft4([o0, (rotate(o1) + o1) * HALF, rotate(o2), (rotate(o3) - o3) * HALF])
    return interleave(even, odd)


def times(a, tr, ti):
    return a[0] * tr - a[1] * ti, a[0] * ti + a[1] * tr


def twiddle(m):
    angle = -2.0 * math.pi * (m % 64) / 64.0
    return math.cos(angle) / 8.0, math.sin(angle) / 8.0


def lane_matrix():
    z, kz = np.arange(64), np.arange(64)
    angle = 2.0 * np.pi * ((z[:, None] * kz[None, :]) % 64) / 64.0
    cos, sin = np.cos(angle) / 8.0, np.sin(angle) / 8.0
    blocks = np.stack([np.concatenate([cos, -sin], 1), np.concatenate([sin, cos], 1)])
    out = np.zeros((2, 2, PACK, 32, PACK, 128))
    for c in range(2):
        for f in range(PACK):
            out[c, :, f, :, f, :] = blocks[:, 32 * c : 32 * c + 32]
    return out.reshape(2, 256, PACK * 128).astype(np.float32)


def sublane_twiddle():
    k1, x2 = np.arange(8), np.arange(8)
    angle = -2.0 * np.pi * (k1[:, None] * x2[None, :]) / 64.0
    both = np.stack([np.cos(angle), np.sin(angle)]) / 8.0
    return np.broadcast_to(both[..., None], (2, 8, 8, 128)).astype(np.float32)


def gather(dst, lane, plane):
    for kx in range(8):
        for q in range(2):
            dst[pl.ds(32 * kx, 32), pl.ds(lane + 128 * q, 128)] = plane(kx // 4, pl.ds(4 * q + kx % 4, 32, stride=8))


def lane_product(lhs, mat, gain, outr, outi, at):
    for n in range(2):
        w = jnp.dot(lhs[...], mat[:, 256 * n : 256 * n + 256], precision=lax.Precision.HIGHEST,
                    preferred_element_type=jnp.float32)
        for f in range(2):
            pair = w[:, 128 * f : 128 * f + 128] * gain
            outr[at(2 * n + f)] = pair[:, :64].reshape(8, 32, 64)
            outi[at(2 * n + f)] = pair[:, 64:].reshape(8, 32, 64)


def body(ur, ui, gf, wz, tw, outr, outi, wv, own, got, gv, inp, xbuf, b2, r2, tv, gs, asc, bsc, lsc,
           in_sem, q_sem, c_sem, s1, d1, s2, d2):
    row, col = lax.axis_index("row"), lax.axis_index("col")
    core = lax.rem(row, 2)
    dests = [1 + 2 * core, 2 - core, 3 - core]
    other = 1 - col

    def arrived(ref, sem):
        pltpu.make_async_remote_copy(src_ref=ref, dst_ref=ref, send_sem=sem, recv_sem=sem,
                                     device_id={"row": row}, device_id_type=MESH).wait_recv()

    def load(g, k):
        src, dst = (ur, ui)[k], inp.at[k]
        return pltpu.make_async_copy(src.at[g], dst.at[lax.rem(g, RING)], in_sem.at[lax.rem(g, RING)])

    pieces = ((0, 2), (2, 2), (4, 4), (8, 4), (12, 4))

    def piece(i, k):
        src, dst = (ur, ui)[k], inp.at[k]
        part = (0, slice(None), pl.ds(*pieces[i]))
        return pltpu.make_async_copy(src.at[part], dst.at[part], q_sem.at[i])

    consts = [
        pltpu.make_async_copy(tw, tv, c_sem.at[0]),
        pltpu.make_async_copy(wz.at[col], wv.at[pl.ds(0, 256)], c_sem.at[1]),
        pltpu.make_async_copy(wz.at[other], wv.at[pl.ds(256, 256)], c_sem.at[1]),
        pltpu.make_async_copy(gf, gs, c_sem.at[2]),
    ]
    def start_piece(i):
        piece(i, 0).start()
        piece(i, 1).start()

    consts[0].start()
    start_piece(0)
    barrier = pltpu.get_barrier_semaphore()
    for p in (1, 2, 3):
        pl.semaphore_signal(barrier, inc=1, device_id={"row": lax.rem(row + p, 4)}, device_id_type=MESH)
    pl.semaphore_signal(barrier, inc=1, device_id={"col": other}, device_id_type=MESH)
    for i in range(1, len(pieces)):
        start_piece(i)

    def step_x(g, first, count):
        ring = lax.rem(g, RING)
        bases = [4 * g * 7 + 3 + lax.rem(k + 4 - row, 4) for k in range(4)]

        def one(i, s):
            y = first + 2 * i + s
            ar = inp[0, ring, :, y].reshape(PACK * 32, 64).T
            ai = inp[1, ring, :, y].reshape(PACK * 32, 64).T
            a = dft8([(ar[8 * j : 8 * j + 8], ai[8 * j : 8 * j + 8]) for j in range(8)])
            for k1 in range(8):
                vr, vi = times(a[k1], tv[0, k1], tv[1, k1])
                asc[s, 0, pl.ds(8 * k1, 8), :] = vr
                asc[s, 1, pl.ds(8 * k1, 8), :] = vi
            b = dft8([tuple(asc[s, q, pl.ds(x2, 8, stride=8), :] for q in range(2)) for x2 in range(8)])
            top = lax.broadcasted_iota(jnp.int32, (8, 128), 0) < 4
            for k2, (vr, vi) in enumerate(b):
                at = bases[k2 // 2] + 14 * (k2 % 2)
                xbuf[at, y] = jnp.where(top, vr, pltpu.roll(vi, 4, 0))
                xbuf[at + 7, y] = jnp.where(top, pltpu.roll(vr, 4, 0), vi)

        @pl.loop(0, count // 2)
        def _(i):
            one(i, 0)
            one(i, 1)

    def send_row(u, j, first=0, count=16):
        p = dests[j]
        return pltpu.make_async_remote_copy(
            src_ref=xbuf.at[u * 7 + 3 + p, pl.ds(first, count)], dst_ref=xbuf.at[u * 7 + 3 - p, pl.ds(first, count)],
            send_sem=s1, recv_sem=d1.at[u],
            device_id={"row": lax.rem(row + p, 4)}, device_id_type=MESH)

    def send_col(u, dst):
        return pltpu.make_async_remote_copy(
            src_ref=b2.at[u * 2 + other], dst_ref=dst,
            send_sem=s2, recv_sem=d2.at[u // 2], device_id={"col": other}, device_id_type=MESH)

    def step_y(u):
        arrived(xbuf.at[pl.ds(u * 7, 3)], d1.at[u])
        slots = [u * 7 + lax.rem(r + 7 - row, 4) for r in range(4)]
        for y2 in range(8):
            a = packed_dft8([xbuf[slots[y1 // 2], 8 * (y1 % 2) + y2] for y1 in range(8)])
            for k1 in range(8):
                tr, ti = twiddle(k1 * y2)
                bsc[k1, y2] = a[k1] * tr - rotate(a[k1]) * ti if k1 * y2 else a[k1] * tr
        for k1 in range(8):
            b = packed_dft8([bsc[k1, y2] for y2 in range(8)])
            for k2 in range(8):
                b2[u * 2 + k2 // 4, pl.ds(8 * (k1 + 8 * (k2 % 4)), 8), :] = b[k2]

        @pl.when(u < UNITS - 2)
        def _():
            send_col(u, r2.at[u]).start()

        @pl.when(u >= UNITS - 2)
        def _():
            send_col(u, got.at[u - UNITS + 2]).start()

    def step_z(m):
        gather(lsc, 0, lambda v, rows: b2[(2 * m + v) * 2 + col, rows, :])
        arrived(r2.at[pl.ds(2 * m, 2)], d2.at[m])
        gather(lsc, 256, lambda v, rows: r2[2 * m + v, rows, :])
        gain = gv[pl.ds(pl.multiple_of(256 * lax.rem(m, 2), 256), 256), :]
        lane_product(lsc, wv, gain, outr, outi, lambda f: (PACK * (m // 2) + f, pl.ds(8 * lax.rem(m, 2), 8)))

    consts[0].wait()
    for i, (first, count) in enumerate(pieces):
        arrived(inp.at[:, 0, :, pl.ds(first, count)], q_sem.at[i])
        step_x(0, first, count)
        if i == 0:
            pl.semaphore_wait(barrier, 4)
        send_row(0, 1, first, count).start()
    send_row(0, 0).start()
    send_row(1, 1).start()
    send_row(1, 0).start()
    send_row(0, 2).start()

    def send_rows(first, last):
        @pl.loop(first, last)
        def _(u):
            send_row(u, 1).start()
            send_row(u, 0).start()
            send_row(u - 1, 2).start()

    send_rows(2, 4)

    @pl.loop(1, RING)
    def _(g):
        load(g, 0).start()
        load(g, 1).start()

    for copy in consts[1:]:
        copy.start()
    step_y(0)
    for k in range(2):
        load(RING, k).start()
    arrived(inp.at[:, 1], in_sem.at[1])
    step_x(1, 0, 16)
    send_rows(4, 8)
    for k in range(2):
        load(RING + 1, k).start()
    arrived(wv, c_sem.at[1])
    consts[3].wait()
    gain = gs[...].reshape(512, 64)
    gv[...] = jnp.concatenate([gain, gain], axis=1)

    @pl.loop(1, UNITS + LAG - 3)
    def _(t):
        @pl.when(t < UNITS)
        def _():
            step_y(t)

        g, i = (t + 7) // 4, lax.rem(t + 3, 4)

        @pl.when(g < GROUPS)
        def _():
            @pl.when(i == 0)
            def _():
                arrived(inp.at[:, lax.rem(g, RING)], in_sem.at[lax.rem(g, RING)])

            step_x(g, 4 * i, 4)

            @pl.when(i == 3)
            def _():
                send_rows(4 * g, 4 * g + 4)

                @pl.when(g == GROUPS - 1)
                def _():
                    send_row(UNITS - 1, 2).start()

                @pl.when(g + RING < GROUPS)
                def _():
                    load(g + RING, 0).start()
                    load(g + RING, 1).start()

        @pl.when((t >= LAG) & (lax.rem(t - LAG, 2) == 0))
        def _():
            step_z((t - LAG) // 2)

    arrived(xbuf.at[pl.ds(0, 3 * UNITS)], s1)
    for v in range(2):
        own[v] = b2[2 * (UNITS - 2 + v) + col]
    arrived(got, d2.at[UNITS // 2 - 1])
    arrived(b2.at[pl.ds(0, UNITS)], s2)


def kernel(*refs):
    dma = pltpu.SemaphoreType.DMA
    pl.run_scoped(functools.partial(body, *refs), in_sem=dma((RING,)), q_sem=dma((5,)), c_sem=dma((3,)), s1=dma,
                  d1=dma((UNITS,)), s2=dma, d2=dma((UNITS // 2,)))


def put(vr, vi, mat, own, got, gain, outr, outi, lr, li, lhs, sem):
    cuts = [(pl.ds(7 * i, 7), slice(None)) for i in range(4)] + [(pl.ds(28, 4), pl.ds(0, 8))]
    copies = [pltpu.make_async_copy(v.at[cut], o.at[cut], sem) for cut in cuts for v, o in ((vr, outr), (vi, outi))]
    for copy in copies:
        copy.start()
    gather(lhs, 0, lambda v, rows: own[v, rows, :])
    gather(lhs, 256, lambda v, rows: got[v, rows, :])
    lane_product(lhs, mat, gain[256:, :], lr, li, lambda f: f)
    cut = (pl.ds(28, 4), pl.ds(8, 8))
    tail = [pltpu.make_async_copy(v, o.at[cut], sem) for v, o in ((lr, outr), (li, outi))]
    for copy in tail:
        copy.start()
    for copy in copies + tail:
        copy.wait()


def solution(mesh):
    f32 = jnp.float32

    def local_forward(u_real, u_imag, g_filter):
        parts = [jnp.transpose(v, (0, 2, 3, 1)).reshape(GROUPS, PACK, 16, 32, 64) for v in (u_real, u_imag)]
        spectrum = pl.pallas_call(
            kernel,
            out_shape=[pltpu.VMEM((32, 16, 32, 64), f32)] * 2 + [
                pltpu.VMEM((512, 512), f32), pltpu.VMEM((2, 256, 128), f32), pltpu.VMEM((2, 256, 128), f32),
                pltpu.VMEM((512, 128), f32)],
            in_specs=[pl.BlockSpec(memory_space=pltpu.HBM)] * 5,
            out_specs=[pl.BlockSpec(memory_space=pltpu.VMEM)] * 6,
            scratch_shapes=[
                pltpu.VMEM((2, RING, PACK, 16, 32, 64), f32),
                pltpu.VMEM((UNITS * 7, 16, 8, 128), f32),
                pltpu.VMEM((UNITS * 2, 256, 128), f32),
                pltpu.VMEM((UNITS, 256, 128), f32),
                pltpu.VMEM((2, 8, 8, 128), f32),
                pltpu.VMEM((16, 32, 64), f32),
                pltpu.VMEM((2, 2, 64, 128), f32),
                pltpu.VMEM((8, 8, 8, 128), f32),
                pltpu.VMEM((256, 512), f32),
            ],
            compiler_params=pltpu.CompilerParams(
                collective_id=0, has_side_effects=True, vmem_limit_bytes=40 * 1024 * 1024),
            name="dft3",
        )(*parts, g_filter, jnp.asarray(lane_matrix()), jnp.asarray(sublane_twiddle()))
        return pl.pallas_call(
            put,
            out_shape=[jax.ShapeDtypeStruct((32, 16, 32, 64), f32)] * 2,
            in_specs=[pl.BlockSpec(memory_space=pltpu.VMEM)] * 6,
            out_specs=[pl.BlockSpec(memory_space=pltpu.HBM)] * 2,
            scratch_shapes=[pltpu.VMEM((PACK, 8, 32, 64), f32)] * 2 + [pltpu.VMEM((256, 512), f32), pltpu.SemaphoreType.DMA],
            compiler_params=pltpu.CompilerParams(vmem_limit_bytes=8 * 1024 * 1024),
            name="put",
        )(*spectrum)

    field_spec = P("fld", None, "row", "col")
    out_spec = P("fld", "row", "col", None)
    return jax.shard_map(local_forward, mesh=mesh, in_specs=(field_spec, field_spec, P("row", "col", None)),
                         out_specs=(out_spec, out_spec), check_vma=False)
```

```python
import functools
import math

import jax
import jax.numpy as jnp
import numpy as np
from jax import lax
from jax.experimental import pallas as pl
from jax.experimental.pallas import tpu as pltpu
from jax.sharding import PartitionSpec as P

MESH = pl.DeviceIdType.MESH
HALF = math.sqrt(0.5)
GROUPS, PACK, UNITS, RING, LAG = 8, 4, 32, 4, 5


def interleave(even, odd):
    return [v for pair in zip(even, odd) for v in pair]


def dft4(b):
    (r0, i0), (r1, i1), (r2, i2), (r3, i3) = b
    sr0, si0, sr1, si1 = r0 + r2, i0 + i2, r0 - r2, i0 - i2
    sr2, si2, sr3, si3 = r1 + r3, i1 + i3, r1 - r3, i1 - i3
    return [(sr0 + sr2, si0 + si2), (sr1 + si3, si1 - sr3), (sr0 - sr2, si0 - si2), (sr1 - si3, si1 + sr3)]


def dft8(a):
    pairs = list(zip(a[:4], a[4:]))
    even = [(vr + wr, vi + wi) for (vr, vi), (wr, wi) in pairs]
    odd = [(vr - wr, vi - wi) for (vr, vi), (wr, wi) in pairs]
    o0, (r1, i1), (r2, i2), (r3, i3) = odd
    odd = [o0, ((r1 + i1) * HALF, (i1 - r1) * HALF), (i2, -r2), ((i3 - r3) * HALF, (r3 + i3) * -HALF)]
    even, odd = dft4(even), dft4(odd)
    return interleave(even, odd)


def rotate(v):
    sign = jnp.where(lax.broadcasted_iota(jnp.int32, v.shape, 0) < 4, 1.0, -1.0)
    return pltpu.roll(v, 4, 0) * sign


def packed_dft4(b):
    b0, b1, b2, b3 = b
    s0, s1, s2, s3 = b0 + b2, b0 - b2, b1 + b3, rotate(b1 - b3)
    return [s0 + s2, s1 + s3, s0 - s2, s1 - s3]


def packed_dft8(a):
    pairs = list(zip(a[:4], a[4:]))
    even = packed_dft4([v + w for v, w in pairs])
    o0, o1, o2, o3 = [v - w for v, w in pairs]
    odd = packed_dft4([o0, (rotate(o1) + o1) * HALF, rotate(o2), (rotate(o3) - o3) * HALF])
    return interleave(even, odd)


def times(a, tr, ti):
    return a[0] * tr - a[1] * ti, a[0] * ti + a[1] * tr


def twiddle(m):
    angle = -2.0 * math.pi * (m % 64) / 64.0
    return math.cos(angle) / 8.0, math.sin(angle) / 8.0


def lane_matrix():
    z, kz = np.arange(64), np.arange(64)
    angle = 2.0 * np.pi * ((z[:, None] * kz[None, :]) % 64) / 64.0
    cos, sin = np.cos(angle) / 8.0, np.sin(angle) / 8.0
    blocks = np.stack([np.concatenate([cos, -sin], 1), np.concatenate([sin, cos], 1)])
    out = np.zeros((2, 2, PACK, 32, PACK, 128))
    for c in range(2):
        for f in range(PACK):
            out[c, :, f, :, f, :] = blocks[:, 32 * c : 32 * c + 32]
    return out.reshape(2, 256, PACK * 128).astype(np.float32)


def sublane_twiddle():
    k1, x2 = np.arange(8), np.arange(8)
    angle = -2.0 * np.pi * (k1[:, None] * x2[None, :]) / 64.0
    both = np.stack([np.cos(angle), np.sin(angle)]) / 8.0
    return np.broadcast_to(both[..., None], (2, 8, 8, 128)).astype(np.float32)


def gather(dst, lane, plane):
    for kx in range(8):
        for q in range(2):
            dst[pl.ds(32 * kx, 32), pl.ds(lane + 128 * q, 128)] = plane(kx // 4, pl.ds(4 * q + kx % 4, 32, stride=8))


def lane_product(lhs, mat, gain, outr, outi, at):
    for n in range(2):
        w = jnp.dot(lhs[...], mat[:, 256 * n : 256 * n + 256], precision=lax.Precision.HIGHEST,
                    preferred_element_type=jnp.float32)
        for f in range(2):
            pair = w[:, 128 * f : 128 * f + 128] * gain
            outr[at(2 * n + f)] = pair[:, :64].reshape(8, 32, 64)
            outi[at(2 * n + f)] = pair[:, 64:].reshape(8, 32, 64)


def body(ur, ui, gf, wz, tw, outr, outi, wv, own, got, gv, inp, xbuf, b2, r2, tv, gs, asc, bsc, lsc,
           in_sem, q_sem, c_sem, s1, d1, s2, d2):
    row, col = lax.axis_index("row"), lax.axis_index("col")
    core = lax.rem(row, 2)
    dests = [1 + 2 * core, 2 - core, 3 - core]
    other = 1 - col

    def arrived(ref, sem):
        pltpu.make_async_remote_copy(src_ref=ref, dst_ref=ref, send_sem=sem, recv_sem=sem,
                                     device_id={"row": row}, device_id_type=MESH).wait_recv()

    def load(g, k):
        src, dst = (ur, ui)[k], inp.at[k]
        return pltpu.make_async_copy(src.at[g], dst.at[lax.rem(g, RING)], in_sem.at[lax.rem(g, RING)])

    def piece(i, k):
        src, dst = (ur, ui)[k], inp.at[k]
        part = (0, slice(None), pl.ds(2 * i, 2))
        return pltpu.make_async_copy(src.at[part], dst.at[part], q_sem.at[i])

    consts = [
        pltpu.make_async_copy(tw, tv, c_sem.at[0]),
        pltpu.make_async_copy(wz.at[col], wv.at[pl.ds(0, 256)], c_sem.at[1]),
        pltpu.make_async_copy(wz.at[other], wv.at[pl.ds(256, 256)], c_sem.at[1]),
        pltpu.make_async_copy(gf, gs, c_sem.at[2]),
    ]
    def start_piece(i):
        piece(i, 0).start()
        piece(i, 1).start()

    consts[0].start()
    start_piece(0)
    barrier = pltpu.get_barrier_semaphore()
    for p in (1, 2, 3):
        pl.semaphore_signal(barrier, inc=1, device_id={"row": lax.rem(row + p, 4)}, device_id_type=MESH)
    pl.semaphore_signal(barrier, inc=1, device_id={"col": other}, device_id_type=MESH)

    @pl.loop(1, 8)
    def _(i):
        start_piece(i)


    def step_x(g, first, count):
        ring = lax.rem(g, RING)
        bases = [4 * g * 7 + 3 + lax.rem(k + 4 - row, 4) for k in range(4)]

        def one(i, s):
            y = first + 2 * i + s
            ar = inp[0, ring, :, y].reshape(PACK * 32, 64).T
            ai = inp[1, ring, :, y].reshape(PACK * 32, 64).T
            a = dft8([(ar[8 * j : 8 * j + 8], ai[8 * j : 8 * j + 8]) for j in range(8)])
            for k1 in range(8):
                vr, vi = times(a[k1], tv[0, k1], tv[1, k1])
                asc[s, 0, pl.ds(8 * k1, 8), :] = vr
                asc[s, 1, pl.ds(8 * k1, 8), :] = vi
            b = dft8([tuple(asc[s, q, pl.ds(x2, 8, stride=8), :] for q in range(2)) for x2 in range(8)])
            top = lax.broadcasted_iota(jnp.int32, (8, 128), 0) < 4
            for k2, (vr, vi) in enumerate(b):
                at = bases[k2 // 2] + 14 * (k2 % 2)
                xbuf[at, y] = jnp.where(top, vr, pltpu.roll(vi, 4, 0))
                xbuf[at + 7, y] = jnp.where(top, pltpu.roll(vr, 4, 0), vi)

        def pair(i):
            one(i, 0)
            one(i, 1)

        pl.loop(0, count // 2)(pair) if count > 2 else pair(0)

    def send_row(u, j, first=0, count=16):
        p = dests[j]
        return pltpu.make_async_remote_copy(
            src_ref=xbuf.at[u * 7 + 3 + p, pl.ds(first, count)], dst_ref=xbuf.at[u * 7 + 3 - p, pl.ds(first, count)],
            send_sem=s1, recv_sem=d1.at[u],
            device_id={"row": lax.rem(row + p, 4)}, device_id_type=MESH)

    def send_col(u, dst):
        return pltpu.make_async_remote_copy(
            src_ref=b2.at[u * 2 + other], dst_ref=dst,
            send_sem=s2, recv_sem=d2.at[u // 2], device_id={"col": other}, device_id_type=MESH)

    def step_y(u):
        arrived(xbuf.at[pl.ds(u * 7, 3)], d1.at[u])
        slots = [u * 7 + lax.rem(r + 7 - row, 4) for r in range(4)]
        for y2 in range(8):
            a = packed_dft8([xbuf[slots[y1 // 2], 8 * (y1 % 2) + y2] for y1 in range(8)])
            for k1 in range(8):
                tr, ti = twiddle(k1 * y2)
                bsc[k1, y2] = a[k1] * tr - rotate(a[k1]) * ti if k1 * y2 else a[k1] * tr
        for k1 in range(8):
            b = packed_dft8([bsc[k1, y2] for y2 in range(8)])
            for k2 in range(8):
                b2[u * 2 + k2 // 4, pl.ds(8 * (k1 + 8 * (k2 % 4)), 8), :] = b[k2]

        @pl.when(u < UNITS - 2)
        def _():
            send_col(u, r2.at[u]).start()

        @pl.when(u >= UNITS - 2)
        def _():
            send_col(u, got.at[u - UNITS + 2]).start()

    def step_z(m):
        gather(lsc, 0, lambda v, rows: b2[(2 * m + v) * 2 + col, rows, :])
        arrived(r2.at[pl.ds(2 * m, 2)], d2.at[m])
        gather(lsc, 256, lambda v, rows: r2[2 * m + v, rows, :])
        gain = gv[pl.ds(pl.multiple_of(256 * lax.rem(m, 2), 256), 256), :]
        lane_product(lsc, wv, gain, outr, outi, lambda f: (PACK * (m // 2) + f, pl.ds(8 * lax.rem(m, 2), 8)))

    consts[0].wait()
    def first_group(i):
        arrived(inp.at[:, 0, :, pl.ds(2 * i, 2)], q_sem.at[i])
        step_x(0, 2 * i, 2)

    first_group(0)
    pl.semaphore_wait(barrier, 4)
    send_row(0, 1, 0, 2).start()

    @pl.loop(1, 8)
    def _(i):
        first_group(i)
        send_row(0, 1, 2 * i, 2).start()

    send_row(0, 0).start()
    send_row(1, 1).start()
    send_row(1, 0).start()
    send_row(0, 2).start()

    def send_rows(first, last):
        @pl.loop(first, last)
        def _(u):
            send_row(u, 1).start()
            send_row(u, 0).start()
            send_row(u - 1, 2).start()

    send_rows(2, 4)

    @pl.loop(1, RING)
    def _(g):
        load(g, 0).start()
        load(g, 1).start()

    for copy in consts[1:]:
        copy.start()
    step_y(0)
    for k in range(2):
        load(RING, k).start()
    arrived(inp.at[:, 1], in_sem.at[1])
    step_x(1, 0, 16)
    send_rows(4, 8)
    for k in range(2):
        load(RING + 1, k).start()
    arrived(wv, c_sem.at[1])
    consts[3].wait()
    gain = gs[...].reshape(512, 64)
    gv[...] = jnp.concatenate([gain, gain], axis=1)

    @pl.loop(1, UNITS + LAG - 3)
    def _(t):
        @pl.when(t < UNITS)
        def _():
            step_y(t)

        g, i = (t + 7) // 4, lax.rem(t + 3, 4)

        @pl.when(g < GROUPS)
        def _():
            @pl.when(i == 0)
            def _():
                arrived(inp.at[:, lax.rem(g, RING)], in_sem.at[lax.rem(g, RING)])

            step_x(g, 4 * i, 4)

            @pl.when(i == 3)
            def _():
                send_rows(4 * g, 4 * g + 4)

                @pl.when(g == GROUPS - 1)
                def _():
                    send_row(UNITS - 1, 2).start()

                @pl.when(g + RING < GROUPS)
                def _():
                    load(g + RING, 0).start()
                    load(g + RING, 1).start()

        @pl.when((t >= LAG) & (lax.rem(t - LAG, 2) == 0))
        def _():
            step_z((t - LAG) // 2)

    arrived(xbuf.at[pl.ds(0, 3 * UNITS)], s1)
    for v in range(2):
        own[v] = b2[2 * (UNITS - 2 + v) + col]
    arrived(got, d2.at[UNITS // 2 - 1])
    arrived(b2.at[pl.ds(0, UNITS)], s2)


def kernel(*refs):
    dma = pltpu.SemaphoreType.DMA
    pl.run_scoped(functools.partial(body, *refs), in_sem=dma((RING,)), q_sem=dma((8,)), c_sem=dma((3,)), s1=dma,
                  d1=dma((UNITS,)), s2=dma, d2=dma((UNITS // 2,)))


def put(vr, vi, mat, own, got, gain, outr, outi, lr, li, lhs, sem):
    cuts = [(pl.ds(7 * i, 7), slice(None)) for i in range(4)] + [(pl.ds(28, 4), pl.ds(0, 8))]
    copies = [pltpu.make_async_copy(v.at[cut], o.at[cut], sem) for cut in cuts for v, o in ((vr, outr), (vi, outi))]
    for copy in copies:
        copy.start()
    gather(lhs, 0, lambda v, rows: own[v, rows, :])
    gather(lhs, 256, lambda v, rows: got[v, rows, :])
    lane_product(lhs, mat, gain[256:, :], lr, li, lambda f: f)
    cut = (pl.ds(28, 4), pl.ds(8, 8))
    tail = [pltpu.make_async_copy(v, o.at[cut], sem) for v, o in ((lr, outr), (li, outi))]
    for copy in tail:
        copy.start()
    for copy in copies + tail:
        copy.wait()


def solution(mesh):
    f32 = jnp.float32

    def local_forward(u_real, u_imag, g_filter):
        parts = [jnp.transpose(v, (0, 2, 3, 1)).reshape(GROUPS, PACK, 16, 32, 64) for v in (u_real, u_imag)]
        spectrum = pl.pallas_call(
            kernel,
            out_shape=[pltpu.VMEM((32, 16, 32, 64), f32)] * 2 + [
                pltpu.VMEM((512, 512), f32), pltpu.VMEM((2, 256, 128), f32), pltpu.VMEM((2, 256, 128), f32),
                pltpu.VMEM((512, 128), f32)],
            in_specs=[pl.BlockSpec(memory_space=pltpu.HBM)] * 5,
            out_specs=[pl.BlockSpec(memory_space=pltpu.VMEM)] * 6,
            scratch_shapes=[
                pltpu.VMEM((2, RING, PACK, 16, 32, 64), f32),
                pltpu.VMEM((UNITS * 7, 16, 8, 128), f32),
                pltpu.VMEM((UNITS * 2, 256, 128), f32),
                pltpu.VMEM((UNITS, 256, 128), f32),
                pltpu.VMEM((2, 8, 8, 128), f32),
                pltpu.VMEM((16, 32, 64), f32),
                pltpu.VMEM((2, 2, 64, 128), f32),
                pltpu.VMEM((8, 8, 8, 128), f32),
                pltpu.VMEM((256, 512), f32),
            ],
            compiler_params=pltpu.CompilerParams(
                collective_id=0, has_side_effects=True, vmem_limit_bytes=40 * 1024 * 1024),
            name="dft3",
        )(*parts, g_filter, jnp.asarray(lane_matrix()), jnp.asarray(sublane_twiddle()))
        return pl.pallas_call(
            put,
            out_shape=[jax.ShapeDtypeStruct((32, 16, 32, 64), f32)] * 2,
            in_specs=[pl.BlockSpec(memory_space=pltpu.VMEM)] * 6,
            out_specs=[pl.BlockSpec(memory_space=pltpu.HBM)] * 2,
            scratch_shapes=[pltpu.VMEM((PACK, 8, 32, 64), f32)] * 2 + [pltpu.VMEM((256, 512), f32), pltpu.SemaphoreType.DMA],
            compiler_params=pltpu.CompilerParams(vmem_limit_bytes=8 * 1024 * 1024),
            name="put",
        )(*spectrum)

    field_spec = P("fld", None, "row", "col")
    out_spec = P("fld", "row", "col", None)
    return jax.shard_map(local_forward, mesh=mesh, in_specs=(field_spec, field_spec, P("row", "col", None)),
                         out_specs=(out_spec, out_spec), check_vma=False)
```

```python
import functools
import math

import jax
import jax.numpy as jnp
import numpy as np
from jax import lax
from jax.experimental import pallas as pl
from jax.experimental.pallas import tpu as pltpu
from jax.sharding import PartitionSpec as P

MESH = pl.DeviceIdType.MESH
HALF = math.sqrt(0.5)
GROUPS, PACK, UNITS, RING, LAG, BEHIND = 8, 4, 32, 4, 5, 2


def interleave(even, odd):
    return [v for pair in zip(even, odd) for v in pair]


def dft4(b):
    (r0, i0), (r1, i1), (r2, i2), (r3, i3) = b
    sr0, si0, sr1, si1 = r0 + r2, i0 + i2, r0 - r2, i0 - i2
    sr2, si2, sr3, si3 = r1 + r3, i1 + i3, r1 - r3, i1 - i3
    return [(sr0 + sr2, si0 + si2), (sr1 + si3, si1 - sr3), (sr0 - sr2, si0 - si2), (sr1 - si3, si1 + sr3)]


def dft8(a):
    pairs = list(zip(a[:4], a[4:]))
    even = [(vr + wr, vi + wi) for (vr, vi), (wr, wi) in pairs]
    odd = [(vr - wr, vi - wi) for (vr, vi), (wr, wi) in pairs]
    o0, (r1, i1), (r2, i2), (r3, i3) = odd
    odd = [o0, ((r1 + i1) * HALF, (i1 - r1) * HALF), (i2, -r2), ((i3 - r3) * HALF, (r3 + i3) * -HALF)]
    even, odd = dft4(even), dft4(odd)
    return interleave(even, odd)


def rotate(v):
    sign = jnp.where(lax.broadcasted_iota(jnp.int32, v.shape, 0) < 4, 1.0, -1.0)
    return pltpu.roll(v, 4, 0) * sign


def packed_dft4(b):
    b0, b1, b2, b3 = b
    s0, s1, s2, s3 = b0 + b2, b0 - b2, b1 + b3, rotate(b1 - b3)
    return [s0 + s2, s1 + s3, s0 - s2, s1 - s3]


def packed_dft8(a):
    pairs = list(zip(a[:4], a[4:]))
    even = packed_dft4([v + w for v, w in pairs])
    o0, o1, o2, o3 = [v - w for v, w in pairs]
    odd = packed_dft4([o0, (rotate(o1) + o1) * HALF, rotate(o2), (rotate(o3) - o3) * HALF])
    return interleave(even, odd)


def times(a, tr, ti):
    return a[0] * tr - a[1] * ti, a[0] * ti + a[1] * tr


def twiddle(m):
    angle = -2.0 * math.pi * (m % 64) / 64.0
    return math.cos(angle) / 8.0, math.sin(angle) / 8.0


def lane_matrix():
    z, kz = np.arange(64), np.arange(64)
    angle = 2.0 * np.pi * ((z[:, None] * kz[None, :]) % 64) / 64.0
    cos, sin = np.cos(angle) / 8.0, np.sin(angle) / 8.0
    blocks = np.stack([np.concatenate([cos, -sin], 1), np.concatenate([sin, cos], 1)])
    out = np.zeros((2, 2, PACK, 32, PACK, 128))
    for c in range(2):
        for f in range(PACK):
            out[c, :, f, :, f, :] = blocks[:, 32 * c : 32 * c + 32]
    return out.reshape(2, 256, PACK * 128).astype(np.float32)


def sublane_twiddle():
    k1, x2 = np.arange(8), np.arange(8)
    angle = -2.0 * np.pi * (k1[:, None] * x2[None, :]) / 64.0
    both = np.stack([np.cos(angle), np.sin(angle)]) / 8.0
    return np.broadcast_to(both[..., None], (2, 8, 8, 128)).astype(np.float32)


def gather(dst, lane, plane):
    for kx in range(8):
        for q in range(2):
            dst[pl.ds(32 * kx, 32), pl.ds(lane + 128 * q, 128)] = plane(kx // 4, pl.ds(4 * q + kx % 4, 32, stride=8))


def lane_product(lhs, mat, gain, outr, outi, at):
    for n in range(2):
        w = jnp.dot(lhs[...], mat[:, 256 * n : 256 * n + 256], precision=lax.Precision.HIGHEST,
                    preferred_element_type=jnp.float32)
        for f in range(2):
            pair = w[:, 128 * f : 128 * f + 128] * gain
            outr[at(2 * n + f)] = pair[:, :64].reshape(8, 32, 64)
            outi[at(2 * n + f)] = pair[:, 64:].reshape(8, 32, 64)


def body(ur, ui, gf, wz, tw, outr, outi, wv, own, got, gv, inp, xbuf, b2, r2, tv, gs, asc, bsc, lsc,
           in_sem, q_sem, c_sem, s1, d1, s2, d2):
    row, col = lax.axis_index("row"), lax.axis_index("col")
    core = lax.rem(row, 2)
    dests = [1 + 2 * core, 2 - core, 3 - core]
    other = 1 - col

    def arrived(ref, sem):
        pltpu.make_async_remote_copy(src_ref=ref, dst_ref=ref, send_sem=sem, recv_sem=sem,
                                     device_id={"row": row}, device_id_type=MESH).wait_recv()

    def load(g, k):
        src, dst = (ur, ui)[k], inp.at[k]
        return pltpu.make_async_copy(src.at[g], dst.at[lax.rem(g, RING)], in_sem.at[lax.rem(g, RING)])

    def piece(i, k):
        src, dst = (ur, ui)[k], inp.at[k]
        part = (0, slice(None), pl.ds(2 * i, 2))
        return pltpu.make_async_copy(src.at[part], dst.at[part], q_sem.at[i])

    consts = [
        pltpu.make_async_copy(tw, tv, c_sem.at[0]),
        pltpu.make_async_copy(wz.at[col], wv.at[pl.ds(0, 256)], c_sem.at[1]),
        pltpu.make_async_copy(wz.at[other], wv.at[pl.ds(256, 256)], c_sem.at[1]),
        pltpu.make_async_copy(gf, gs, c_sem.at[2]),
    ]
    def start_piece(i):
        piece(i, 0).start()
        piece(i, 1).start()

    consts[0].start()
    start_piece(0)
    barrier = pltpu.get_barrier_semaphore()
    for p in (1, 2, 3):
        pl.semaphore_signal(barrier, inc=1, device_id={"row": lax.rem(row + p, 4)}, device_id_type=MESH)
    pl.semaphore_signal(barrier, inc=1, device_id={"col": other}, device_id_type=MESH)

    @pl.loop(1, 8)
    def _(i):
        start_piece(i)


    def step_x(g, first, count):
        ring = lax.rem(g, RING)
        bases = [4 * g * 7 + 3 + lax.rem(k + 4 - row, 4) for k in range(4)]

        def one(i, s):
            y = first + 2 * i + s
            ar = inp[0, ring, :, y].reshape(PACK * 32, 64).T
            ai = inp[1, ring, :, y].reshape(PACK * 32, 64).T
            a = dft8([(ar[8 * j : 8 * j + 8], ai[8 * j : 8 * j + 8]) for j in range(8)])
            for k1 in range(8):
                vr, vi = times(a[k1], tv[0, k1], tv[1, k1])
                asc[s, 0, pl.ds(8 * k1, 8), :] = vr
                asc[s, 1, pl.ds(8 * k1, 8), :] = vi
            b = dft8([tuple(asc[s, q, pl.ds(x2, 8, stride=8), :] for q in range(2)) for x2 in range(8)])
            top = lax.broadcasted_iota(jnp.int32, (8, 128), 0) < 4
            for k2, (vr, vi) in enumerate(b):
                at = bases[k2 // 2] + 14 * (k2 % 2)
                xbuf[at, y] = jnp.where(top, vr, pltpu.roll(vi, 4, 0))
                xbuf[at + 7, y] = jnp.where(top, pltpu.roll(vr, 4, 0), vi)

        def pair(i):
            one(i, 0)
            one(i, 1)

        pl.loop(0, count // 2)(pair) if count > 2 else pair(0)

    def send_row(u, j, first=0, count=16):
        p = dests[j]
        return pltpu.make_async_remote_copy(
            src_ref=xbuf.at[u * 7 + 3 + p, pl.ds(first, count)], dst_ref=xbuf.at[u * 7 + 3 - p, pl.ds(first, count)],
            send_sem=s1, recv_sem=d1.at[u],
            device_id={"row": lax.rem(row + p, 4)}, device_id_type=MESH)

    def send_col(u, dst):
        return pltpu.make_async_remote_copy(
            src_ref=b2.at[u * 2 + other], dst_ref=dst,
            send_sem=s2, recv_sem=d2.at[u // 2], device_id={"col": other}, device_id_type=MESH)

    def step_y(u):
        arrived(xbuf.at[pl.ds(u * 7, 3)], d1.at[u])
        slots = [u * 7 + lax.rem(r + 7 - row, 4) for r in range(4)]
        for y2 in range(8):
            a = packed_dft8([xbuf[slots[y1 // 2], 8 * (y1 % 2) + y2] for y1 in range(8)])
            for k1 in range(8):
                tr, ti = twiddle(k1 * y2)
                bsc[k1, y2] = a[k1] * tr - rotate(a[k1]) * ti if k1 * y2 else a[k1] * tr
        for k1 in range(8):
            b = packed_dft8([bsc[k1, y2] for y2 in range(8)])
            for k2 in range(8):
                b2[u * 2 + k2 // 4, pl.ds(8 * (k1 + 8 * (k2 % 4)), 8), :] = b[k2]

        @pl.when(u < UNITS - 2)
        def _():
            send_col(u, r2.at[u]).start()

        @pl.when(u >= UNITS - 2)
        def _():
            send_col(u, got.at[u - UNITS + 2]).start()

    def step_z(m):
        gather(lsc, 0, lambda v, rows: b2[(2 * m + v) * 2 + col, rows, :])
        arrived(r2.at[pl.ds(2 * m, 2)], d2.at[m])
        gather(lsc, 256, lambda v, rows: r2[2 * m + v, rows, :])
        gain = gv[pl.ds(pl.multiple_of(256 * lax.rem(m, 2), 256), 256), :]
        lane_product(lsc, wv, gain, outr, outi, lambda f: (PACK * (m // 2) + f, pl.ds(8 * lax.rem(m, 2), 8)))

    consts[0].wait()
    def first_group(i):
        arrived(inp.at[:, 0, :, pl.ds(2 * i, 2)], q_sem.at[i])
        step_x(0, 2 * i, 2)

    first_group(0)
    pl.semaphore_wait(barrier, 4)

    @pl.when(core == 0)
    def _():
        send_row(0, 1, 0, 2).start()

    @pl.loop(1, 8)
    def _(i):
        first_group(i)

        @pl.when(core == 0)
        def _():
            send_row(0, 1, 2 * i, 2).start()

        @pl.when((core == 1) & (i >= BEHIND))
        def _():
            send_row(0, 1, 2 * (i - BEHIND), 2).start()

    @pl.when(core == 1)
    def _():
        send_row(0, 1, 16 - 2 * BEHIND, 2 * BEHIND).start()

    send_row(0, 0).start()
    send_row(1, 1).start()
    send_row(1, 0).start()
    send_row(0, 2).start()

    def send_rows(first, last):
        @pl.loop(first, last)
        def _(u):
            send_row(u, 1).start()
            send_row(u, 0).start()
            send_row(u - 1, 2).start()

    send_rows(2, 4)

    @pl.loop(1, RING)
    def _(g):
        load(g, 0).start()
        load(g, 1).start()

    for copy in consts[1:]:
        copy.start()
    step_y(0)
    for k in range(2):
        load(RING, k).start()
    arrived(inp.at[:, 1], in_sem.at[1])
    step_x(1, 0, 16)
    send_rows(4, 8)
    for k in range(2):
        load(RING + 1, k).start()
    arrived(wv, c_sem.at[1])
    consts[3].wait()
    gain = gs[...].reshape(512, 64)
    gv[...] = jnp.concatenate([gain, gain], axis=1)

    @pl.loop(1, UNITS + LAG - 3)
    def _(t):
        @pl.when(t < UNITS)
        def _():
            step_y(t)

        g, i = (t + 7) // 4, lax.rem(t + 3, 4)

        @pl.when(g < GROUPS)
        def _():
            @pl.when(i == 0)
            def _():
                arrived(inp.at[:, lax.rem(g, RING)], in_sem.at[lax.rem(g, RING)])

            step_x(g, 4 * i, 4)

            @pl.when(i == 3)
            def _():
                send_rows(4 * g, 4 * g + 4)

                @pl.when(g == GROUPS - 1)
                def _():
                    send_row(UNITS - 1, 2).start()

                @pl.when(g + RING < GROUPS)
                def _():
                    load(g + RING, 0).start()
                    load(g + RING, 1).start()

        @pl.when((t >= LAG) & (lax.rem(t - LAG, 2) == 0))
        def _():
            step_z((t - LAG) // 2)

    arrived(xbuf.at[pl.ds(0, 3 * UNITS)], s1)
    for v in range(2):
        own[v] = b2[2 * (UNITS - 2 + v) + col]
    arrived(got, d2.at[UNITS // 2 - 1])
    arrived(b2.at[pl.ds(0, UNITS)], s2)


def kernel(*refs):
    dma = pltpu.SemaphoreType.DMA
    pl.run_scoped(functools.partial(body, *refs), in_sem=dma((RING,)), q_sem=dma((8,)), c_sem=dma((3,)), s1=dma,
                  d1=dma((UNITS,)), s2=dma, d2=dma((UNITS // 2,)))


def put(vr, vi, mat, own, got, gain, outr, outi, lr, li, lhs, sem):
    cuts = [(pl.ds(7 * i, 7), slice(None)) for i in range(4)] + [(pl.ds(28, 4), pl.ds(0, 8))]
    copies = [pltpu.make_async_copy(v.at[cut], o.at[cut], sem) for cut in cuts for v, o in ((vr, outr), (vi, outi))]
    for copy in copies:
        copy.start()
    gather(lhs, 0, lambda v, rows: own[v, rows, :])
    gather(lhs, 256, lambda v, rows: got[v, rows, :])
    lane_product(lhs, mat, gain[256:, :], lr, li, lambda f: f)
    cut = (pl.ds(28, 4), pl.ds(8, 8))
    tail = [pltpu.make_async_copy(v, o.at[cut], sem) for v, o in ((lr, outr), (li, outi))]
    for copy in tail:
        copy.start()
    for copy in copies + tail:
        copy.wait()


def solution(mesh):
    f32 = jnp.float32

    def local_forward(u_real, u_imag, g_filter):
        parts = [jnp.transpose(v, (0, 2, 3, 1)).reshape(GROUPS, PACK, 16, 32, 64) for v in (u_real, u_imag)]
        spectrum = pl.pallas_call(
            kernel,
            out_shape=[pltpu.VMEM((32, 16, 32, 64), f32)] * 2 + [
                pltpu.VMEM((512, 512), f32), pltpu.VMEM((2, 256, 128), f32), pltpu.VMEM((2, 256, 128), f32),
                pltpu.VMEM((512, 128), f32)],
            in_specs=[pl.BlockSpec(memory_space=pltpu.HBM)] * 5,
            out_specs=[pl.BlockSpec(memory_space=pltpu.VMEM)] * 6,
            scratch_shapes=[
                pltpu.VMEM((2, RING, PACK, 16, 32, 64), f32),
                pltpu.VMEM((UNITS * 7, 16, 8, 128), f32),
                pltpu.VMEM((UNITS * 2, 256, 128), f32),
                pltpu.VMEM((UNITS, 256, 128), f32),
                pltpu.VMEM((2, 8, 8, 128), f32),
                pltpu.VMEM((16, 32, 64), f32),
                pltpu.VMEM((2, 2, 64, 128), f32),
                pltpu.VMEM((8, 8, 8, 128), f32),
                pltpu.VMEM((256, 512), f32),
            ],
            compiler_params=pltpu.CompilerParams(
                collective_id=0, has_side_effects=True, vmem_limit_bytes=40 * 1024 * 1024),
            name="dft3",
        )(*parts, g_filter, jnp.asarray(lane_matrix()), jnp.asarray(sublane_twiddle()))
        return pl.pallas_call(
            put,
            out_shape=[jax.ShapeDtypeStruct((32, 16, 32, 64), f32)] * 2,
            in_specs=[pl.BlockSpec(memory_space=pltpu.VMEM)] * 6,
            out_specs=[pl.BlockSpec(memory_space=pltpu.HBM)] * 2,
            scratch_shapes=[pltpu.VMEM((PACK, 8, 32, 64), f32)] * 2 + [pltpu.VMEM((256, 512), f32), pltpu.SemaphoreType.DMA],
            compiler_params=pltpu.CompilerParams(vmem_limit_bytes=8 * 1024 * 1024),
            name="put",
        )(*spectrum)

    field_spec = P("fld", None, "row", "col")
    out_spec = P("fld", "row", "col", None)
    return jax.shard_map(local_forward, mesh=mesh, in_specs=(field_spec, field_spec, P("row", "col", None)),
                         out_specs=(out_spec, out_spec), check_vma=False)
```

```python
import functools
import math

import jax
import jax.numpy as jnp
import numpy as np
from jax import lax
from jax.experimental import pallas as pl
from jax.experimental.pallas import tpu as pltpu
from jax.sharding import PartitionSpec as P

MESH = pl.DeviceIdType.MESH
HALF = math.sqrt(0.5)
GROUPS, PACK, UNITS, RING, LAG, BEHIND = 8, 4, 32, 4, 5, 2


def interleave(even, odd):
    return [v for pair in zip(even, odd) for v in pair]


def dft4(b):
    (r0, i0), (r1, i1), (r2, i2), (r3, i3) = b
    sr0, si0, sr1, si1 = r0 + r2, i0 + i2, r0 - r2, i0 - i2
    sr2, si2, sr3, si3 = r1 + r3, i1 + i3, r1 - r3, i1 - i3
    return [(sr0 + sr2, si0 + si2), (sr1 + si3, si1 - sr3), (sr0 - sr2, si0 - si2), (sr1 - si3, si1 + sr3)]


def dft8(a):
    pairs = list(zip(a[:4], a[4:]))
    even = [(vr + wr, vi + wi) for (vr, vi), (wr, wi) in pairs]
    odd = [(vr - wr, vi - wi) for (vr, vi), (wr, wi) in pairs]
    o0, (r1, i1), (r2, i2), (r3, i3) = odd
    odd = [o0, ((r1 + i1) * HALF, (i1 - r1) * HALF), (i2, -r2), ((i3 - r3) * HALF, (r3 + i3) * -HALF)]
    even, odd = dft4(even), dft4(odd)
    return interleave(even, odd)


def rotate(v):
    sign = jnp.where(lax.broadcasted_iota(jnp.int32, v.shape, 0) < 4, 1.0, -1.0)
    return pltpu.roll(v, 4, 0) * sign


def packed_dft4(b):
    b0, b1, b2, b3 = b
    s0, s1, s2, s3 = b0 + b2, b0 - b2, b1 + b3, rotate(b1 - b3)
    return [s0 + s2, s1 + s3, s0 - s2, s1 - s3]


def packed_dft8(a):
    pairs = list(zip(a[:4], a[4:]))
    even = packed_dft4([v + w for v, w in pairs])
    o0, o1, o2, o3 = [v - w for v, w in pairs]
    odd = packed_dft4([o0, (rotate(o1) + o1) * HALF, rotate(o2), (rotate(o3) - o3) * HALF])
    return interleave(even, odd)


def times(a, tr, ti):
    return a[0] * tr - a[1] * ti, a[0] * ti + a[1] * tr


def twiddle(m):
    angle = -2.0 * math.pi * (m % 64) / 64.0
    return math.cos(angle) / 8.0, math.sin(angle) / 8.0


def lane_matrix():
    z, kz = np.arange(64), np.arange(64)
    angle = 2.0 * np.pi * ((z[:, None] * kz[None, :]) % 64) / 64.0
    cos, sin = np.cos(angle) / 8.0, np.sin(angle) / 8.0
    blocks = np.stack([np.concatenate([cos, -sin], 1), np.concatenate([sin, cos], 1)])
    out = np.zeros((2, 2, PACK, 32, PACK, 128))
    for c in range(2):
        for f in range(PACK):
            out[c, :, f, :, f, :] = blocks[:, 32 * c : 32 * c + 32]
    return out.reshape(2, 256, PACK * 128).astype(np.float32)


def sublane_twiddle():
    k1, x2 = np.arange(8), np.arange(8)
    angle = -2.0 * np.pi * (k1[:, None] * x2[None, :]) / 64.0
    both = np.stack([np.cos(angle), np.sin(angle)]) / 8.0
    return np.broadcast_to(both[..., None], (2, 8, 8, 128)).astype(np.float32)


def gather(dst, lane, plane):
    for kx in range(8):
        for q in range(2):
            dst[pl.ds(32 * kx, 32), pl.ds(lane + 128 * q, 128)] = plane(kx // 4, pl.ds(4 * q + kx % 4, 32, stride=8))


def lane_product(lhs, mat, gain, outr, outi, at):
    for n in range(2):
        w = jnp.dot(lhs[...], mat[:, 256 * n : 256 * n + 256], precision=lax.Precision.HIGHEST,
                    preferred_element_type=jnp.float32)
        for f in range(2):
            pair = w[:, 128 * f : 128 * f + 128] * gain
            outr[at(2 * n + f)] = pair[:, :64].reshape(8, 32, 64)
            outi[at(2 * n + f)] = pair[:, 64:].reshape(8, 32, 64)


def body(ur, ui, gf, wz, tw, outr, outi, wv, own, got, gv, inp, xbuf, b2, r2, tv, gs, asc, bsc, lsc,
           in_sem, q_sem, c_sem, s1, d1, s2, d2):
    row, col = lax.axis_index("row"), lax.axis_index("col")
    core = lax.rem(row, 2)
    dests = [1 + 2 * core, 2 - core, 3 - core]
    other = 1 - col

    def arrived(ref, sem):
        pltpu.make_async_remote_copy(src_ref=ref, dst_ref=ref, send_sem=sem, recv_sem=sem,
                                     device_id={"row": row}, device_id_type=MESH).wait_recv()

    def load(g, k):
        src, dst = (ur, ui)[k], inp.at[k]
        return pltpu.make_async_copy(src.at[g], dst.at[lax.rem(g, RING)], in_sem.at[lax.rem(g, RING)])

    def piece(i, k):
        src, dst = (ur, ui)[k], inp.at[k]
        part = (0, slice(None), pl.ds(2 * i, 2))
        return pltpu.make_async_copy(src.at[part], dst.at[part], q_sem.at[i])

    consts = [
        pltpu.make_async_copy(tw, tv, c_sem.at[0]),
        pltpu.make_async_copy(wz.at[col], wv.at[pl.ds(0, 256)], c_sem.at[1]),
        pltpu.make_async_copy(wz.at[other], wv.at[pl.ds(256, 256)], c_sem.at[1]),
        pltpu.make_async_copy(gf, gs, c_sem.at[2]),
    ]
    def start_piece(i):
        piece(i, 0).start()
        piece(i, 1).start()

    consts[0].start()
    start_piece(0)
    barrier = pltpu.get_barrier_semaphore()
    for p in (1, 2, 3):
        pl.semaphore_signal(barrier, inc=1, device_id={"row": lax.rem(row + p, 4)}, device_id_type=MESH)
    pl.semaphore_signal(barrier, inc=1, device_id={"col": other}, device_id_type=MESH)

    @pl.loop(1, 8)
    def _(i):
        start_piece(i)


    def step_x(g, first, count):
        ring = lax.rem(g, RING)
        bases = [4 * g * 7 + 3 + lax.rem(k + 4 - row, 4) for k in range(4)]

        def one(i, s):
            y = first + 2 * i + s
            ar = inp[0, ring, :, y].reshape(PACK * 32, 64).T
            ai = inp[1, ring, :, y].reshape(PACK * 32, 64).T
            a = dft8([(ar[8 * j : 8 * j + 8], ai[8 * j : 8 * j + 8]) for j in range(8)])
            for k1 in range(8):
                vr, vi = times(a[k1], tv[0, k1], tv[1, k1])
                asc[s, 0, pl.ds(8 * k1, 8), :] = vr
                asc[s, 1, pl.ds(8 * k1, 8), :] = vi
            b = dft8([tuple(asc[s, q, pl.ds(x2, 8, stride=8), :] for q in range(2)) for x2 in range(8)])
            top = lax.broadcasted_iota(jnp.int32, (8, 128), 0) < 4
            for k2, (vr, vi) in enumerate(b):
                at = bases[k2 // 2] + 14 * (k2 % 2)
                xbuf[at, y] = jnp.where(top, vr, pltpu.roll(vi, 4, 0))
                xbuf[at + 7, y] = jnp.where(top, pltpu.roll(vr, 4, 0), vi)

        def pair(i):
            one(i, 0)
            one(i, 1)

        pl.loop(0, count // 2)(pair) if count > 2 else pair(0)

    def send_row(u, j, first=0, count=16):
        p = dests[j]
        return pltpu.make_async_remote_copy(
            src_ref=xbuf.at[u * 7 + 3 + p, pl.ds(first, count)], dst_ref=xbuf.at[u * 7 + 3 - p, pl.ds(first, count)],
            send_sem=s1, recv_sem=d1.at[u],
            device_id={"row": lax.rem(row + p, 4)}, device_id_type=MESH)

    def send_col(u, dst):
        return pltpu.make_async_remote_copy(
            src_ref=b2.at[u * 2 + other], dst_ref=dst,
            send_sem=s2, recv_sem=d2.at[u // 2], device_id={"col": other}, device_id_type=MESH)

    def step_y(u):
        arrived(xbuf.at[pl.ds(u * 7, 3)], d1.at[u])
        slots = [u * 7 + lax.rem(r + 7 - row, 4) for r in range(4)]
        for y2 in range(8):
            a = packed_dft8([xbuf[slots[y1 // 2], 8 * (y1 % 2) + y2] for y1 in range(8)])
            for k1 in range(8):
                tr, ti = twiddle(k1 * y2)
                bsc[k1, y2] = a[k1] * tr - rotate(a[k1]) * ti if k1 * y2 else a[k1] * tr
        for k1 in range(8):
            b = packed_dft8([bsc[k1, y2] for y2 in range(8)])
            for k2 in range(8):
                b2[u * 2 + k2 // 4, pl.ds(8 * (k1 + 8 * (k2 % 4)), 8), :] = b[k2]

        @pl.when(u < UNITS - 2)
        def _():
            send_col(u, r2.at[u]).start()

        @pl.when(u >= UNITS - 2)
        def _():
            send_col(u, got.at[u - UNITS + 2]).start()

    def step_z(m):
        gather(lsc, 0, lambda v, rows: b2[(2 * m + v) * 2 + col, rows, :])
        arrived(r2.at[pl.ds(2 * m, 2)], d2.at[m])
        gather(lsc, 256, lambda v, rows: r2[2 * m + v, rows, :])
        gain = gv[pl.ds(pl.multiple_of(256 * lax.rem(m, 2), 256), 256), :]
        lane_product(lsc, wv, gain, outr, outi, lambda f: (PACK * (m // 2) + f, pl.ds(8 * lax.rem(m, 2), 8)))

    consts[0].wait()
    def first_group(i):
        arrived(inp.at[:, 0, :, pl.ds(2 * i, 2)], q_sem.at[i])
        step_x(0, 2 * i, 2)

    first_group(0)
    pl.semaphore_wait(barrier, 4)

    @pl.when(core == 0)
    def _():
        send_row(0, 1, 0, 2).start()

    @pl.loop(1, 8)
    def _(i):
        first_group(i)

        @pl.when(core == 0)
        def _():
            send_row(0, 1, 2 * i, 2).start()

        @pl.when((core == 1) & (i >= BEHIND))
        def _():
            send_row(0, 1, 2 * (i - BEHIND), 2).start()

    @pl.when(core == 1)
    def _():
        send_row(0, 1, 16 - 2 * BEHIND, 2 * BEHIND).start()

    send_row(0, 0).start()

    @pl.when(core == 1)
    def _():
        pl.delay(500)

    send_row(1, 1).start()
    send_row(1, 0).start()
    send_row(0, 2).start()

    def send_rows(first, last):
        @pl.loop(first, last)
        def _(u):
            send_row(u, 1).start()
            send_row(u, 0).start()
            send_row(u - 1, 2).start()

    send_rows(2, 4)

    @pl.loop(1, RING)
    def _(g):
        load(g, 0).start()
        load(g, 1).start()

    for copy in consts[1:]:
        copy.start()
    step_y(0)
    for k in range(2):
        load(RING, k).start()
    arrived(inp.at[:, 1], in_sem.at[1])
    step_x(1, 0, 16)
    send_rows(4, 8)
    for k in range(2):
        load(RING + 1, k).start()
    arrived(wv, c_sem.at[1])
    consts[3].wait()
    gain = gs[...].reshape(512, 64)
    gv[...] = jnp.concatenate([gain, gain], axis=1)

    @pl.loop(1, UNITS + LAG - 3)
    def _(t):
        @pl.when(t < UNITS)
        def _():
            step_y(t)

        g, i = (t + 7) // 4, lax.rem(t + 3, 4)

        @pl.when(g < GROUPS)
        def _():
            @pl.when(i == 0)
            def _():
                arrived(inp.at[:, lax.rem(g, RING)], in_sem.at[lax.rem(g, RING)])

            step_x(g, 4 * i, 4)

            @pl.when(i == 3)
            def _():
                send_rows(4 * g, 4 * g + 4)

                @pl.when(g == GROUPS - 1)
                def _():
                    send_row(UNITS - 1, 2).start()

                @pl.when(g + RING < GROUPS)
                def _():
                    load(g + RING, 0).start()
                    load(g + RING, 1).start()

        @pl.when((t >= LAG) & (lax.rem(t - LAG, 2) == 0))
        def _():
            step_z((t - LAG) // 2)

    arrived(xbuf.at[pl.ds(0, 3 * UNITS)], s1)
    for v in range(2):
        own[v] = b2[2 * (UNITS - 2 + v) + col]
    arrived(got, d2.at[UNITS // 2 - 1])
    arrived(b2.at[pl.ds(0, UNITS)], s2)


def kernel(*refs):
    dma = pltpu.SemaphoreType.DMA
    pl.run_scoped(functools.partial(body, *refs), in_sem=dma((RING,)), q_sem=dma((8,)), c_sem=dma((3,)), s1=dma,
                  d1=dma((UNITS,)), s2=dma, d2=dma((UNITS // 2,)))


def put(vr, vi, mat, own, got, gain, outr, outi, lr, li, lhs, sem):
    cuts = [(pl.ds(7 * i, 7), slice(None)) for i in range(4)] + [(pl.ds(28, 4), pl.ds(0, 8))]
    copies = [pltpu.make_async_copy(v.at[cut], o.at[cut], sem) for cut in cuts for v, o in ((vr, outr), (vi, outi))]
    for copy in copies:
        copy.start()
    gather(lhs, 0, lambda v, rows: own[v, rows, :])
    gather(lhs, 256, lambda v, rows: got[v, rows, :])
    lane_product(lhs, mat, gain[256:, :], lr, li, lambda f: f)
    cut = (pl.ds(28, 4), pl.ds(8, 8))
    tail = [pltpu.make_async_copy(v, o.at[cut], sem) for v, o in ((lr, outr), (li, outi))]
    for copy in tail:
        copy.start()
    for copy in copies + tail:
        copy.wait()


def solution(mesh):
    f32 = jnp.float32

    def local_forward(u_real, u_imag, g_filter):
        parts = [jnp.transpose(v, (0, 2, 3, 1)).reshape(GROUPS, PACK, 16, 32, 64) for v in (u_real, u_imag)]
        spectrum = pl.pallas_call(
            kernel,
            out_shape=[pltpu.VMEM((32, 16, 32, 64), f32)] * 2 + [
                pltpu.VMEM((512, 512), f32), pltpu.VMEM((2, 256, 128), f32), pltpu.VMEM((2, 256, 128), f32),
                pltpu.VMEM((512, 128), f32)],
            in_specs=[pl.BlockSpec(memory_space=pltpu.HBM)] * 5,
            out_specs=[pl.BlockSpec(memory_space=pltpu.VMEM)] * 6,
            scratch_shapes=[
                pltpu.VMEM((2, RING, PACK, 16, 32, 64), f32),
                pltpu.VMEM((UNITS * 7, 16, 8, 128), f32),
                pltpu.VMEM((UNITS * 2, 256, 128), f32),
                pltpu.VMEM((UNITS, 256, 128), f32),
                pltpu.VMEM((2, 8, 8, 128), f32),
                pltpu.VMEM((16, 32, 64), f32),
                pltpu.VMEM((2, 2, 64, 128), f32),
                pltpu.VMEM((8, 8, 8, 128), f32),
                pltpu.VMEM((256, 512), f32),
            ],
            compiler_params=pltpu.CompilerParams(
                collective_id=0, has_side_effects=True, vmem_limit_bytes=40 * 1024 * 1024),
            name="dft3",
        )(*parts, g_filter, jnp.asarray(lane_matrix()), jnp.asarray(sublane_twiddle()))
        return pl.pallas_call(
            put,
            out_shape=[jax.ShapeDtypeStruct((32, 16, 32, 64), f32)] * 2,
            in_specs=[pl.BlockSpec(memory_space=pltpu.VMEM)] * 6,
            out_specs=[pl.BlockSpec(memory_space=pltpu.HBM)] * 2,
            scratch_shapes=[pltpu.VMEM((PACK, 8, 32, 64), f32)] * 2 + [pltpu.VMEM((256, 512), f32), pltpu.SemaphoreType.DMA],
            compiler_params=pltpu.CompilerParams(vmem_limit_bytes=8 * 1024 * 1024),
            name="put",
        )(*spectrum)

    field_spec = P("fld", None, "row", "col")
    out_spec = P("fld", "row", "col", None)
    return jax.shard_map(local_forward, mesh=mesh, in_specs=(field_spec, field_spec, P("row", "col", None)),
                         out_specs=(out_spec, out_spec), check_vma=False)
```

```python
import functools
import math

import jax
import jax.numpy as jnp
import numpy as np
from jax import lax
from jax.experimental import pallas as pl
from jax.experimental.pallas import tpu as pltpu
from jax.sharding import PartitionSpec as P

MESH = pl.DeviceIdType.MESH
HALF = math.sqrt(0.5)
GROUPS, PACK, UNITS, RING, LAG = 8, 4, 32, 4, 3


def interleave(even, odd):
    return [v for pair in zip(even, odd) for v in pair]


def dft4(b):
    (r0, i0), (r1, i1), (r2, i2), (r3, i3) = b
    sr0, si0, sr1, si1 = r0 + r2, i0 + i2, r0 - r2, i0 - i2
    sr2, si2, sr3, si3 = r1 + r3, i1 + i3, r1 - r3, i1 - i3
    return [(sr0 + sr2, si0 + si2), (sr1 + si3, si1 - sr3), (sr0 - sr2, si0 - si2), (sr1 - si3, si1 + sr3)]


def dft8(a):
    pairs = list(zip(a[:4], a[4:]))
    even = [(vr + wr, vi + wi) for (vr, vi), (wr, wi) in pairs]
    odd = [(vr - wr, vi - wi) for (vr, vi), (wr, wi) in pairs]
    o0, (r1, i1), (r2, i2), (r3, i3) = odd
    odd = [o0, ((r1 + i1) * HALF, (i1 - r1) * HALF), (i2, -r2), ((i3 - r3) * HALF, (r3 + i3) * -HALF)]
    even, odd = dft4(even), dft4(odd)
    return interleave(even, odd)


def rotate(v):
    sign = jnp.where(lax.broadcasted_iota(jnp.int32, v.shape, 0) < 4, 1.0, -1.0)
    return pltpu.roll(v, 4, 0) * sign


def packed_dft4(b):
    b0, b1, b2, b3 = b
    s0, s1, s2, s3 = b0 + b2, b0 - b2, b1 + b3, rotate(b1 - b3)
    return [s0 + s2, s1 + s3, s0 - s2, s1 - s3]


def packed_dft8(a):
    pairs = list(zip(a[:4], a[4:]))
    even = packed_dft4([v + w for v, w in pairs])
    o0, o1, o2, o3 = [v - w for v, w in pairs]
    odd = packed_dft4([o0, (rotate(o1) + o1) * HALF, rotate(o2), (rotate(o3) - o3) * HALF])
    return interleave(even, odd)


def times(a, tr, ti):
    return a[0] * tr - a[1] * ti, a[0] * ti + a[1] * tr


def twiddle(m):
    angle = -2.0 * math.pi * (m % 64) / 64.0
    return math.cos(angle) / 8.0, math.sin(angle) / 8.0


def lane_matrix():
    z, kz = np.arange(64), np.arange(64)
    angle = 2.0 * np.pi * ((z[:, None] * kz[None, :]) % 64) / 64.0
    cos, sin = np.cos(angle) / 8.0, np.sin(angle) / 8.0
    blocks = np.stack([np.concatenate([cos, -sin], 1), np.concatenate([sin, cos], 1)])
    out = np.zeros((2, 2, PACK, 32, PACK, 128))
    for c in range(2):
        for f in range(PACK):
            out[c, :, f, :, f, :] = blocks[:, 32 * c : 32 * c + 32]
    return out.reshape(2, 256, PACK * 128).astype(np.float32)


def sublane_twiddle():
    k1, x2 = np.arange(8), np.arange(8)
    angle = -2.0 * np.pi * (k1[:, None] * x2[None, :]) / 64.0
    both = np.stack([np.cos(angle), np.sin(angle)]) / 8.0
    return np.broadcast_to(both[..., None], (2, 8, 8, 128)).astype(np.float32)


def gather(dst, lane, plane):
    for kx in range(8):
        for q in range(2):
            dst[pl.ds(32 * kx, 32), pl.ds(lane + 128 * q, 128)] = plane(kx // 4, pl.ds(4 * q + kx % 4, 32, stride=8))


def lane_product(lhs, mat, gain, outr, outi, at):
    for n in range(2):
        w = jnp.dot(lhs[...], mat[:, 256 * n : 256 * n + 256], precision=lax.Precision.HIGHEST,
                    preferred_element_type=jnp.float32)
        for f in range(2):
            pair = w[:, 128 * f : 128 * f + 128] * gain
            outr[at(2 * n + f)] = pair[:, :64].reshape(8, 32, 64)
            outi[at(2 * n + f)] = pair[:, 64:].reshape(8, 32, 64)


def body(ur, ui, gf, wz, tw, outr, outi, wv, own, got, gv, inp, xbuf, b2, r2, tv, gs, asc, bsc, lsc,
           in_sem, q_sem, c_sem, s1, d1, s2, d2):
    row, col = lax.axis_index("row"), lax.axis_index("col")
    core = lax.rem(row, 2)
    dests = [1 + 2 * core, 2 - core, 3 - core]
    other = 1 - col

    def arrived(ref, sem):
        pltpu.make_async_remote_copy(src_ref=ref, dst_ref=ref, send_sem=sem, recv_sem=sem,
                                     device_id={"row": row}, device_id_type=MESH).wait_recv()

    def load(g, k):
        src, dst = (ur, ui)[k], inp.at[k]
        return pltpu.make_async_copy(src.at[g], dst.at[lax.rem(g, RING)], in_sem.at[lax.rem(g, RING)])

    def piece(i, k):
        src, dst = (ur, ui)[k], inp.at[k]
        part = (0, slice(None), pl.ds(2 * i, 2))
        return pltpu.make_async_copy(src.at[part], dst.at[part], q_sem.at[i])

    consts = [
        pltpu.make_async_copy(tw, tv, c_sem.at[0]),
        pltpu.make_async_copy(wz.at[col], wv.at[pl.ds(0, 256)], c_sem.at[1]),
        pltpu.make_async_copy(wz.at[other], wv.at[pl.ds(256, 256)], c_sem.at[1]),
        pltpu.make_async_copy(gf, gs, c_sem.at[2]),
    ]
    def start_piece(i):
        piece(i, 0).start()
        piece(i, 1).start()

    consts[0].start()
    start_piece(0)
    barrier = pltpu.get_barrier_semaphore()
    for p in (1, 2, 3):
        pl.semaphore_signal(barrier, inc=1, device_id={"row": lax.rem(row + p, 4)}, device_id_type=MESH)
    pl.semaphore_signal(barrier, inc=1, device_id={"col": other}, device_id_type=MESH)

    @pl.loop(1, 8)
    def _(i):
        start_piece(i)


    def step_x(g, first, count):
        ring = lax.rem(g, RING)
        bases = [4 * g * 7 + 3 + lax.rem(k + 4 - row, 4) for k in range(4)]

        def one(i, s):
            y = first + 2 * i + s
            ar = inp[0, ring, :, y].reshape(PACK * 32, 64).T
            ai = inp[1, ring, :, y].reshape(PACK * 32, 64).T
            a = dft8([(ar[8 * j : 8 * j + 8], ai[8 * j : 8 * j + 8]) for j in range(8)])
            for k1 in range(8):
                vr, vi = times(a[k1], tv[0, k1], tv[1, k1])
                asc[s, 0, pl.ds(8 * k1, 8), :] = vr
                asc[s, 1, pl.ds(8 * k1, 8), :] = vi
            b = dft8([tuple(asc[s, q, pl.ds(x2, 8, stride=8), :] for q in range(2)) for x2 in range(8)])
            top = lax.broadcasted_iota(jnp.int32, (8, 128), 0) < 4
            for k2, (vr, vi) in enumerate(b):
                at = bases[k2 // 2] + 14 * (k2 % 2)
                xbuf[at, y] = jnp.where(top, vr, pltpu.roll(vi, 4, 0))
                xbuf[at + 7, y] = jnp.where(top, pltpu.roll(vr, 4, 0), vi)

        def pair(i):
            one(i, 0)
            one(i, 1)

        pl.loop(0, count // 2)(pair) if count > 2 else pair(0)

    def send_row(u, j, first=0, count=16):
        p = dests[j]
        return pltpu.make_async_remote_copy(
            src_ref=xbuf.at[u * 7 + 3 + p, pl.ds(first, count)], dst_ref=xbuf.at[u * 7 + 3 - p, pl.ds(first, count)],
            send_sem=s1, recv_sem=d1.at[u],
            device_id={"row": lax.rem(row + p, 4)}, device_id_type=MESH)

    def send_col(u, dst):
        return pltpu.make_async_remote_copy(
            src_ref=b2.at[u * 2 + other], dst_ref=dst,
            send_sem=s2, recv_sem=d2.at[u // 2], device_id={"col": other}, device_id_type=MESH)

    def step_y(u):
        arrived(xbuf.at[pl.ds(u * 7, 3)], d1.at[u])
        slots = [u * 7 + lax.rem(r + 7 - row, 4) for r in range(4)]
        for y2 in range(8):
            a = packed_dft8([xbuf[slots[y1 // 2], 8 * (y1 % 2) + y2] for y1 in range(8)])
            for k1 in range(8):
                tr, ti = twiddle(k1 * y2)
                bsc[k1, y2] = a[k1] * tr - rotate(a[k1]) * ti if k1 * y2 else a[k1] * tr
        for k1 in range(8):
            b = packed_dft8([bsc[k1, y2] for y2 in range(8)])
            for k2 in range(8):
                b2[u * 2 + k2 // 4, pl.ds(8 * (k1 + 8 * (k2 % 4)), 8), :] = b[k2]

        @pl.when(u < UNITS - 2)
        def _():
            send_col(u, r2.at[u]).start()

        @pl.when(u >= UNITS - 2)
        def _():
            send_col(u, got.at[u - UNITS + 2]).start()

    def step_z(m):
        gather(lsc, 0, lambda v, rows: b2[(2 * m + v) * 2 + col, rows, :])
        arrived(r2.at[pl.ds(2 * m, 2)], d2.at[m])
        gather(lsc, 256, lambda v, rows: r2[2 * m + v, rows, :])
        gain = gv[pl.ds(pl.multiple_of(256 * lax.rem(m, 2), 256), 256), :]
        lane_product(lsc, wv, gain, outr, outi, lambda f: (PACK * (m // 2) + f, pl.ds(8 * lax.rem(m, 2), 8)))

    consts[0].wait()
    def first_group(i):
        arrived(inp.at[:, 0, :, pl.ds(2 * i, 2)], q_sem.at[i])
        step_x(0, 2 * i, 2)

    first_group(0)
    pl.semaphore_wait(barrier, 4)
    send_row(0, 1, 0, 2).start()

    @pl.loop(1, 8)
    def _(i):
        first_group(i)
        send_row(0, 1, 2 * i, 2).start()

    send_row(0, 0).start()
    send_row(1, 1).start()
    send_row(1, 0).start()
    send_row(0, 2).start()

    def send_rows(first, last):
        @pl.loop(first, last)
        def _(u):
            send_row(u, 1).start()
            send_row(u, 0).start()
            send_row(u - 1, 2).start()

    send_rows(2, 4)

    @pl.loop(1, RING)
    def _(g):
        load(g, 0).start()
        load(g, 1).start()

    for copy in consts[1:]:
        copy.start()
    step_y(0)
    for k in range(2):
        load(RING, k).start()
    arrived(inp.at[:, 1], in_sem.at[1])
    step_x(1, 0, 16)
    send_rows(4, 8)
    for k in range(2):
        load(RING + 1, k).start()
    arrived(wv, c_sem.at[1])
    consts[3].wait()
    gain = gs[...].reshape(512, 64)
    gv[...] = jnp.concatenate([gain, gain], axis=1)

    @pl.loop(1, UNITS + LAG - 3)
    def _(t):
        @pl.when(t < UNITS)
        def _():
            step_y(t)

        g, i = (t + 7) // 4, lax.rem(t + 3, 4)

        @pl.when(g < GROUPS)
        def _():
            @pl.when(i == 0)
            def _():
                arrived(inp.at[:, lax.rem(g, RING)], in_sem.at[lax.rem(g, RING)])

            step_x(g, 4 * i, 4)

            @pl.when(i == 3)
            def _():
                send_rows(4 * g, 4 * g + 4)

                @pl.when(g == GROUPS - 1)
                def _():
                    send_row(UNITS - 1, 2).start()

                @pl.when(g + RING < GROUPS)
                def _():
                    load(g + RING, 0).start()
                    load(g + RING, 1).start()

        @pl.when((t >= LAG) & (lax.rem(t - LAG, 2) == 0))
        def _():
            step_z((t - LAG) // 2)

    arrived(xbuf.at[pl.ds(0, 3 * UNITS)], s1)
    for v in range(2):
        own[v] = b2[2 * (UNITS - 2 + v) + col]
    arrived(got, d2.at[UNITS // 2 - 1])
    arrived(b2.at[pl.ds(0, UNITS)], s2)


def kernel(*refs):
    dma = pltpu.SemaphoreType.DMA
    pl.run_scoped(functools.partial(body, *refs), in_sem=dma((RING,)), q_sem=dma((8,)), c_sem=dma((3,)), s1=dma,
                  d1=dma((UNITS,)), s2=dma, d2=dma((UNITS // 2,)))


def put(vr, vi, mat, own, got, gain, outr, outi, lr, li, lhs, sem):
    cuts = [(pl.ds(7 * i, 7), slice(None)) for i in range(4)] + [(pl.ds(28, 4), pl.ds(0, 8))]
    copies = [pltpu.make_async_copy(v.at[cut], o.at[cut], sem) for cut in cuts for v, o in ((vr, outr), (vi, outi))]
    for copy in copies:
        copy.start()
    gather(lhs, 0, lambda v, rows: own[v, rows, :])
    gather(lhs, 256, lambda v, rows: got[v, rows, :])
    lane_product(lhs, mat, gain[256:, :], lr, li, lambda f: f)
    cut = (pl.ds(28, 4), pl.ds(8, 8))
    tail = [pltpu.make_async_copy(v, o.at[cut], sem) for v, o in ((lr, outr), (li, outi))]
    for copy in tail:
        copy.start()
    for copy in copies + tail:
        copy.wait()


def solution(mesh):
    f32 = jnp.float32

    def local_forward(u_real, u_imag, g_filter):
        parts = [jnp.transpose(v, (0, 2, 3, 1)).reshape(GROUPS, PACK, 16, 32, 64) for v in (u_real, u_imag)]
        spectrum = pl.pallas_call(
            kernel,
            out_shape=[pltpu.VMEM((32, 16, 32, 64), f32)] * 2 + [
                pltpu.VMEM((512, 512), f32), pltpu.VMEM((2, 256, 128), f32), pltpu.VMEM((2, 256, 128), f32),
                pltpu.VMEM((512, 128), f32)],
            in_specs=[pl.BlockSpec(memory_space=pltpu.HBM)] * 5,
            out_specs=[pl.BlockSpec(memory_space=pltpu.VMEM)] * 6,
            scratch_shapes=[
                pltpu.VMEM((2, RING, PACK, 16, 32, 64), f32),
                pltpu.VMEM((UNITS * 7, 16, 8, 128), f32),
                pltpu.VMEM((UNITS * 2, 256, 128), f32),
                pltpu.VMEM((UNITS, 256, 128), f32),
                pltpu.VMEM((2, 8, 8, 128), f32),
                pltpu.VMEM((16, 32, 64), f32),
                pltpu.VMEM((2, 2, 64, 128), f32),
                pltpu.VMEM((8, 8, 8, 128), f32),
                pltpu.VMEM((256, 512), f32),
            ],
            compiler_params=pltpu.CompilerParams(
                collective_id=0, has_side_effects=True, vmem_limit_bytes=40 * 1024 * 1024),
            name="dft3",
        )(*parts, g_filter, jnp.asarray(lane_matrix()), jnp.asarray(sublane_twiddle()))
        return pl.pallas_call(
            put,
            out_shape=[jax.ShapeDtypeStruct((32, 16, 32, 64), f32)] * 2,
            in_specs=[pl.BlockSpec(memory_space=pltpu.VMEM)] * 6,
            out_specs=[pl.BlockSpec(memory_space=pltpu.HBM)] * 2,
            scratch_shapes=[pltpu.VMEM((PACK, 8, 32, 64), f32)] * 2 + [pltpu.VMEM((256, 512), f32), pltpu.SemaphoreType.DMA],
            compiler_params=pltpu.CompilerParams(vmem_limit_bytes=8 * 1024 * 1024),
            name="put",
        )(*spectrum)

    field_spec = P("fld", None, "row", "col")
    out_spec = P("fld", "row", "col", None)
    return jax.shard_map(local_forward, mesh=mesh, in_specs=(field_spec, field_spec, P("row", "col", None)),
                         out_specs=(out_spec, out_spec), check_vma=False)
```

```python
import functools
import math

import jax
import jax.numpy as jnp
import numpy as np
from jax import lax
from jax.experimental import pallas as pl
from jax.experimental.pallas import tpu as pltpu
from jax.sharding import PartitionSpec as P

MESH = pl.DeviceIdType.MESH
HALF = math.sqrt(0.5)
GROUPS, PACK, UNITS, RING, LAG = 8, 4, 32, 4, 5


def interleave(even, odd):
    return [v for pair in zip(even, odd) for v in pair]


def dft4(b):
    (r0, i0), (r1, i1), (r2, i2), (r3, i3) = b
    sr0, si0, sr1, si1 = r0 + r2, i0 + i2, r0 - r2, i0 - i2
    sr2, si2, sr3, si3 = r1 + r3, i1 + i3, r1 - r3, i1 - i3
    return [(sr0 + sr2, si0 + si2), (sr1 + si3, si1 - sr3), (sr0 - sr2, si0 - si2), (sr1 - si3, si1 + sr3)]


def dft8(a):
    pairs = list(zip(a[:4], a[4:]))
    even = [(vr + wr, vi + wi) for (vr, vi), (wr, wi) in pairs]
    odd = [(vr - wr, vi - wi) for (vr, vi), (wr, wi) in pairs]
    o0, (r1, i1), (r2, i2), (r3, i3) = odd
    odd = [o0, ((r1 + i1) * HALF, (i1 - r1) * HALF), (i2, -r2), ((i3 - r3) * HALF, (r3 + i3) * -HALF)]
    even, odd = dft4(even), dft4(odd)
    return interleave(even, odd)


def rotate(v):
    sign = jnp.where(lax.broadcasted_iota(jnp.int32, v.shape, 0) < 4, 1.0, -1.0)
    return pltpu.roll(v, 4, 0) * sign


def packed_dft4(b):
    b0, b1, b2, b3 = b
    s0, s1, s2, s3 = b0 + b2, b0 - b2, b1 + b3, rotate(b1 - b3)
    return [s0 + s2, s1 + s3, s0 - s2, s1 - s3]


def packed_dft8(a):
    pairs = list(zip(a[:4], a[4:]))
    even = packed_dft4([v + w for v, w in pairs])
    o0, o1, o2, o3 = [v - w for v, w in pairs]
    odd = packed_dft4([o0, (rotate(o1) + o1) * HALF, rotate(o2), (rotate(o3) - o3) * HALF])
    return interleave(even, odd)


def times(a, tr, ti):
    return a[0] * tr - a[1] * ti, a[0] * ti + a[1] * tr


def twiddle(m):
    angle = -2.0 * math.pi * (m % 64) / 64.0
    return math.cos(angle) / 8.0, math.sin(angle) / 8.0


def lane_matrix():
    z, kz = np.arange(64), np.arange(64)
    angle = 2.0 * np.pi * ((z[:, None] * kz[None, :]) % 64) / 64.0
    cos, sin = np.cos(angle) / 8.0, np.sin(angle) / 8.0
    blocks = np.stack([np.concatenate([cos, -sin], 1), np.concatenate([sin, cos], 1)])
    out = np.zeros((2, 2, PACK, 32, PACK, 128))
    for c in range(2):
        for f in range(PACK):
            out[c, :, f, :, f, :] = blocks[:, 32 * c : 32 * c + 32]
    return out.reshape(2, 256, PACK * 128).astype(np.float32)


def sublane_twiddle():
    k1, x2 = np.arange(8), np.arange(8)
    angle = -2.0 * np.pi * (k1[:, None] * x2[None, :]) / 64.0
    both = np.stack([np.cos(angle), np.sin(angle)]) / 8.0
    return np.broadcast_to(both[..., None], (2, 8, 8, 128)).astype(np.float32)


def gather(dst, lane, plane):
    for kx in range(8):
        for q in range(2):
            dst[pl.ds(32 * kx, 32), pl.ds(lane + 128 * q, 128)] = plane(kx // 4, pl.ds(4 * q + kx % 4, 32, stride=8))


def lane_product(lhs, mat, gain, outr, outi, at):
    for n in range(2):
        w = jnp.dot(lhs[...], mat[:, 256 * n : 256 * n + 256], precision=lax.Precision.HIGHEST,
                    preferred_element_type=jnp.float32)
        for f in range(2):
            pair = w[:, 128 * f : 128 * f + 128] * gain
            outr[at(2 * n + f)] = pair[:, :64].reshape(8, 32, 64)
            outi[at(2 * n + f)] = pair[:, 64:].reshape(8, 32, 64)


def body(ur, ui, gf, wz, tw, outr, outi, wv, own, got, gv, inp, xbuf, b2, r2, tv, gs, asc, bsc, lsc,
           in_sem, q_sem, c_sem, s1, d1, s2, d2):
    row, col = lax.axis_index("row"), lax.axis_index("col")
    core = lax.rem(row, 2)
    dests = [1 + 2 * core, 2 - core, 3 - core]
    other = 1 - col

    def arrived(ref, sem):
        pltpu.make_async_remote_copy(src_ref=ref, dst_ref=ref, send_sem=sem, recv_sem=sem,
                                     device_id={"row": row}, device_id_type=MESH).wait_recv()

    def load(g, k):
        src, dst = (ur, ui)[k], inp.at[k]
        return pltpu.make_async_copy(src.at[g], dst.at[lax.rem(g, RING)], in_sem.at[lax.rem(g, RING)])

    def piece(i, k):
        src, dst = (ur, ui)[k], inp.at[k]
        part = (0, slice(None), pl.ds(2 * i, 2))
        return pltpu.make_async_copy(src.at[part], dst.at[part], q_sem.at[i])

    consts = [
        pltpu.make_async_copy(tw, tv, c_sem.at[0]),
        pltpu.make_async_copy(wz.at[col], wv.at[pl.ds(0, 256)], c_sem.at[1]),
        pltpu.make_async_copy(wz.at[other], wv.at[pl.ds(256, 256)], c_sem.at[1]),
        pltpu.make_async_copy(gf, gs, c_sem.at[2]),
    ]
    def start_piece(i):
        piece(i, 0).start()
        piece(i, 1).start()

    consts[0].start()
    start_piece(0)
    barrier = pltpu.get_barrier_semaphore()
    pl.semaphore_signal(barrier, inc=1, device_id={"col": other}, device_id_type=MESH)
    for p in (dests[1], dests[2], dests[0]):
        pl.semaphore_signal(barrier, inc=1, device_id={"row": lax.rem(row + p, 4)}, device_id_type=MESH)

    @pl.loop(1, 8)
    def _(i):
        start_piece(i)


    def step_x(g, first, count):
        ring = lax.rem(g, RING)
        bases = [4 * g * 7 + 3 + lax.rem(k + 4 - row, 4) for k in range(4)]

        def one(i, s):
            y = first + 2 * i + s
            ar = inp[0, ring, :, y].reshape(PACK * 32, 64).T
            ai = inp[1, ring, :, y].reshape(PACK * 32, 64).T
            a = dft8([(ar[8 * j : 8 * j + 8], ai[8 * j : 8 * j + 8]) for j in range(8)])
            for k1 in range(8):
                vr, vi = times(a[k1], tv[0, k1], tv[1, k1])
                asc[s, 0, pl.ds(8 * k1, 8), :] = vr
                asc[s, 1, pl.ds(8 * k1, 8), :] = vi
            b = dft8([tuple(asc[s, q, pl.ds(x2, 8, stride=8), :] for q in range(2)) for x2 in range(8)])
            top = lax.broadcasted_iota(jnp.int32, (8, 128), 0) < 4
            for k2, (vr, vi) in enumerate(b):
                at = bases[k2 // 2] + 14 * (k2 % 2)
                xbuf[at, y] = jnp.where(top, vr, pltpu.roll(vi, 4, 0))
                xbuf[at + 7, y] = jnp.where(top, pltpu.roll(vr, 4, 0), vi)

        def pair(i):
            one(i, 0)
            one(i, 1)

        pl.loop(0, count // 2)(pair) if count > 2 else pair(0)

    def send_row(u, j, first=0, count=16):
        p = dests[j]
        return pltpu.make_async_remote_copy(
            src_ref=xbuf.at[u * 7 + 3 + p, pl.ds(first, count)], dst_ref=xbuf.at[u * 7 + 3 - p, pl.ds(first, count)],
            send_sem=s1, recv_sem=d1.at[u],
            device_id={"row": lax.rem(row + p, 4)}, device_id_type=MESH)

    def send_col(u, dst):
        return pltpu.make_async_remote_copy(
            src_ref=b2.at[u * 2 + other], dst_ref=dst,
            send_sem=s2, recv_sem=d2.at[u // 2], device_id={"col": other}, device_id_type=MESH)

    def step_y(u):
        arrived(xbuf.at[pl.ds(u * 7, 3)], d1.at[u])
        slots = [u * 7 + lax.rem(r + 7 - row, 4) for r in range(4)]
        for y2 in range(8):
            a = packed_dft8([xbuf[slots[y1 // 2], 8 * (y1 % 2) + y2] for y1 in range(8)])
            for k1 in range(8):
                tr, ti = twiddle(k1 * y2)
                bsc[k1, y2] = a[k1] * tr - rotate(a[k1]) * ti if k1 * y2 else a[k1] * tr
        for k1 in range(8):
            b = packed_dft8([bsc[k1, y2] for y2 in range(8)])
            for k2 in range(8):
                b2[u * 2 + k2 // 4, pl.ds(8 * (k1 + 8 * (k2 % 4)), 8), :] = b[k2]

        @pl.when(u < UNITS - 2)
        def _():
            send_col(u, r2.at[u]).start()

        @pl.when(u >= UNITS - 2)
        def _():
            send_col(u, got.at[u - UNITS + 2]).start()

    def step_z(m):
        gather(lsc, 0, lambda v, rows: b2[(2 * m + v) * 2 + col, rows, :])
        arrived(r2.at[pl.ds(2 * m, 2)], d2.at[m])
        gather(lsc, 256, lambda v, rows: r2[2 * m + v, rows, :])
        gain = gv[pl.ds(pl.multiple_of(256 * lax.rem(m, 2), 256), 256), :]
        lane_product(lsc, wv, gain, outr, outi, lambda f: (PACK * (m // 2) + f, pl.ds(8 * lax.rem(m, 2), 8)))

    consts[0].wait()
    def first_group(i):
        arrived(inp.at[:, 0, :, pl.ds(2 * i, 2)], q_sem.at[i])
        step_x(0, 2 * i, 2)

    first_group(0)
    pl.semaphore_wait(barrier, 4)
    send_row(0, 1, 0, 2).start()

    @pl.loop(1, 8)
    def _(i):
        first_group(i)
        send_row(0, 1, 2 * i, 2).start()

    send_row(0, 0).start()
    send_row(1, 1).start()
    send_row(1, 0).start()
    send_row(0, 2).start()

    def send_rows(first, last):
        @pl.loop(first, last)
        def _(u):
            send_row(u, 1).start()
            send_row(u, 0).start()
            send_row(u - 1, 2).start()

    send_rows(2, 4)

    @pl.loop(1, RING)
    def _(g):
        load(g, 0).start()
        load(g, 1).start()

    for copy in consts[1:]:
        copy.start()
    step_y(0)
    for k in range(2):
        load(RING, k).start()
    arrived(inp.at[:, 1], in_sem.at[1])
    step_x(1, 0, 16)
    send_rows(4, 8)
    for k in range(2):
        load(RING + 1, k).start()
    arrived(wv, c_sem.at[1])
    consts[3].wait()
    gain = gs[...].reshape(512, 64)
    gv[...] = jnp.concatenate([gain, gain], axis=1)

    @pl.loop(1, UNITS + LAG - 3)
    def _(t):
        @pl.when(t < UNITS)
        def _():
            step_y(t)

        g, i = (t + 7) // 4, lax.rem(t + 3, 4)

        @pl.when(g < GROUPS)
        def _():
            @pl.when(i == 0)
            def _():
                arrived(inp.at[:, lax.rem(g, RING)], in_sem.at[lax.rem(g, RING)])

            step_x(g, 4 * i, 4)

            @pl.when(i == 3)
            def _():
                send_rows(4 * g, 4 * g + 4)

                @pl.when(g == GROUPS - 1)
                def _():
                    send_row(UNITS - 1, 2).start()

                @pl.when(g + RING < GROUPS)
                def _():
                    load(g + RING, 0).start()
                    load(g + RING, 1).start()

        @pl.when((t >= LAG) & (lax.rem(t - LAG, 2) == 0))
        def _():
            step_z((t - LAG) // 2)

    arrived(xbuf.at[pl.ds(0, 3 * UNITS)], s1)
    for v in range(2):
        own[v] = b2[2 * (UNITS - 2 + v) + col]
    arrived(got, d2.at[UNITS // 2 - 1])
    arrived(b2.at[pl.ds(0, UNITS)], s2)


def kernel(*refs):
    dma = pltpu.SemaphoreType.DMA
    pl.run_scoped(functools.partial(body, *refs), in_sem=dma((RING,)), q_sem=dma((8,)), c_sem=dma((3,)), s1=dma,
                  d1=dma((UNITS,)), s2=dma, d2=dma((UNITS // 2,)))


def put(vr, vi, mat, own, got, gain, outr, outi, lr, li, lhs, sem):
    cuts = [(pl.ds(7 * i, 7), slice(None)) for i in range(4)] + [(pl.ds(28, 4), pl.ds(0, 8))]
    copies = [pltpu.make_async_copy(v.at[cut], o.at[cut], sem) for cut in cuts for v, o in ((vr, outr), (vi, outi))]
    for copy in copies:
        copy.start()
    gather(lhs, 0, lambda v, rows: own[v, rows, :])
    gather(lhs, 256, lambda v, rows: got[v, rows, :])
    lane_product(lhs, mat, gain[256:, :], lr, li, lambda f: f)
    cut = (pl.ds(28, 4), pl.ds(8, 8))
    tail = [pltpu.make_async_copy(v, o.at[cut], sem) for v, o in ((lr, outr), (li, outi))]
    for copy in tail:
        copy.start()
    for copy in copies + tail:
        copy.wait()


def solution(mesh):
    f32 = jnp.float32

    def local_forward(u_real, u_imag, g_filter):
        parts = [jnp.transpose(v, (0, 2, 3, 1)).reshape(GROUPS, PACK, 16, 32, 64) for v in (u_real, u_imag)]
        spectrum = pl.pallas_call(
            kernel,
            out_shape=[pltpu.VMEM((32, 16, 32, 64), f32)] * 2 + [
                pltpu.VMEM((512, 512), f32), pltpu.VMEM((2, 256, 128), f32), pltpu.VMEM((2, 256, 128), f32),
                pltpu.VMEM((512, 128), f32)],
            in_specs=[pl.BlockSpec(memory_space=pltpu.HBM)] * 5,
            out_specs=[pl.BlockSpec(memory_space=pltpu.VMEM)] * 6,
            scratch_shapes=[
                pltpu.VMEM((2, RING, PACK, 16, 32, 64), f32),
                pltpu.VMEM((UNITS * 7, 16, 8, 128), f32),
                pltpu.VMEM((UNITS * 2, 256, 128), f32),
                pltpu.VMEM((UNITS, 256, 128), f32),
                pltpu.VMEM((2, 8, 8, 128), f32),
                pltpu.VMEM((16, 32, 64), f32),
                pltpu.VMEM((2, 2, 64, 128), f32),
                pltpu.VMEM((8, 8, 8, 128), f32),
                pltpu.VMEM((256, 512), f32),
            ],
            compiler_params=pltpu.CompilerParams(
                collective_id=0, has_side_effects=True, vmem_limit_bytes=40 * 1024 * 1024),
            name="dft3",
        )(*parts, g_filter, jnp.asarray(lane_matrix()), jnp.asarray(sublane_twiddle()))
        return pl.pallas_call(
            put,
            out_shape=[jax.ShapeDtypeStruct((32, 16, 32, 64), f32)] * 2,
            in_specs=[pl.BlockSpec(memory_space=pltpu.VMEM)] * 6,
            out_specs=[pl.BlockSpec(memory_space=pltpu.HBM)] * 2,
            scratch_shapes=[pltpu.VMEM((PACK, 8, 32, 64), f32)] * 2 + [pltpu.VMEM((256, 512), f32), pltpu.SemaphoreType.DMA],
            compiler_params=pltpu.CompilerParams(vmem_limit_bytes=8 * 1024 * 1024),
            name="put",
        )(*spectrum)

    field_spec = P("fld", None, "row", "col")
    out_spec = P("fld", "row", "col", None)
    return jax.shard_map(local_forward, mesh=mesh, in_specs=(field_spec, field_spec, P("row", "col", None)),
                         out_specs=(out_spec, out_spec), check_vma=False)
```
